128 devices in a mesh: cuts: 32 (over x_hi, y, z), event: 4 (over x_lo, core).
Axes of the slice: x: 4 (x_hi: 2, x_lo: 2; x = x_hi * 2 + x_lo), y: 4, z: 4, core: 2. Of those that a mesh axis runs over, the one named last changes fastest.
Arguments:
- kernels: float32 [4, 256, 128, 256], P('event', 'cuts'), may hold values from -24 to 24
- steps: float32 [8, 256, 128, 256], P(None, 'cuts', 'event'), may hold values from -11 to 11
- curvature: float32 [8, 256, 128, 256], P(None, 'cuts', 'event'), may hold values from 0.2 to 5
Outputs:
- gradient: float32 [256, 128, 256], P('cuts', 'event')
- direction: float32 [256, 128, 256], P('cuts', 'event')
The draws below stay inside these ranges and needn't reach their ends.
All inputs are finite; a program needn't handle non-finite values.
Results may differ from the reference program's by a relative error of at most 0.00021.
Values sent between devices are 32-bit elements; how exact they have to be, the bound alone decides.
No kernel may reach another device: no remote copies, remote signals or barrier semaphores. Data moves between devices by JAX's collectives and lax.ppermute only.
A program may use at most 64 MiB of HBM per device.

```python
import math
import jax
import jax.numpy as jnp
from jax import lax

NR = 128
NB = 256
PAIRS = 8
RIM = 4
NA = 256
GROUPS = 4


def band_matrix(length, sigma):
    points = jnp.arange(length, dtype=jnp.float32)
    offset = points[:, None] - points[None, :]
    return jnp.exp(-offset * offset / (2.0 * sigma * sigma))


def circle_matrix(length, sigma):
    points = jnp.arange(length, dtype=jnp.float32)
    offset = jnp.abs(points[:, None] - points[None, :])
    offset = jnp.minimum(offset, length - offset)
    return jnp.exp(-offset * offset / (2.0 * sigma * sigma))


def shared_field(key):
    white = jax.random.truncated_normal(jax.random.fold_in(key, 101), -4.0, 4.0, (NA, NR, NB), jnp.float32)
    lon_mat = circle_matrix(NA, 3.0)
    rad_mat = band_matrix(NR, max(2.0, NR / 16.0))
    lat_mat = band_matrix(NB, max(2.0, NB / 32.0))
    field = jnp.einsum('ia,ajb->ijb', lon_mat, white, precision=lax.Precision.HIGHEST)
    field = jnp.einsum('rj,ajb->arb', rad_mat, field, precision=lax.Precision.HIGHEST)
    field = jnp.einsum('ajb,cb->ajc', field, lat_mat, precision=lax.Precision.HIGHEST)
    field = field / jnp.sqrt(jnp.mean(field * field))
    field = jnp.clip(field, -4.0, 4.0)
    return field


def draw_kernels(key, part):
    field = shared_field(key)
    gains = jax.random.uniform(jax.random.fold_in(key, 202), (GROUPS,), jnp.float32, 0.5, 1.5)
    noise = 4.0 * jax.random.truncated_normal(jax.random.fold_in(key, 203), -4.0, 4.0, (GROUPS, NA, NR, NB), jnp.float32)
    return gains[:, None, None, None] * field[None] + noise


def draw_steps(key, part):
    field = shared_field(key)
    factors = jax.random.uniform(jax.random.fold_in(key, 303), (PAIRS,), jnp.float32, 0.3, 1.5)
    noise = jax.random.truncated_normal(jax.random.fold_in(key, 304), -4.0, 4.0, (PAIRS, NA, NR, NB), jnp.float32)
    return -factors[:, None, None, None] * field[None] + noise


def levels(rng, dims, split, smallest, top_value):
    factor_of, own = 1.0, jax.random.fold_in(rng, 6)
    for dim, parts in split:
        steps = jnp.exp(jax.random.uniform(jax.random.fold_in(own, dim), (parts,), jnp.float32, smallest / len(split), top_value / len(split)))
        factor_of = factor_of * jnp.repeat(steps, dims[dim] // parts).reshape([-1 if axis == dim else 1 for axis in range(len(dims))])
    return factor_of


def setup_inputs(seed: int = 0) -> dict:
    streams_of = jax.random.split(jax.random.key(seed), 4)
    kernels = draw_kernels(jax.random.fold_in(streams_of[3], 71), 0)
    steps = draw_steps(jax.random.fold_in(streams_of[3], 71), 0)
    curvature = jnp.clip(jnp.exp(math.log(5.0) - 3.218876 * jax.random.uniform(streams_of[2], (PAIRS, NA, NR, NB), jnp.float32) ** levels(streams_of[2], (PAIRS, NA, NR, NB), ((1, 32), (2, 4)), -0.2, 0.2)), 0.2, 5.0)
    return {"kernels": kernels, "steps": steps, "curvature": curvature}


def gauss_matrix(length, sigma):
    points = jnp.arange(length, dtype=jnp.float32)
    offset = points[:, None] - points[None, :]
    matrix = jnp.exp(-offset * offset / (2.0 * sigma * sigma))
    return matrix / jnp.sum(matrix, axis=1, keepdims=True)


def cycle_weights():
    unscaled = [math.exp(-((column - RIM) ** 2) / 4.5) for column in range(2 * RIM + 1)]
    whole = sum(unscaled)
    return [weight / whole for weight in unscaled]


def reference(kernels, steps, curvature):
    summed = jnp.sum(kernels, axis=0)
    radial = jnp.einsum("ij,ajb->aib", gauss_matrix(summed.shape[1], 3.0), summed, precision=lax.Precision.HIGHEST)
    lat_len = radial.shape[2]
    plane = jnp.dot(radial.reshape(-1, lat_len), gauss_matrix(lat_len, 4.0).T, precision=lax.Precision.HIGHEST).reshape(radial.shape)
    weights = cycle_weights()
    gradient = jnp.zeros_like(plane)
    for column in range(2 * RIM + 1):
        gradient = gradient + weights[column] * jnp.roll(plane, RIM - column, axis=0)
    changes = curvature * steps
    curvs = jnp.sum(changes * steps, axis=(1, 2, 3))
    inverse = 1.0 / curvs
    scaling = curvs[PAIRS - 1] / jnp.sum(changes[PAIRS - 1] * changes[PAIRS - 1])
    carried = gradient
    alphas = [None] * PAIRS
    for pair in reversed(range(PAIRS)):
        alphas[pair] = inverse[pair] * jnp.sum(steps[pair] * carried)
        carried = carried - alphas[pair] * changes[pair]
    result = scaling * carried
    for pair in range(PAIRS):
        second = inverse[pair] * jnp.sum(changes[pair] * result)
        result = result + (alphas[pair] - second) * steps[pair]
    return gradient, -result
```

```python
import functools
import math

import jax
import jax.numpy as jnp
import numpy as np
from jax import lax
from jax.experimental import pallas as pl
from jax.experimental.pallas import tpu as pltpu
from jax.sharding import Mesh
from jax.sharding import PartitionSpec as P

PAIRS = 8
RIM = 4
CUTS = ("cuts_0", "cuts_1", "cuts_2")
EVENT = ("event_0", "event_1")
CUTS_EVENT = ("cuts_0", "cuts_1", "cuts_2", "event_0", "event_1")
LANES = 128
SQUARES, STEPS_GRADIENT, CHANGES_GRADIENT = 64, 100, 108


def square_lane(i, j):
    low, high = min(i, j), max(i, j)
    return SQUARES + low * PAIRS - low * (low - 1) // 2 + high - low


def gauss_matrix(length, sigma):
    points = np.arange(length, dtype=np.float64)
    offset = points[:, None] - points[None, :]
    matrix = np.exp(-offset * offset / (2.0 * sigma * sigma))
    return (matrix / matrix.sum(axis=1, keepdims=True)).astype(np.float32)


def halves(matrix):
    high = matrix.astype(jnp.bfloat16)
    low = (matrix - high.astype(np.float32)).astype(jnp.bfloat16)
    return high, low


def cycle_weights():
    unscaled = [math.exp(-((column - RIM) ** 2) / 4.5) for column in range(2 * RIM + 1)]
    whole = sum(unscaled)
    return [weight / whole for weight in unscaled]


def split(x):
    high = x.astype(jnp.bfloat16)
    low = (x - high.astype(jnp.float32)).astype(jnp.bfloat16)
    return high, low


def dot(a, b):
    return jnp.dot(a, b, preferred_element_type=jnp.float32)


def call(kernel, outs, flops, moved, limit=16):
    return pl.pallas_call(
        kernel,
        out_shape=[jax.ShapeDtypeStruct(shape, jnp.float32) for shape in outs],
        compiler_params=pltpu.CompilerParams(vmem_limit_bytes=limit << 20),
        cost_estimate=pl.CostEstimate(flops=flops, bytes_accessed=moved, transcendentals=0),
    )


def radial_kernel(kernels_ref, high_ref, low_ref, keep_ref, pass_ref, send_ref):
    part = 2 * lax.axis_index("event_0") + lax.axis_index("event_1")
    rows = kernels_ref.shape[2] // 4
    order = [part, part ^ 2, part ^ 1, part ^ 3]
    starts = [pl.multiple_of(block * rows, rows) for block in order]
    weights = jnp.concatenate(
        [ref[pl.ds(start, rows), :] for ref in (high_ref, low_ref) for start in starts], axis=0
    )
    for a in range(kernels_ref.shape[1]):
        both = dot(weights, jnp.concatenate(split(kernels_ref[0, a]), axis=0))
        out = both[: 4 * rows] + both[4 * rows :]
        keep_ref[a] = out[:rows]
        pass_ref[a] = out[rows : 2 * rows]
        send_ref[0, a] = out[2 * rows : 3 * rows]
        send_ref[1, a] = out[3 * rows :]


def latitude_kernel(keep_ref, near_ref, far_ref, high_ref, low_ref, head_ref, tail_ref):
    lons, rows, lats = keep_ref.shape
    summed = (keep_ref[...] + near_ref[0] + far_ref[...]).reshape(lons * rows, lats)
    both = jnp.concatenate(split(summed), axis=0)
    out = dot(both, high_ref[...]) + dot(both, low_ref[...])
    plane = (out[: lons * rows] + out[lons * rows :]).reshape(lons, rows, lats)
    head_ref[...] = plane[:RIM]
    tail_ref[...] = plane[lons - RIM :]


def lane_numbers():
    return lax.broadcasted_iota(jnp.int32, (8, LANES), 1)


def tiles(shape):
    return [
        (a, slice(8 * r, 8 * r + 8), slice(LANES * b, LANES * (b + 1)))
        for r in range(shape[1] // 8)
        for b in range(shape[2] // LANES)
        for a in range(shape[0])
    ]


def placed(sums):
    lanes = lane_numbers()
    row = jnp.zeros((8, LANES), jnp.float32)
    for lane, value in sums:
        row = row + jnp.where(lanes == lane, jnp.sum(value, axis=1, keepdims=True), 0.0)
    return row


def gram_kernel(steps_ref, curvature_ref, changes_ref, row_ref):
    lons, rows, lats = steps_ref.shape[1:]
    zero = jnp.zeros((8, LANES), jnp.float32)

    def tile(ref, pair, t):
        r = t // (lats // LANES) % (rows // 8)
        b = t % (lats // LANES)
        a = t // (lats // LANES * (rows // 8))
        return (pair, a, pl.ds(pl.multiple_of(r * 8, 8), 8), pl.ds(pl.multiple_of(b * LANES, LANES), LANES))

    count = lons * (rows // 8) * (lats // LANES)

    def first(t, sums):
        steps = [steps_ref[tile(None, i, t)] for i in range(PAIRS)]
        changes = [curvature_ref[tile(None, i, t)] * steps[i] for i in range(PAIRS)]
        for i in range(PAIRS):
            changes_ref[tile(None, i, t)] = changes[i]
        return [sums[i * PAIRS + j] + steps[i] * changes[j] for i in range(4) for j in range(PAIRS)]

    def second(t, sums):
        steps = [steps_ref[tile(None, i, t)] for i in range(4, PAIRS)]
        changes = [changes_ref[tile(None, i, t)] for i in range(PAIRS)]
        return [sums[i * PAIRS + j] + steps[i] * changes[j] for i in range(4) for j in range(PAIRS)]

    upper = [(i, j) for i in range(PAIRS) for j in range(i, PAIRS)]

    def third(t, sums):
        changes = [changes_ref[tile(None, i, t)] for i in range(PAIRS)]
        return [value + changes[i] * changes[j] for value, (i, j) in zip(sums, upper)]

    row = zero
    for number, step, size in ((0, first, 32), (1, second, 32), (2, third, len(upper))):
        sums = lax.fori_loop(0, count, step, [zero] * size)
        row = row + placed([(32 * number + k, value) for k, value in enumerate(sums)])
    row_ref[...] = row


def product_kernel(head_ref, tail_ref, left_ref, right_ref, steps_ref, changes_ref, gram_ref, gradient_ref, rows_ref):
    lons, rows, lats = gradient_ref.shape
    weights = cycle_weights()
    sums = [jnp.zeros((8, LANES), jnp.float32) for _ in range(2 * PAIRS)]
    for r in range(rows // 8):
        for b in range(lats // LANES):
            at = (slice(8 * r, 8 * r + 8), slice(LANES * b, LANES * (b + 1)))
            padded = [ref[(a, *at)] for ref in (left_ref, head_ref, tail_ref, right_ref) for a in range(RIM)]
            for a in range(lons):
                value = weights[RIM] * padded[a + RIM]
                for k in range(RIM):
                    value = value + weights[k] * (padded[a + k] + padded[a + 2 * RIM - k])
                gradient_ref[(a, *at)] = value
                for pair in range(PAIRS):
                    sums[pair] = sums[pair] + steps_ref[(pair, a, *at)] * value
                    sums[PAIRS + pair] = sums[PAIRS + pair] + changes_ref[(pair, a, *at)] * value
    row = gram_ref[...] + placed([(STEPS_GRADIENT + k, value) for k, value in enumerate(sums)])
    row = jnp.sum(row, axis=0, keepdims=True)
    rows_ref[...] = jnp.broadcast_to(row[None], rows_ref.shape)


def direction_kernel(rows_ref, gradient_ref, steps_ref, changes_ref, direction_ref):
    row = jnp.broadcast_to(jnp.sum(rows_ref[...], axis=0), (8, LANES))
    lanes = lane_numbers()
    pairs = lax.broadcasted_iota(jnp.int32, (8, LANES), 0)

    def column(lane_of):
        picked = jnp.where(lanes == lane_of, row, 0.0)
        return jnp.broadcast_to(jnp.sum(picked, axis=1, keepdims=True), (8, LANES))

    def element(vector, i):
        return jnp.broadcast_to(vector[i : i + 1], (8, LANES))

    def square_lanes(j):
        low, high = jnp.minimum(pairs, j), jnp.maximum(pairs, j)
        return SQUARES + low * PAIRS - ((low * (low - 1)) >> 1) + high - low

    by_change = [column(pairs * PAIRS + i) for i in range(PAIRS)]
    by_step = [column(pairs + PAIRS * i) for i in range(PAIRS)]
    squares = [column(square_lanes(i)) for i in range(PAIRS)]
    curvs = column(pairs * (PAIRS + 1))
    steps_part = column(pairs + STEPS_GRADIENT)
    changes_part = column(pairs + CHANGES_GRADIENT)
    inverse = 1.0 / curvs
    scaling = element(curvs, PAIRS - 1) / element(squares[PAIRS - 1], PAIRS - 1)
    alphas = [None] * PAIRS
    for i in reversed(range(PAIRS)):
        alphas[i] = element(inverse * steps_part, i)
        steps_part = steps_part - alphas[i] * by_change[i]
        changes_part = changes_part - alphas[i] * squares[i]
    changes_part = scaling * changes_part
    weights = [None] * PAIRS
    for i in range(PAIRS):
        weights[i] = alphas[i] - element(inverse * changes_part, i)
        changes_part = changes_part + weights[i] * by_step[i]
    change_weights = [scaling * alpha for alpha in alphas]
    for a, r, b in tiles(gradient_ref.shape):
        value = -(scaling * gradient_ref[a, r, b])
        for i in range(PAIRS):
            value = value + change_weights[i] * changes_ref[i, a, r, b]
            value = value - weights[i] * steps_ref[i, a, r, b]
        direction_ref[a, r, b] = value


def shifted(x, axis, shift):
    count = lax.axis_size(axis)
    return lax.ppermute(x, axis, [(i, (i + shift) % count) for i in range(count)])


def shards(kernels, steps, curvature):
    _, lons, rad_len, lats = kernels.shape
    rows = rad_len // 4
    block = (lons, rows, lats)
    size = lons * rows * lats
    high, low = (np.concatenate([m, m], axis=1) for m in halves(gauss_matrix(rad_len, 3.0)))
    keep, pass_on, send = call(
        radial_kernel, [block, block, (2, *block)], 2 * 4 * rad_len * kernels.size, 8 * kernels.size
    )(kernels, jnp.asarray(high), jnp.asarray(low))
    near = shifted(send, "event_1", 1)
    far = shifted(pass_on + near[1], "event_0", 1)
    changes, gram = call(
        gram_kernel, [steps.shape, (8, LANES)], 2 * 100 * size, 12 * steps.size
    )(steps, curvature)
    high, low = halves(gauss_matrix(lats, 4.0).T)
    side = (RIM, rows, lats)
    head, tail = call(latitude_kernel, [side, side], 2 * 4 * lats * size, 16 * size)(
        keep, near, far, jnp.asarray(high), jnp.asarray(low)
    )
    left = shifted(tail, CUTS, 1)
    right = shifted(head, CUTS, -1)
    devices = lax.axis_size(CUTS_EVENT)
    gradient, outgoing = call(
        product_kernel, [block, (devices, 1, LANES)], 2 * 30 * size, 4 * 20 * size
    )(head, tail, left, right, steps, changes, gram)
    arrived = lax.all_to_all(outgoing, CUTS_EVENT, 0, 0, tiled=True)
    (direction,) = call(direction_kernel, [block], 2 * 17 * size, 4 * 18 * size)(
        arrived, gradient, steps, changes
    )
    return (gradient, direction)


def solution(mesh):
    torus = Mesh(
        mesh.devices.reshape(2, 4, 4, 2, 2), ("cuts_0", "cuts_1", "cuts_2", "event_0", "event_1")
    )
    in_specs = (P(EVENT, CUTS, None, None), P(None, CUTS, EVENT, None), P(None, CUTS, EVENT, None))
    out_specs = (P(CUTS, EVENT, None), P(CUTS, EVENT, None))
    return jax.shard_map(
        shards, mesh=torus, in_specs=in_specs, out_specs=out_specs, check_vma=False
    )
```

```python
import functools
import math

import jax
import jax.numpy as jnp
from jax import lax
from jax.experimental import pallas as pl
from jax.experimental.pallas import tpu as pltpu
from jax.sharding import Mesh
from jax.sharding import PartitionSpec as P

PAIRS = 8
RIM = 4
CUTS = ("cuts_0", "cuts_1", "cuts_2")
EVENT = ("event_0", "event_1")
CUTS_EVENT = ("cuts_0", "cuts_1", "cuts_2", "event_0", "event_1")
LANES = 128
SQUARES, STEPS_GRADIENT, CHANGES_GRADIENT = 64, 100, 108


def square_lane(i, j):
    low, high = min(i, j), max(i, j)
    return SQUARES + low * PAIRS - low * (low - 1) // 2 + high - low


def cycle_weights():
    unscaled = [math.exp(-((column - RIM) ** 2) / 4.5) for column in range(2 * RIM + 1)]
    whole = sum(unscaled)
    return [weight / whole for weight in unscaled]


def split(x):
    high = x.astype(jnp.bfloat16)
    low = (x - high.astype(jnp.float32)).astype(jnp.bfloat16)
    return high, low


def dot(a, b):
    return jnp.dot(a, b, preferred_element_type=jnp.float32)


def call(kernel, outs, flops, moved, limit=16, **options):
    return pl.pallas_call(
        kernel,
        out_shape=[jax.ShapeDtypeStruct(*out) for out in outs],
        compiler_params=pltpu.CompilerParams(vmem_limit_bytes=limit << 20),
        cost_estimate=pl.CostEstimate(flops=flops, bytes_accessed=moved, transcendentals=0),
        **options,
    )


def gauss_rows(length, sigma, rows, axis):
    offset = (rows - lax.broadcasted_iota(jnp.int32, rows.shape, axis)).astype(jnp.float32)
    matrix = jnp.exp(-offset * offset / (2.0 * sigma * sigma))
    return matrix / jnp.sum(matrix, axis=axis, keepdims=True)


def radial_kernel(kernels_ref, keep_ref, pass_ref, send_ref, held_ref, semaphores):
    _, lons, length, lats = kernels_ref.shape
    copies = [
        pltpu.make_async_copy(kernels_ref.at[0, a], held_ref.at[a], semaphores.at[a])
        for a in range(lons)
    ]
    for copy in copies:
        copy.start()
    part = 2 * lax.axis_index("event_0") + lax.axis_index("event_1")
    rows = length // 4
    local = lax.broadcasted_iota(jnp.int32, (rows, length), 0)
    order = [part, part ^ 2, part ^ 1, part ^ 3]
    matrix = jnp.concatenate(
        [gauss_rows(length, 3.0, local + rows * block, 1) for block in order], axis=0
    )
    weights = jnp.concatenate([jnp.concatenate([m, m], axis=1) for m in split(matrix)], axis=0)
    for a in range(lons):
        copies[a].wait()
        both = dot(weights, jnp.concatenate(split(held_ref[a]), axis=0))
        out = both[:length] + both[length:]
        keep_ref[a] = out[:rows]
        pass_ref[a] = out[rows : 2 * rows]
        send_ref[0, a] = out[2 * rows : 3 * rows]
        send_ref[1, a] = out[3 * rows :]


def latitude_kernel(keep_ref, near_ref, far_ref, high_ref, low_ref, head_ref, tail_ref):
    lons, rows, lats = keep_ref.shape
    summed = (keep_ref[...] + near_ref[0] + far_ref[...]).reshape(lons * rows, lats)
    both = jnp.concatenate(split(summed), axis=0)
    out = dot(both, high_ref[...]) + dot(both, low_ref[...])
    plane = (out[: lons * rows] + out[lons * rows :]).reshape(lons, rows, lats)
    head_ref[...] = plane[:RIM]
    tail_ref[...] = plane[lons - RIM :]


def lane_numbers():
    return lax.broadcasted_iota(jnp.int32, (8, LANES), 1)


def tiles(shape):
    return [
        (a, slice(8 * r, 8 * r + 8), slice(LANES * b, LANES * (b + 1)))
        for r in range(shape[1] // 8)
        for b in range(shape[2] // LANES)
        for a in range(shape[0])
    ]


def placed(sums):
    lanes = lane_numbers()
    row = jnp.zeros((8, LANES), jnp.float32)
    for lane, value in sums:
        row = row + jnp.where(lanes == lane, jnp.sum(value, axis=1, keepdims=True), 0.0)
    return row


def gram_kernel(steps_ref, curvature_ref, changes_ref, row_ref, high_ref, low_ref):
    lons, rows, lats = steps_ref.shape[1:]
    column = lax.broadcasted_iota(jnp.int32, (lats, lats), 1)
    high_ref[...], low_ref[...] = split(gauss_rows(lats, 4.0, column, 0))
    spots = [
        (slice(8 * r, 8 * r + 8), slice(LANES * b, LANES * (b + 1)))
        for r in range(rows // 8)
        for b in range(lats // LANES)
    ]
    half = PAIRS // 2
    upper = [(i, j) for i in range(PAIRS) for j in range(i, PAIRS)]

    def first(a, sums):
        for at in spots:
            steps = [steps_ref[(i, a, *at)] for i in range(half)]
            changes = [None] * PAIRS
            for i in range(PAIRS):
                step = steps[i] if i < half else steps_ref[(i, a, *at)]
                changes[i] = curvature_ref[(i, a, *at)] * step
                changes_ref[(i, a, *at)] = changes[i]
            sums = [sums[k] + steps[k // PAIRS] * changes[k % PAIRS] for k in range(half * PAIRS)]
        return sums

    def second(a, sums):
        for at in spots:
            steps = [steps_ref[(i, a, *at)] for i in range(half, PAIRS)]
            changes = [changes_ref[(i, a, *at)] for i in range(PAIRS)]
            sums = [sums[k] + steps[k // PAIRS] * changes[k % PAIRS] for k in range(half * PAIRS)]
        return sums

    def third(a, sums):
        for at in spots:
            changes = [changes_ref[(i, a, *at)] for i in range(PAIRS)]
            sums = [value + changes[i] * changes[j] for value, (i, j) in zip(sums, upper)]
        return sums

    zero = jnp.zeros((8, LANES), jnp.float32)
    row = zero
    for start, step, size in ((0, first, 32), (32, second, 32), (SQUARES, third, len(upper))):
        sums = lax.fori_loop(0, lons, step, [zero] * size)
        row = row + placed([(start + k, value) for k, value in enumerate(sums)])
    row_ref[...] = row


def product_kernel(head_ref, tail_ref, left_ref, right_ref, steps_ref, changes_ref, gram_ref, gradient_ref, kept_ref, rows_ref):
    lons, rows, lats = gradient_ref.shape
    weights = cycle_weights()
    sums = [jnp.zeros((8, LANES), jnp.float32) for _ in range(2 * PAIRS)]
    for r in range(rows // 8):
        for b in range(lats // LANES):
            at = (slice(8 * r, 8 * r + 8), slice(LANES * b, LANES * (b + 1)))
            padded = [ref[(a, *at)] for ref in (left_ref, head_ref, tail_ref, right_ref) for a in range(RIM)]
            for a in range(lons):
                value = weights[RIM] * padded[a + RIM]
                for k in range(RIM):
                    value = value + weights[k] * (padded[a + k] + padded[a + 2 * RIM - k])
                gradient_ref[(a, *at)] = value
                kept_ref[(a, *at)] = value
                for pair in range(PAIRS):
                    sums[pair] = sums[pair] + steps_ref[(pair, a, *at)] * value
                    sums[PAIRS + pair] = sums[PAIRS + pair] + changes_ref[(pair, a, *at)] * value
    row = gram_ref[...] + placed([(STEPS_GRADIENT + k, value) for k, value in enumerate(sums)])
    row = jnp.sum(row, axis=0, keepdims=True)
    rows_ref[...] = jnp.broadcast_to(row[None], rows_ref.shape)


def direction_kernel(rows_ref, gradient_ref, steps_ref, changes_ref, direction_ref):
    row = jnp.broadcast_to(jnp.sum(rows_ref[...], axis=0), (8, LANES))
    lanes = lane_numbers()
    pairs = lax.broadcasted_iota(jnp.int32, (8, LANES), 0)

    def column(lane_of):
        picked = jnp.where(lanes == lane_of, row, 0.0)
        return jnp.broadcast_to(jnp.sum(picked, axis=1, keepdims=True), (8, LANES))

    def element(vector, i):
        return jnp.broadcast_to(vector[i : i + 1], (8, LANES))

    def square_lanes(j):
        low, high = jnp.minimum(pairs, j), jnp.maximum(pairs, j)
        return SQUARES + low * PAIRS - ((low * (low - 1)) >> 1) + high - low

    by_change = [column(pairs * PAIRS + i) for i in range(PAIRS)]
    by_step = [column(pairs + PAIRS * i) for i in range(PAIRS)]
    squares = [column(square_lanes(i)) for i in range(PAIRS)]
    curvs = column(pairs * (PAIRS + 1))
    steps_part = column(pairs + STEPS_GRADIENT)
    changes_part = column(pairs + CHANGES_GRADIENT)
    inverse = 1.0 / curvs
    scaling = element(curvs, PAIRS - 1) / element(squares[PAIRS - 1], PAIRS - 1)
    alphas = [None] * PAIRS
    for i in reversed(range(PAIRS)):
        alphas[i] = element(inverse * steps_part, i)
        steps_part = steps_part - alphas[i] * by_change[i]
        changes_part = changes_part - alphas[i] * squares[i]
    changes_part = scaling * changes_part
    weights = [None] * PAIRS
    for i in range(PAIRS):
        weights[i] = alphas[i] - element(inverse * changes_part, i)
        changes_part = changes_part + weights[i] * by_step[i]
    change_weights = [scaling * alpha for alpha in alphas]
    for a, r, b in tiles(gradient_ref.shape):
        value = -(scaling * gradient_ref[a, r, b])
        for i in range(PAIRS):
            value = value + change_weights[i] * changes_ref[i, a, r, b]
            value = value - weights[i] * steps_ref[i, a, r, b]
        direction_ref[a, r, b] = value


def shifted(x, axis, shift):
    count = lax.axis_size(axis)
    return lax.ppermute(x, axis, [(i, (i + shift) % count) for i in range(count)])


def shards(kernels, steps, curvature):
    _, lons, rad_len, lats = kernels.shape
    rows = rad_len // 4
    block = ((lons, rows, lats), jnp.float32)
    size = lons * rows * lats
    keep, pass_on, send = call(
        radial_kernel,
        [block, block, ((2, lons, rows, lats), jnp.float32)],
        2 * 4 * rad_len * kernels.size,
        8 * kernels.size,
        in_specs=[pl.BlockSpec(memory_space=pltpu.HBM)],
        scratch_shapes=[
            pltpu.VMEM(kernels.shape[1:], jnp.float32),
            pltpu.SemaphoreType.DMA((lons,)),
        ],
    )(pltpu.with_memory_space_constraint(kernels, pltpu.HBM))
    near = shifted(send, "event_1", 1)
    far = shifted(pass_on + near[1], "event_0", 1)
    square = ((lats, lats), jnp.bfloat16)
    changes, gram, high, low = call(
        gram_kernel,
        [(steps.shape, jnp.float32), ((8, LANES), jnp.float32), square, square],
        2 * 100 * size,
        12 * steps.size,
    )(steps, curvature)
    side = ((RIM, rows, lats), jnp.float32)
    head, tail = call(latitude_kernel, [side, side], 2 * 4 * lats * size, 16 * size)(
        keep, near, far, high, low
    )
    left = shifted(tail, CUTS, 1)
    right = shifted(head, CUTS, -1)
    devices = lax.axis_size(CUTS_EVENT)
    gradient, kept, outgoing = call(
        product_kernel,
        [block, block, ((devices, 1, LANES), jnp.float32)],
        2 * 30 * size,
        4 * 20 * size,
    )(head, tail, left, right, steps, changes, gram)
    arrived = lax.all_to_all(outgoing, CUTS_EVENT, 0, 0, tiled=True)
    (direction,) = call(direction_kernel, [block], 2 * 17 * size, 4 * 18 * size)(
        arrived, kept, steps, changes
    )
    return (gradient, direction)


def solution(mesh):
    torus = Mesh(
        mesh.devices.reshape(2, 4, 4, 2, 2), ("cuts_0", "cuts_1", "cuts_2", "event_0", "event_1")
    )
    in_specs = (P(EVENT, CUTS, None, None), P(None, CUTS, EVENT, None), P(None, CUTS, EVENT, None))
    out_specs = (P(CUTS, EVENT, None), P(CUTS, EVENT, None))
    return jax.shard_map(
        shards, mesh=torus, in_specs=in_specs, out_specs=out_specs, check_vma=False
    )
```

```python
import functools
import math

import jax
import jax.numpy as jnp
import numpy as np
from jax import lax
from jax.experimental import pallas as pl
from jax.experimental.pallas import tpu as pltpu
from jax.sharding import Mesh
from jax.sharding import PartitionSpec as P

PAIRS = 8
RIM = 4
CUTS = ("cuts_0", "cuts_1", "cuts_2")
EVENT = ("event_0", "event_1")
CUTS_EVENT = ("cuts_0", "cuts_1", "cuts_2", "event_0", "event_1")
LANES = 128
SQUARES, STEPS_GRADIENT, CHANGES_GRADIENT = 64, 100, 108


def square_lane(i, j):
    low, high = min(i, j), max(i, j)
    return SQUARES + low * PAIRS - low * (low - 1) // 2 + high - low


def gauss_matrix(length, sigma):
    points = np.arange(length, dtype=np.float64)
    offset = points[:, None] - points[None, :]
    matrix = np.exp(-offset * offset / (2.0 * sigma * sigma))
    return (matrix / matrix.sum(axis=1, keepdims=True)).astype(np.float32)


def radial_table(length):
    matrix = gauss_matrix(length, 3.0)
    high = matrix.astype(jnp.bfloat16)
    low = (matrix - high.astype(np.float32)).astype(jnp.bfloat16)
    return np.stack([np.concatenate([m, m], axis=1) for m in (high, low)])


def cycle_weights():
    unscaled = [math.exp(-((column - RIM) ** 2) / 4.5) for column in range(2 * RIM + 1)]
    whole = sum(unscaled)
    return [weight / whole for weight in unscaled]


def split(x):
    high = x.astype(jnp.bfloat16)
    low = (x - high.astype(jnp.float32)).astype(jnp.bfloat16)
    return high, low


def dot(a, b):
    return jnp.dot(a, b, preferred_element_type=jnp.float32)


def call(kernel, outs, flops, moved, limit=16, **options):
    return pl.pallas_call(
        kernel,
        out_shape=[jax.ShapeDtypeStruct(*out) for out in outs],
        compiler_params=pltpu.CompilerParams(vmem_limit_bytes=limit << 20),
        cost_estimate=pl.CostEstimate(flops=flops, bytes_accessed=moved, transcendentals=0),
        **options,
    )


def gauss_rows(length, sigma, rows, axis):
    offset = (rows - lax.broadcasted_iota(jnp.int32, rows.shape, axis)).astype(jnp.float32)
    matrix = jnp.exp(-offset * offset / (2.0 * sigma * sigma))
    return matrix / jnp.sum(matrix, axis=axis, keepdims=True)


def radial_kernel(kernels_ref, table_ref, keep_ref, pass_ref, send_ref, held_ref, weights_ref, semaphores):
    _, lons, length, lats = kernels_ref.shape
    part = 2 * lax.axis_index("event_0") + lax.axis_index("event_1")
    rows = length // 4
    copies = []
    for half in range(2):
        for k, block in enumerate((part, part ^ 2, part ^ 1, part ^ 3)):
            at = pl.ds(pl.multiple_of(block * rows, rows), rows)
            copies.append(
                pltpu.make_async_copy(
                    table_ref.at[half, at],
                    weights_ref.at[pl.ds(half * length + k * rows, rows)],
                    semaphores.at[len(copies)],
                )
            )
    for a in range(lons):
        copies.append(
            pltpu.make_async_copy(kernels_ref.at[0, a], held_ref.at[a], semaphores.at[len(copies)])
        )
    for copy in copies:
        copy.start()
    for copy in copies[:8]:
        copy.wait()
    weights = weights_ref[...]
    for a in range(lons):
        copies[8 + a].wait()
        both = dot(weights, jnp.concatenate(split(held_ref[a]), axis=0))
        out = both[:length] + both[length:]
        keep_ref[a] = out[:rows]
        pass_ref[a] = out[rows : 2 * rows]
        send_ref[0, a] = out[2 * rows : 3 * rows]
        send_ref[1, a] = out[3 * rows :]


def latitude_kernel(keep_ref, near_ref, far_ref, high_ref, low_ref, tail_ref, head_ref):
    lons, rows, lats = keep_ref.shape
    summed = (keep_ref[...] + near_ref[0] + far_ref[...]).reshape(lons * rows, lats)
    both = jnp.concatenate(split(summed), axis=0)
    out = dot(both, high_ref[...]) + dot(both, low_ref[...])
    plane = (out[: lons * rows] + out[lons * rows :]).reshape(lons, rows, lats)
    head_ref[...] = plane[:RIM]
    tail_ref[...] = plane[lons - RIM :]


def lane_numbers():
    return lax.broadcasted_iota(jnp.int32, (8, LANES), 1)


def tiles(shape):
    return [
        (a, slice(8 * r, 8 * r + 8), slice(LANES * b, LANES * (b + 1)))
        for r in range(shape[1] // 8)
        for b in range(shape[2] // LANES)
        for a in range(shape[0])
    ]


def placed(sums):
    lanes = lane_numbers()
    row = jnp.zeros((8, LANES), jnp.float32)
    for lane, value in sums:
        row = row + jnp.where(lanes == lane, jnp.sum(value, axis=1, keepdims=True), 0.0)
    return row


def gram_kernel(steps_ref, curvature_ref, changes_ref, row_ref, high_ref, low_ref):
    lons, rows, lats = steps_ref.shape[1:]
    column = lax.broadcasted_iota(jnp.int32, (lats, lats), 1)
    high_ref[...], low_ref[...] = split(gauss_rows(lats, 4.0, column, 0))
    spots = [
        (slice(8 * r, 8 * r + 8), slice(LANES * b, LANES * (b + 1)))
        for r in range(rows // 8)
        for b in range(lats // LANES)
    ]
    half = PAIRS // 2
    upper = [(i, j) for i in range(PAIRS) for j in range(i, PAIRS)]

    def first(a, sums):
        for at in spots:
            steps = [steps_ref[(i, a, *at)] for i in range(half)]
            changes = [None] * PAIRS
            for i in range(PAIRS):
                step = steps[i] if i < half else steps_ref[(i, a, *at)]
                changes[i] = curvature_ref[(i, a, *at)] * step
                changes_ref[(i, a, *at)] = changes[i]
            sums = [sums[k] + steps[k // PAIRS] * changes[k % PAIRS] for k in range(half * PAIRS)]
        return sums

    def second(a, sums):
        for at in spots:
            steps = [steps_ref[(i, a, *at)] for i in range(half, PAIRS)]
            changes = [changes_ref[(i, a, *at)] for i in range(PAIRS)]
            sums = [sums[k] + steps[k // PAIRS] * changes[k % PAIRS] for k in range(half * PAIRS)]
        return sums

    def third(a, sums):
        for at in spots:
            changes = [changes_ref[(i, a, *at)] for i in range(PAIRS)]
            sums = [value + changes[i] * changes[j] for value, (i, j) in zip(sums, upper)]
        return sums

    zero = jnp.zeros((8, LANES), jnp.float32)
    row = zero
    for start, step, size in ((0, first, 32), (32, second, 32), (SQUARES, third, len(upper))):
        sums = lax.fori_loop(0, lons, step, [zero] * size)
        row = row + placed([(start + k, value) for k, value in enumerate(sums)])
    row_ref[...] = row


def product_kernel(head_ref, tail_ref, right_ref, left_ref, steps_ref, changes_ref, gram_ref, gradient_ref, kept_ref, rows_ref):
    lons, rows, lats = gradient_ref.shape
    weights = cycle_weights()
    sums = [jnp.zeros((8, LANES), jnp.float32) for _ in range(2 * PAIRS)]
    for r in range(rows // 8):
        for b in range(lats // LANES):
            at = (slice(8 * r, 8 * r + 8), slice(LANES * b, LANES * (b + 1)))
            padded = [ref[(a, *at)] for ref in (left_ref, head_ref, tail_ref, right_ref) for a in range(RIM)]
            for a in range(lons):
                value = weights[RIM] * padded[a + RIM]
                for k in range(RIM):
                    value = value + weights[k] * (padded[a + k] + padded[a + 2 * RIM - k])
                gradient_ref[(a, *at)] = value
                kept_ref[(a, *at)] = value
                for pair in range(PAIRS):
                    sums[pair] = sums[pair] + steps_ref[(pair, a, *at)] * value
                    sums[PAIRS + pair] = sums[PAIRS + pair] + changes_ref[(pair, a, *at)] * value
    row = gram_ref[...] + placed([(STEPS_GRADIENT + k, value) for k, value in enumerate(sums)])
    row = jnp.sum(row, axis=0, keepdims=True)
    rows_ref[...] = jnp.broadcast_to(row[None], rows_ref.shape)


def direction_kernel(rows_ref, gradient_ref, steps_ref, changes_ref, direction_ref):
    row = jnp.broadcast_to(jnp.sum(rows_ref[...], axis=0), (8, LANES))
    lanes = lane_numbers()
    pairs = lax.broadcasted_iota(jnp.int32, (8, LANES), 0)

    def column(lane_of):
        picked = jnp.where(lanes == lane_of, row, 0.0)
        return jnp.broadcast_to(jnp.sum(picked, axis=1, keepdims=True), (8, LANES))

    def element(vector, i):
        return jnp.broadcast_to(vector[i : i + 1], (8, LANES))

    def square_lanes(j):
        low, high = jnp.minimum(pairs, j), jnp.maximum(pairs, j)
        return SQUARES + low * PAIRS - ((low * (low - 1)) >> 1) + high - low

    by_change = [column(pairs * PAIRS + i) for i in range(PAIRS)]
    by_step = [column(pairs + PAIRS * i) for i in range(PAIRS)]
    squares = [column(square_lanes(i)) for i in range(PAIRS)]
    curvs = column(pairs * (PAIRS + 1))
    steps_part = column(pairs + STEPS_GRADIENT)
    changes_part = column(pairs + CHANGES_GRADIENT)
    inverse = 1.0 / curvs
    scaling = element(curvs, PAIRS - 1) / element(squares[PAIRS - 1], PAIRS - 1)
    alphas = [None] * PAIRS
    for i in reversed(range(PAIRS)):
        alphas[i] = element(inverse * steps_part, i)
        steps_part = steps_part - alphas[i] * by_change[i]
        changes_part = changes_part - alphas[i] * squares[i]
    changes_part = scaling * changes_part
    weights = [None] * PAIRS
    for i in range(PAIRS):
        weights[i] = alphas[i] - element(inverse * changes_part, i)
        changes_part = changes_part + weights[i] * by_step[i]
    change_weights = [scaling * alpha for alpha in alphas]
    for a, r, b in tiles(gradient_ref.shape):
        value = -(scaling * gradient_ref[a, r, b])
        for i in range(PAIRS):
            value = value + change_weights[i] * changes_ref[i, a, r, b]
            value = value - weights[i] * steps_ref[i, a, r, b]
        direction_ref[a, r, b] = value


def in_hbm(x):
    return pltpu.with_memory_space_constraint(x, pltpu.HBM)


def shifted(x, axis, shift):
    count = lax.axis_size(axis)
    return lax.ppermute(x, axis, [(i, (i + shift) % count) for i in range(count)])


def shards(kernels, steps, curvature):
    _, lons, rad_len, lats = kernels.shape
    rows = rad_len // 4
    block = ((lons, rows, lats), jnp.float32)
    size = lons * rows * lats
    keep, pass_on, send = call(
        radial_kernel,
        [block, block, ((2, lons, rows, lats), jnp.float32)],
        2 * 4 * rad_len * kernels.size,
        8 * kernels.size,
        in_specs=[pl.BlockSpec(memory_space=pltpu.HBM)] * 2,
        scratch_shapes=[
            pltpu.VMEM(kernels.shape[1:], jnp.float32),
            pltpu.VMEM((2 * rad_len, 2 * rad_len), jnp.bfloat16),
            pltpu.SemaphoreType.DMA((8 + lons,)),
        ],
    )(in_hbm(kernels), in_hbm(jnp.asarray(radial_table(rad_len))))
    near = shifted(send, "event_1", 1)
    far = shifted(pass_on + near[1], "event_0", 1)
    square = ((lats, lats), jnp.bfloat16)
    changes, gram, high, low = call(
        gram_kernel,
        [(steps.shape, jnp.float32), ((8, LANES), jnp.float32), square, square],
        2 * 100 * size,
        12 * steps.size,
    )(steps, curvature)
    side = ((RIM, rows, lats), jnp.float32)
    tail, head = call(latitude_kernel, [side, side], 2 * 4 * lats * size, 16 * size)(
        keep, near, far, high, low
    )
    left = shifted(tail, CUTS, 1)
    right = shifted(head, CUTS, -1)
    devices = lax.axis_size(CUTS_EVENT)
    gradient, kept, outgoing = call(
        product_kernel,
        [block, block, ((devices, 1, LANES), jnp.float32)],
        2 * 30 * size,
        4 * 20 * size,
    )(head, tail, right, left, steps, changes, gram)
    arrived = lax.all_to_all(outgoing, CUTS_EVENT, 0, 0, tiled=True)
    (direction,) = call(direction_kernel, [block], 2 * 17 * size, 4 * 18 * size)(
        arrived, kept, steps, changes
    )
    return (gradient, direction)


def solution(mesh):
    torus = Mesh(
        mesh.devices.reshape(2, 4, 4, 2, 2), ("cuts_0", "cuts_1", "cuts_2", "event_0", "event_1")
    )
    in_specs = (P(EVENT, CUTS, None, None), P(None, CUTS, EVENT, None), P(None, CUTS, EVENT, None))
    out_specs = (P(CUTS, EVENT, None), P(CUTS, EVENT, None))
    return jax.shard_map(
        shards, mesh=torus, in_specs=in_specs, out_specs=out_specs, check_vma=False
    )
```

```python
import math

import jax
import jax.numpy as jnp
import numpy as np
from jax import lax
from jax.experimental import pallas as pl
from jax.experimental.pallas import tpu as pltpu
from jax.sharding import Mesh
from jax.sharding import PartitionSpec as P

PAIRS = 8
RIM = 4
CUTS = ("cuts_0", "cuts_1", "cuts_2")
EVENT = ("event_0", "event_1")
CUTS_EVENT = ("cuts_0", "cuts_1", "cuts_2", "event_0", "event_1")
LANES = 128
SQUARES, STEPS_GRADIENT, CHANGES_GRADIENT = 64, 100, 108


def gauss_matrix(length, sigma):
    points = np.arange(length, dtype=np.float64)
    offset = points[:, None] - points[None, :]
    matrix = np.exp(-offset * offset / (2.0 * sigma * sigma))
    return (matrix / matrix.sum(axis=1, keepdims=True)).astype(np.float32)


def radial_table(length):
    matrix = gauss_matrix(length, 3.0)
    high = matrix.astype(jnp.bfloat16)
    low = (matrix - high.astype(np.float32)).astype(jnp.bfloat16)
    return np.stack([np.concatenate([m, m], axis=1) for m in (high, low)])


def cycle_weights():
    unscaled = [math.exp(-((column - RIM) ** 2) / 4.5) for column in range(2 * RIM + 1)]
    whole = sum(unscaled)
    return [weight / whole for weight in unscaled]


def split(x):
    high = x.astype(jnp.bfloat16)
    low = (x - high.astype(jnp.float32)).astype(jnp.bfloat16)
    return high, low


def dot(a, b):
    return jnp.dot(a, b, preferred_element_type=jnp.float32)


def call(kernel, outs, flops, moved, limit=16, **options):
    return pl.pallas_call(
        kernel,
        out_shape=[jax.ShapeDtypeStruct(*out) for out in outs],
        compiler_params=pltpu.CompilerParams(vmem_limit_bytes=limit << 20),
        cost_estimate=pl.CostEstimate(flops=flops, bytes_accessed=moved, transcendentals=0),
        **options,
    )


def gauss_rows(sigma, rows, axis):
    offset = (rows - lax.broadcasted_iota(jnp.int32, rows.shape, axis)).astype(jnp.float32)
    matrix = jnp.exp(-offset * offset / (2.0 * sigma * sigma))
    return matrix / jnp.sum(matrix, axis=axis, keepdims=True)


def radial_kernel(kernels_ref, table_ref, keep_ref, pass_ref, send_ref, held_ref, weights_ref, semaphores):
    _, lons, length, _ = kernels_ref.shape
    part = 2 * lax.axis_index("event_0") + lax.axis_index("event_1")
    rows = length // 4
    copies = []
    for half in range(2):
        for k, block in enumerate((part, part ^ 2, part ^ 1, part ^ 3)):
            at = pl.ds(pl.multiple_of(block * rows, rows), rows)
            copies.append(
                pltpu.make_async_copy(
                    table_ref.at[half, at],
                    weights_ref.at[pl.ds(half * length + k * rows, rows)],
                    semaphores.at[len(copies)],
                )
            )
    half = lons // 2
    for part in range(2):
        at = slice(part * half, part * half + half)
        copies.append(
            pltpu.make_async_copy(kernels_ref.at[0, at], held_ref.at[at], semaphores.at[len(copies)])
        )
    for copy in copies:
        copy.start()
    for copy in copies[:8]:
        copy.wait()
    for part in range(2):
        copies[8 + part].wait()
        weights = weights_ref[...]
        for a in range(part * half, part * half + half):
            both = dot(weights, jnp.concatenate(split(held_ref[a]), axis=0))
            out = both[:length] + both[length:]
            keep_ref[a] = out[:rows]
            pass_ref[a] = out[rows : 2 * rows]
            send_ref[0, a] = out[2 * rows : 3 * rows]
            send_ref[1, a] = out[3 * rows :]


def latitude_kernel(keep_ref, near_ref, far_ref, high_ref, low_ref, tail_ref, head_ref):
    lons, rows, lats = keep_ref.shape
    summed = (keep_ref[...] + near_ref[0] + far_ref[...]).reshape(lons * rows, lats)
    both = jnp.concatenate(split(summed), axis=0)
    out = dot(both, high_ref[...]) + dot(both, low_ref[...])
    plane = (out[: lons * rows] + out[lons * rows :]).reshape(lons, rows, lats)
    head_ref[...] = plane[:RIM]
    tail_ref[...] = plane[lons - RIM :]


def lane_numbers():
    return lax.broadcasted_iota(jnp.int32, (8, LANES), 1)


def tiles(shape):
    return [
        (a, slice(8 * r, 8 * r + 8), slice(LANES * b, LANES * (b + 1)))
        for r in range(shape[1] // 8)
        for b in range(shape[2] // LANES)
        for a in range(shape[0])
    ]


def placed(sums):
    lanes = lane_numbers()
    row = jnp.zeros((8, LANES), jnp.float32)
    for lane, value in sums:
        row = row + jnp.where(lanes == lane, jnp.sum(value, axis=1, keepdims=True), 0.0)
    return row


def gram_kernel(steps_ref, curvature_ref, changes_ref, row_ref, high_ref, low_ref):
    lons, rows, lats = steps_ref.shape[1:]
    column = lax.broadcasted_iota(jnp.int32, (lats, lats), 1)
    high_ref[...], low_ref[...] = split(gauss_rows(4.0, column, 0))
    spots = [
        (slice(8 * r, 8 * r + 8), slice(LANES * b, LANES * (b + 1)))
        for r in range(rows // 8)
        for b in range(lats // LANES)
    ]
    half = PAIRS // 2
    upper = [(i, j) for i in range(PAIRS) for j in range(i, PAIRS)]

    def first(a, sums):
        for at in spots:
            steps = [steps_ref[(i, a, *at)] for i in range(half)]
            changes = [None] * PAIRS
            for i in range(PAIRS):
                step = steps[i] if i < half else steps_ref[(i, a, *at)]
                changes[i] = curvature_ref[(i, a, *at)] * step
                changes_ref[(i, a, *at)] = changes[i]
            sums = [sums[k] + steps[k // PAIRS] * changes[k % PAIRS] for k in range(half * PAIRS)]
        return sums

    def second(a, sums):
        for at in spots:
            steps = [steps_ref[(i, a, *at)] for i in range(half, PAIRS)]
            changes = [changes_ref[(i, a, *at)] for i in range(PAIRS)]
            sums = [sums[k] + steps[k // PAIRS] * changes[k % PAIRS] for k in range(half * PAIRS)]
        return sums

    def third(a, sums):
        for at in spots:
            changes = [changes_ref[(i, a, *at)] for i in range(PAIRS)]
            sums = [value + changes[i] * changes[j] for value, (i, j) in zip(sums, upper)]
        return sums

    zero = jnp.zeros((8, LANES), jnp.float32)
    row = zero
    for start, step, size in ((0, first, 32), (32, second, 32), (SQUARES, third, len(upper))):
        sums = lax.fori_loop(0, lons, step, [zero] * size)
        row = row + placed([(start + k, value) for k, value in enumerate(sums)])
    row_ref[...] = row


def product_kernel(head_ref, tail_ref, right_ref, left_ref, steps_ref, changes_ref, gram_ref, gradient_ref, kept_ref, rows_ref):
    lons, rows, lats = gradient_ref.shape
    weights = cycle_weights()
    sums = [jnp.zeros((8, LANES), jnp.float32) for _ in range(2 * PAIRS)]
    for r in range(rows // 8):
        for b in range(lats // LANES):
            at = (slice(8 * r, 8 * r + 8), slice(LANES * b, LANES * (b + 1)))
            padded = [ref[(a, *at)] for ref in (left_ref, head_ref, tail_ref, right_ref) for a in range(RIM)]
            for a in range(lons):
                value = weights[RIM] * padded[a + RIM]
                for k in range(RIM):
                    value = value + weights[k] * (padded[a + k] + padded[a + 2 * RIM - k])
                gradient_ref[(a, *at)] = value
                kept_ref[(a, *at)] = value
                for pair in range(PAIRS):
                    sums[pair] = sums[pair] + steps_ref[(pair, a, *at)] * value
                    sums[PAIRS + pair] = sums[PAIRS + pair] + changes_ref[(pair, a, *at)] * value
    row = gram_ref[...] + placed([(STEPS_GRADIENT + k, value) for k, value in enumerate(sums)])
    row = jnp.sum(row, axis=0, keepdims=True)
    rows_ref[...] = jnp.broadcast_to(row[None], rows_ref.shape)


def direction_kernel(rows_ref, gradient_ref, steps_ref, changes_ref, direction_ref):
    row = jnp.broadcast_to(jnp.sum(rows_ref[...], axis=0), (8, LANES))
    lanes = lane_numbers()
    pairs = lax.broadcasted_iota(jnp.int32, (8, LANES), 0)

    def column(lane_of):
        picked = jnp.where(lanes == lane_of, row, 0.0)
        return jnp.broadcast_to(jnp.sum(picked, axis=1, keepdims=True), (8, LANES))

    def element(vector, i):
        return jnp.broadcast_to(vector[i : i + 1], (8, LANES))

    def square_lanes(j):
        low, high = jnp.minimum(pairs, j), jnp.maximum(pairs, j)
        return SQUARES + low * PAIRS - ((low * (low - 1)) >> 1) + high - low

    by_change = [column(pairs * PAIRS + i) for i in range(PAIRS)]
    by_step = [column(pairs + PAIRS * i) for i in range(PAIRS)]
    squares = [column(square_lanes(i)) for i in range(PAIRS)]
    curvs = column(pairs * (PAIRS + 1))
    steps_part = column(pairs + STEPS_GRADIENT)
    changes_part = column(pairs + CHANGES_GRADIENT)
    inverse = 1.0 / curvs
    scaling = element(curvs, PAIRS - 1) / element(squares[PAIRS - 1], PAIRS - 1)
    alphas = [None] * PAIRS
    for i in reversed(range(PAIRS)):
        alphas[i] = element(inverse * steps_part, i)
        steps_part = steps_part - alphas[i] * by_change[i]
        changes_part = changes_part - alphas[i] * squares[i]
    changes_part = scaling * changes_part
    weights = [None] * PAIRS
    for i in range(PAIRS):
        weights[i] = alphas[i] - element(inverse * changes_part, i)
        changes_part = changes_part + weights[i] * by_step[i]
    change_weights = [scaling * alpha for alpha in alphas]
    for a, r, b in tiles(gradient_ref.shape):
        value = -(scaling * gradient_ref[a, r, b])
        for i in range(PAIRS):
            value = value + change_weights[i] * changes_ref[i, a, r, b]
            value = value - weights[i] * steps_ref[i, a, r, b]
        direction_ref[a, r, b] = value


def in_hbm(x):
    return pltpu.with_memory_space_constraint(x, pltpu.HBM)


def shifted(x, axis, shift):
    count = lax.axis_size(axis)
    return lax.ppermute(x, axis, [(i, (i + shift) % count) for i in range(count)])


def shards(kernels, steps, curvature):
    _, lons, rad_len, lats = kernels.shape
    rows = rad_len // 4
    block = ((lons, rows, lats), jnp.float32)
    size = lons * rows * lats
    keep, pass_on, send = call(
        radial_kernel,
        [block, block, ((2, lons, rows, lats), jnp.float32)],
        2 * 4 * rad_len * kernels.size,
        8 * kernels.size,
        in_specs=[pl.BlockSpec(memory_space=pltpu.HBM)] * 2,
        scratch_shapes=[
            pltpu.VMEM(kernels.shape[1:], jnp.float32),
            pltpu.VMEM((2 * rad_len, 2 * rad_len), jnp.bfloat16),
            pltpu.SemaphoreType.DMA((10,)),
        ],
    )(in_hbm(kernels), in_hbm(jnp.asarray(radial_table(rad_len))))
    near = shifted(send, "event_1", 1)
    far = shifted(pass_on + near[1], "event_0", 1)
    square = ((lats, lats), jnp.bfloat16)
    changes, gram, high, low = call(
        gram_kernel,
        [(steps.shape, jnp.float32), ((8, LANES), jnp.float32), square, square],
        2 * 100 * size,
        12 * steps.size,
    )(steps, curvature)
    side = ((RIM, rows, lats), jnp.float32)
    tail, head = call(latitude_kernel, [side, side], 2 * 4 * lats * size, 16 * size)(
        keep, near, far, high, low
    )
    left = shifted(tail, CUTS, 1)
    right = shifted(head, CUTS, -1)
    devices = lax.axis_size(CUTS_EVENT)
    gradient, kept, outgoing = call(
        product_kernel,
        [block, block, ((devices, 1, LANES), jnp.float32)],
        2 * 30 * size,
        4 * 20 * size,
    )(head, tail, right, left, steps, changes, gram)
    arrived = lax.all_to_all(outgoing, CUTS_EVENT, 0, 0, tiled=True)
    (direction,) = call(direction_kernel, [block], 2 * 17 * size, 4 * 18 * size)(
        arrived, kept, steps, changes
    )
    return (gradient, direction)


def solution(mesh):
    torus = Mesh(
        mesh.devices.reshape(2, 4, 4, 2, 2), ("cuts_0", "cuts_1", "cuts_2", "event_0", "event_1")
    )
    in_specs = (P(EVENT, CUTS, None, None), P(None, CUTS, EVENT, None), P(None, CUTS, EVENT, None))
    out_specs = (P(CUTS, EVENT, None), P(CUTS, EVENT, None))
    return jax.shard_map(
        shards, mesh=torus, in_specs=in_specs, out_specs=out_specs, check_vma=False
    )
```

```python
import math

import jax
import jax.numpy as jnp
from jax import lax
from jax.experimental import pallas as pl
from jax.experimental.pallas import tpu as pltpu
from jax.sharding import Mesh
from jax.sharding import PartitionSpec as P

PAIRS = 8
RIM = 4
CUTS = ("cuts_0", "cuts_1", "cuts_2")
EVENT = ("event_0", "event_1")
CUTS_EVENT = ("cuts_0", "cuts_1", "cuts_2", "event_0", "event_1")
LANES = 128
SQUARES, STEPS_GRADIENT, CHANGES_GRADIENT = 64, 100, 108


def cycle_weights():
    unscaled = [math.exp(-((column - RIM) ** 2) / 4.5) for column in range(2 * RIM + 1)]
    whole = sum(unscaled)
    return [weight / whole for weight in unscaled]


def split(x):
    high = x.astype(jnp.bfloat16)
    low = (x - high.astype(jnp.float32)).astype(jnp.bfloat16)
    return high, low


def dot(a, b):
    return jnp.dot(a, b, preferred_element_type=jnp.float32)


def call(kernel, outs, flops, moved, limit=16, **options):
    return pl.pallas_call(
        kernel,
        out_shape=[jax.ShapeDtypeStruct(*out) for out in outs],
        compiler_params=pltpu.CompilerParams(vmem_limit_bytes=limit << 20),
        cost_estimate=pl.CostEstimate(flops=flops, bytes_accessed=moved, transcendentals=0),
        **options,
    )


def gauss_rows(length, sigma, rows, axis):
    offset = (rows - lax.broadcasted_iota(jnp.int32, rows.shape, axis)).astype(jnp.float32)
    matrix = jnp.exp(-offset * offset / (2.0 * sigma * sigma))
    return matrix / jnp.sum(matrix, axis=axis, keepdims=True)


def gauss_rows(length, sigma, rows, axis):
    offset = (rows - lax.broadcasted_iota(jnp.int32, rows.shape, axis)).astype(jnp.float32)
    matrix = jnp.exp(-offset * offset / (2.0 * sigma * sigma))
    return matrix / jnp.sum(matrix, axis=axis, keepdims=True)


def radial_kernel(kernels_ref, keep_ref, pass_ref, send_keep_ref, send_pass_ref, held_ref, semaphores):
    _, lons, length, _ = kernels_ref.shape
    half = lons // 2
    copies = []
    for piece in range(2):
        at = slice(piece * half, piece * half + half)
        copies.append(
            pltpu.make_async_copy(kernels_ref.at[0, at], held_ref.at[at], semaphores.at[piece])
        )
        copies[piece].start()
    part = 2 * lax.axis_index("event_0") + lax.axis_index("event_1")
    rows = length // 4
    local = lax.broadcasted_iota(jnp.int32, (rows, length), 0)
    order = [part, part ^ 2, part ^ 1, part ^ 3]
    matrix = jnp.concatenate(
        [gauss_rows(length, 3.0, local + rows * block, 1) for block in order], axis=0
    )
    weights = jnp.concatenate([jnp.concatenate([m, m], axis=1) for m in split(matrix)], axis=0)
    outs = (keep_ref, pass_ref, send_keep_ref, send_pass_ref)
    for piece in range(2):
        copies[piece].wait()
        for a in range(piece * half, piece * half + half):
            both = dot(weights, jnp.concatenate(split(held_ref[a]), axis=0))
            out = both[:length] + both[length:]
            for k, ref in enumerate(outs):
                ref[a] = out[k * rows : (k + 1) * rows]


def smoothed(field, high, low):
    count = field.shape[0]
    both = jnp.concatenate(split(field), axis=0)
    out = dot(both, high) + dot(both, low)
    return out[:count] + out[count:]


def fetch_kernel(curvature_ref, held_ref, high_ref, low_ref, semaphore):
    copy = pltpu.make_async_copy(curvature_ref, held_ref, semaphore)
    copy.start()
    lats = high_ref.shape[0]
    column = lax.broadcasted_iota(jnp.int32, (lats, lats), 1)
    high_ref[...], low_ref[...] = split(gauss_rows(lats, 4.0, column, 0))
    copy.wait()


def latitude_kernel(keep_ref, near_ref, far_ref, high_ref, low_ref, tail_ref, head_ref):
    lons, rows, lats = keep_ref.shape
    summed = (keep_ref[...] + near_ref[...] + far_ref[...]).reshape(lons * rows, lats)
    plane = smoothed(summed, high_ref[...], low_ref[...]).reshape(lons, rows, lats)
    head_ref[...] = plane[:RIM]
    tail_ref[...] = plane[lons - RIM :]


def lane_numbers():
    return lax.broadcasted_iota(jnp.int32, (8, LANES), 1)


def tiles(shape):
    return [
        (a, slice(8 * r, 8 * r + 8), slice(LANES * b, LANES * (b + 1)))
        for r in range(shape[1] // 8)
        for b in range(shape[2] // LANES)
        for a in range(shape[0])
    ]


def placed(sums):
    lanes = lane_numbers()
    row = jnp.zeros((8, LANES), jnp.float32)
    for lane, value in sums:
        row = row + jnp.where(lanes == lane, jnp.sum(value, axis=1, keepdims=True), 0.0)
    return row


def gram_kernel(steps_ref, curvature_ref, changes_ref, row_ref):
    lons, rows, lats = steps_ref.shape[1:]
    spots = [
        (slice(8 * r, 8 * r + 8), slice(LANES * b, LANES * (b + 1)))
        for r in range(rows // 8)
        for b in range(lats // LANES)
    ]
    half = PAIRS // 2
    upper = [(i, j) for i in range(PAIRS) for j in range(i, PAIRS)]

    def first(a, sums):
        for at in spots:
            steps = [steps_ref[(i, a, *at)] for i in range(half)]
            changes = [None] * PAIRS
            for i in range(PAIRS):
                step = steps[i] if i < half else steps_ref[(i, a, *at)]
                changes[i] = curvature_ref[(i, a, *at)] * step
                changes_ref[(i, a, *at)] = changes[i]
            sums = [sums[k] + steps[k // PAIRS] * changes[k % PAIRS] for k in range(half * PAIRS)]
        return sums

    def second(a, sums):
        for at in spots:
            steps = [steps_ref[(i, a, *at)] for i in range(half, PAIRS)]
            changes = [changes_ref[(i, a, *at)] for i in range(PAIRS)]
            sums = [sums[k] + steps[k // PAIRS] * changes[k % PAIRS] for k in range(half * PAIRS)]
        return sums

    def third(a, sums):
        for at in spots:
            changes = [changes_ref[(i, a, *at)] for i in range(PAIRS)]
            sums = [value + changes[i] * changes[j] for value, (i, j) in zip(sums, upper)]
        return sums

    zero = jnp.zeros((8, LANES), jnp.float32)
    row = zero
    for start, step, size in ((0, first, 32), (32, second, 32), (SQUARES, third, len(upper))):
        sums = lax.fori_loop(0, lons, step, [zero] * size)
        row = row + placed([(start + k, value) for k, value in enumerate(sums)])
    row_ref[...] = row


def product_kernel(
    head_ref, tail_ref, left_ref, wrap_left_ref, right_ref, wrap_own_ref, wrap_other_ref,
    high_ref, low_ref, steps_ref, changes_ref, gram_ref, gradient_ref, rows_ref, right_scratch,
):
    lons, rows, lats = gradient_ref.shape
    weights = cycle_weights()
    cut = cut_number()
    last = lax.axis_size(CUTS) - 1

    @pl.when(cut == last)
    def _():
        summed = (wrap_own_ref[...] + wrap_other_ref[...]).reshape(RIM * rows, lats)
        plane = smoothed(summed, high_ref[...], low_ref[...])
        right_scratch[...] = plane.reshape(RIM, rows, lats)

    @pl.when(cut != last)
    def _():
        right_scratch[...] = right_ref[...]

    sums = [jnp.zeros((8, LANES), jnp.float32) for _ in range(2 * PAIRS)]
    for r in range(rows // 8):
        for b in range(lats // LANES):
            at = (slice(8 * r, 8 * r + 8), slice(LANES * b, LANES * (b + 1)))
            padded = [left_ref[(a, *at)] + wrap_left_ref[(a, *at)] for a in range(RIM)]
            padded += [ref[(a, *at)] for ref in (head_ref, tail_ref, right_scratch) for a in range(RIM)]
            for a in range(lons):
                value = weights[RIM] * padded[a + RIM]
                for k in range(RIM):
                    value = value + weights[k] * (padded[a + k] + padded[a + 2 * RIM - k])
                gradient_ref[(a, *at)] = value
                for pair in range(PAIRS):
                    sums[pair] = sums[pair] + steps_ref[(pair, a, *at)] * value
                    sums[PAIRS + pair] = sums[PAIRS + pair] + changes_ref[(pair, a, *at)] * value
    row = gram_ref[...] + placed([(STEPS_GRADIENT + k, value) for k, value in enumerate(sums)])
    row = jnp.sum(row, axis=0, keepdims=True)
    rows_ref[...] = jnp.broadcast_to(row[None], rows_ref.shape)


def direction_kernel(
    rows_ref, gradient_ref, steps_ref, changes_ref, gradient_out, direction_out, direction_ref, semaphores
):
    written = pltpu.make_async_copy(gradient_ref, gradient_out, semaphores.at[0])
    written.start()
    row = jnp.broadcast_to(jnp.sum(rows_ref[...], axis=0), (8, LANES))
    lanes = lane_numbers()
    pairs = lax.broadcasted_iota(jnp.int32, (8, LANES), 0)

    def column(lane_of):
        picked = jnp.where(lanes == lane_of, row, 0.0)
        return jnp.broadcast_to(jnp.sum(picked, axis=1, keepdims=True), (8, LANES))

    def element(vector, i):
        return jnp.broadcast_to(vector[i : i + 1], (8, LANES))

    def square_lanes(j):
        low, high = jnp.minimum(pairs, j), jnp.maximum(pairs, j)
        return SQUARES + low * PAIRS - ((low * (low - 1)) >> 1) + high - low

    by_change = [column(pairs * PAIRS + i) for i in range(PAIRS)]
    by_step = [column(pairs + PAIRS * i) for i in range(PAIRS)]
    squares = [column(square_lanes(i)) for i in range(PAIRS)]
    curvs = column(pairs * (PAIRS + 1))
    steps_part = column(pairs + STEPS_GRADIENT)
    changes_part = column(pairs + CHANGES_GRADIENT)
    inverse = 1.0 / curvs
    scaling = element(curvs, PAIRS - 1) / element(squares[PAIRS - 1], PAIRS - 1)
    alphas = [None] * PAIRS
    for i in reversed(range(PAIRS)):
        alphas[i] = element(inverse * steps_part, i)
        steps_part = steps_part - alphas[i] * by_change[i]
        changes_part = changes_part - alphas[i] * squares[i]
    changes_part = scaling * changes_part
    weights = [None] * PAIRS
    for i in range(PAIRS):
        weights[i] = alphas[i] - element(inverse * changes_part, i)
        changes_part = changes_part + weights[i] * by_step[i]
    change_weights = [scaling * alpha for alpha in alphas]
    copies = []
    lons, pieces = gradient_ref.shape[0], 4
    for piece in range(pieces):
        at = slice(piece * lons // pieces, (piece + 1) * lons // pieces)
        for a, r, b in tiles(gradient_ref.shape):
            if at.start <= a < at.stop:
                value = -(scaling * gradient_ref[a, r, b])
                for i in range(PAIRS):
                    value = value + change_weights[i] * changes_ref[i, a, r, b]
                    value = value - weights[i] * steps_ref[i, a, r, b]
                direction_ref[a, r, b] = value
        if copies:
            copies[-1].start()
        copies.append(
            pltpu.make_async_copy(
                direction_ref.at[at], direction_out.at[at], semaphores.at[1 + piece]
            )
        )
    copies[-1].start()
    for copy in copies:
        copy.wait()
    written.wait()


def in_hbm(x):
    return pltpu.with_memory_space_constraint(x, pltpu.HBM)


def shifted(x, axis, shift):
    count = lax.axis_size(axis)
    return lax.ppermute(x, axis, [(i, i + shift) for i in range(count) if 0 <= i + shift < count])


def swapped(x, axis):
    return lax.ppermute(x, axis, [(0, 1), (1, 0)])


def cut_number():
    number = 0
    for axis in CUTS:
        number = number * lax.axis_size(axis) + lax.axis_index(axis)
    return number


def shards(kernels, steps, curvature):
    _, lons, rad_len, lats = kernels.shape
    rows = rad_len // 4
    block = ((lons, rows, lats), jnp.float32)
    size = lons * rows * lats
    keep, pass_on, send_keep, send_pass = call(
        radial_kernel,
        [block] * 4,
        2 * 4 * rad_len * kernels.size,
        8 * kernels.size,
        in_specs=[pl.BlockSpec(memory_space=pltpu.HBM)],
        scratch_shapes=[pltpu.VMEM(kernels.shape[1:], jnp.float32), pltpu.SemaphoreType.DMA((2,))],
    )(in_hbm(kernels))
    near_pass = swapped(send_pass, "event_1")
    passed = pass_on + near_pass
    far = swapped(passed, "event_0")
    near_keep = swapped(send_keep, "event_1")
    square = ((lats, lats), jnp.bfloat16)
    held_curvature, high, low = call(
        fetch_kernel,
        [(curvature.shape, jnp.float32), square, square],
        10 * lats * lats,
        8 * curvature.size,
        in_specs=[pl.BlockSpec(memory_space=pltpu.HBM)],
        scratch_shapes=[pltpu.SemaphoreType.DMA],
    )(in_hbm(curvature))
    cuts, last = lax.axis_size(CUTS), lax.axis_size(CUTS) - 1
    events = lax.axis_size(EVENT)
    wrap_other = lax.ppermute(
        passed[:RIM], CUTS_EVENT, [(e, last * events + (e ^ 2)) for e in range(events)]
    )
    wrap_own = lax.ppermute(keep[:RIM] + near_keep[:RIM], CUTS, [(0, last)])
    side = ((RIM, rows, lats), jnp.float32)
    tail, head = call(latitude_kernel, [side, side], 2 * 4 * lats * size, 16 * size)(
        keep, near_keep, far, high, low
    )
    left = shifted(tail, CUTS, 1)
    right = shifted(head, CUTS, -1)
    wrap_left = lax.ppermute(tail, CUTS, [(last, 0)])
    changes, gram = call(
        gram_kernel,
        [(steps.shape, jnp.float32), ((8, LANES), jnp.float32)],
        2 * 100 * size,
        12 * steps.size,
    )(steps, held_curvature)
    gradient, outgoing = call(
        product_kernel,
        [block, ((cuts * events, 1, LANES), jnp.float32)],
        2 * 30 * size,
        4 * 20 * size,
        scratch_shapes=[pltpu.VMEM((RIM, rows, lats), jnp.float32)],
    )(head, tail, left, wrap_left, right, wrap_own, wrap_other, high, low, steps, changes, gram)
    arrived = lax.all_to_all(outgoing, CUTS_EVENT, 0, 0, tiled=True)
    return call(
        direction_kernel,
        [block] * 2,
        2 * 17 * size,
        4 * 18 * size,
        out_specs=[pl.BlockSpec(memory_space=pltpu.HBM)] * 2,
        scratch_shapes=[pltpu.VMEM((lons, rows, lats), jnp.float32), pltpu.SemaphoreType.DMA((5,))],
    )(arrived, gradient, steps, changes)


def solution(mesh):
    torus = Mesh(
        mesh.devices.reshape(2, 4, 4, 2, 2), ("cuts_0", "cuts_1", "cuts_2", "event_0", "event_1")
    )
    in_specs = (P(EVENT, CUTS, None, None), P(None, CUTS, EVENT, None), P(None, CUTS, EVENT, None))
    out_specs = (P(CUTS, EVENT, None), P(CUTS, EVENT, None))
    return jax.shard_map(
        shards, mesh=torus, in_specs=in_specs, out_specs=out_specs, check_vma=False
    )
```

```python
import math

import jax
import jax.numpy as jnp
from jax import lax
from jax.experimental import pallas as pl
from jax.experimental.pallas import tpu as pltpu
from jax.sharding import Mesh
from jax.sharding import PartitionSpec as P

PAIRS = 8
RIM = 4
CUTS = ("cuts_0", "cuts_1", "cuts_2")
EVENT = ("event_0", "event_1")
CUTS_EVENT = ("cuts_0", "cuts_1", "cuts_2", "event_0", "event_1")
LANES = 128
SQUARES, STEPS_GRADIENT, CHANGES_GRADIENT = 64, 100, 108


def cycle_weights():
    unscaled = [math.exp(-((column - RIM) ** 2) / 4.5) for column in range(2 * RIM + 1)]
    whole = sum(unscaled)
    return [weight / whole for weight in unscaled]


def split(x):
    high = x.astype(jnp.bfloat16)
    low = (x - high.astype(jnp.float32)).astype(jnp.bfloat16)
    return high, low


def dot(a, b):
    return jnp.dot(a, b, preferred_element_type=jnp.float32)


def call(kernel, outs, flops, moved, limit=16, **options):
    return pl.pallas_call(
        kernel,
        out_shape=[jax.ShapeDtypeStruct(*out) for out in outs],
        compiler_params=pltpu.CompilerParams(vmem_limit_bytes=limit << 20),
        cost_estimate=pl.CostEstimate(flops=flops, bytes_accessed=moved, transcendentals=0),
        **options,
    )


def gauss_rows(length, sigma, rows, axis):
    offset = (rows - lax.broadcasted_iota(jnp.int32, rows.shape, axis)).astype(jnp.float32)
    matrix = jnp.exp(-offset * offset / (2.0 * sigma * sigma))
    return matrix / jnp.sum(matrix, axis=axis, keepdims=True)


def gauss_rows(length, sigma, rows, axis):
    offset = (rows - lax.broadcasted_iota(jnp.int32, rows.shape, axis)).astype(jnp.float32)
    matrix = jnp.exp(-offset * offset / (2.0 * sigma * sigma))
    return matrix / jnp.sum(matrix, axis=axis, keepdims=True)


def radial_kernel(kernels_ref, keep_ref, pass_ref, send_keep_ref, send_pass_ref, held_ref, semaphores):
    _, lons, length, _ = kernels_ref.shape
    half = lons // 2
    copies = []
    for piece in range(2):
        at = slice(piece * half, piece * half + half)
        copies.append(
            pltpu.make_async_copy(kernels_ref.at[0, at], held_ref.at[at], semaphores.at[piece])
        )
        copies[piece].start()
    part = 2 * lax.axis_index("event_0") + lax.axis_index("event_1")
    rows = length // 4
    local = lax.broadcasted_iota(jnp.int32, (rows, length), 0)
    order = [part, part ^ 2, part ^ 1, part ^ 3]
    matrix = jnp.concatenate(
        [gauss_rows(length, 3.0, local + rows * block, 1) for block in order], axis=0
    )
    weights = jnp.concatenate([jnp.concatenate([m, m], axis=1) for m in split(matrix)], axis=0)
    outs = (keep_ref, pass_ref, send_keep_ref, send_pass_ref)
    for piece in range(2):
        copies[piece].wait()
        for a in range(piece * half, piece * half + half):
            both = dot(weights, jnp.concatenate(split(held_ref[a]), axis=0))
            out = both[:length] + both[length:]
            for k, ref in enumerate(outs):
                ref[a] = out[k * rows : (k + 1) * rows]


def smoothed(field, high, low):
    count = field.shape[0]
    both = jnp.concatenate(split(field), axis=0)
    out = dot(both, high) + dot(both, low)
    return out[:count] + out[count:]


def fetch_kernel(curvature_ref, held_ref, high_ref, low_ref, semaphore):
    copy = pltpu.make_async_copy(curvature_ref, held_ref, semaphore)
    copy.start()
    lats = high_ref.shape[0]
    column = lax.broadcasted_iota(jnp.int32, (lats, lats), 1)
    high_ref[...], low_ref[...] = split(gauss_rows(lats, 4.0, column, 0))
    copy.wait()


def edge_kernel(keep_ref, near_ref, passed_ref, own_ref, other_ref):
    lons = keep_ref.shape[0]
    start = jnp.where(cut_number() == lax.axis_size(CUTS) - 1, lons - RIM, 0)
    for a in range(RIM):
        own_ref[a] = keep_ref[start + a] + near_ref[start + a]
        other_ref[a] = passed_ref[start + a]


def latitude_kernel(keep_ref, near_ref, far_ref, high_ref, low_ref, plane_ref, first_ref, second_ref):
    lons, rows, lats = keep_ref.shape
    summed = (keep_ref[...] + near_ref[...] + far_ref[...]).reshape(lons * rows, lats)
    plane = smoothed(summed, high_ref[...], low_ref[...]).reshape(lons, rows, lats)
    plane_ref[...] = plane
    odd = lax.rem(cut_number(), 2) == 1

    @pl.when(odd)
    def _():
        first_ref[...] = plane[:RIM]
        second_ref[...] = plane[lons - RIM :]

    @pl.when(jnp.logical_not(odd))
    def _():
        first_ref[...] = plane[lons - RIM :]
        second_ref[...] = plane[:RIM]


def lane_numbers():
    return lax.broadcasted_iota(jnp.int32, (8, LANES), 1)


def tiles(shape):
    return [
        (a, slice(8 * r, 8 * r + 8), slice(LANES * b, LANES * (b + 1)))
        for r in range(shape[1] // 8)
        for b in range(shape[2] // LANES)
        for a in range(shape[0])
    ]


def placed(sums):
    lanes = lane_numbers()
    row = jnp.zeros((8, LANES), jnp.float32)
    for lane, value in sums:
        row = row + jnp.where(lanes == lane, jnp.sum(value, axis=1, keepdims=True), 0.0)
    return row


def gram_kernel(steps_ref, curvature_ref, changes_ref, row_ref):
    lons, rows, lats = steps_ref.shape[1:]
    spots = [
        (slice(8 * r, 8 * r + 8), slice(LANES * b, LANES * (b + 1)))
        for r in range(rows // 8)
        for b in range(lats // LANES)
    ]
    half = PAIRS // 2
    upper = [(i, j) for i in range(PAIRS) for j in range(i, PAIRS)]

    def first(a, sums):
        for at in spots:
            steps = [steps_ref[(i, a, *at)] for i in range(half)]
            changes = [None] * PAIRS
            for i in range(PAIRS):
                step = steps[i] if i < half else steps_ref[(i, a, *at)]
                changes[i] = curvature_ref[(i, a, *at)] * step
                changes_ref[(i, a, *at)] = changes[i]
            sums = [sums[k] + steps[k // PAIRS] * changes[k % PAIRS] for k in range(half * PAIRS)]
        return sums

    def second(a, sums):
        for at in spots:
            steps = [steps_ref[(i, a, *at)] for i in range(half, PAIRS)]
            changes = [changes_ref[(i, a, *at)] for i in range(PAIRS)]
            sums = [sums[k] + steps[k // PAIRS] * changes[k % PAIRS] for k in range(half * PAIRS)]
        return sums

    def third(a, sums):
        for at in spots:
            changes = [changes_ref[(i, a, *at)] for i in range(PAIRS)]
            sums = [value + changes[i] * changes[j] for value, (i, j) in zip(sums, upper)]
        return sums

    zero = jnp.zeros((8, LANES), jnp.float32)
    row = zero
    for start, step, size in ((0, first, 32), (32, second, 32), (SQUARES, third, len(upper))):
        sums = lax.fori_loop(0, lons, step, [zero] * size)
        row = row + placed([(start + k, value) for k, value in enumerate(sums)])
    row_ref[...] = row


def product_kernel(
    plane_ref, first_ref, second_ref, wrap_own_ref, wrap_other_ref, high_ref, low_ref,
    steps_ref, changes_ref, gram_ref, gradient_ref, rows_ref, halo,
):
    lons, rows, lats = gradient_ref.shape
    weights = cycle_weights()
    cut, last = cut_number(), lax.axis_size(CUTS) - 1
    odd = lax.rem(cut, 2)
    halo[odd ^ 1] = first_ref[...]
    halo[odd] = second_ref[...]

    @pl.when(jnp.logical_or(cut == 0, cut == last))
    def _():
        summed = (wrap_own_ref[...] + wrap_other_ref[...]).reshape(RIM * rows, lats)
        halo[odd] = smoothed(summed, high_ref[...], low_ref[...]).reshape(RIM, rows, lats)

    sums = [jnp.zeros((8, LANES), jnp.float32) for _ in range(2 * PAIRS)]
    for r in range(rows // 8):
        for b in range(lats // LANES):
            at = (slice(8 * r, 8 * r + 8), slice(LANES * b, LANES * (b + 1)))
            padded = [halo[(0, a, *at)] for a in range(RIM)]
            padded += [plane_ref[(a, *at)] for a in range(lons)]
            padded += [halo[(1, a, *at)] for a in range(RIM)]
            for a in range(lons):
                value = weights[RIM] * padded[a + RIM]
                for k in range(RIM):
                    value = value + weights[k] * (padded[a + k] + padded[a + 2 * RIM - k])
                gradient_ref[(a, *at)] = value
                for pair in range(PAIRS):
                    sums[pair] = sums[pair] + steps_ref[(pair, a, *at)] * value
                    sums[PAIRS + pair] = sums[PAIRS + pair] + changes_ref[(pair, a, *at)] * value
    row = gram_ref[...] + placed([(STEPS_GRADIENT + k, value) for k, value in enumerate(sums)])
    row = jnp.sum(row, axis=0, keepdims=True)
    rows_ref[...] = jnp.broadcast_to(row[None], rows_ref.shape)


def direction_kernel(
    rows_ref, gradient_ref, steps_ref, changes_ref, gradient_out, direction_out, direction_ref, semaphores
):
    written = pltpu.make_async_copy(gradient_ref, gradient_out, semaphores.at[0])
    written.start()
    row = jnp.broadcast_to(jnp.sum(rows_ref[...], axis=0), (8, LANES))
    lanes = lane_numbers()
    pairs = lax.broadcasted_iota(jnp.int32, (8, LANES), 0)

    def column(lane_of):
        picked = jnp.where(lanes == lane_of, row, 0.0)
        return jnp.broadcast_to(jnp.sum(picked, axis=1, keepdims=True), (8, LANES))

    def element(vector, i):
        return jnp.broadcast_to(vector[i : i + 1], (8, LANES))

    def square_lanes(j):
        low, high = jnp.minimum(pairs, j), jnp.maximum(pairs, j)
        return SQUARES + low * PAIRS - ((low * (low - 1)) >> 1) + high - low

    by_change = [column(pairs * PAIRS + i) for i in range(PAIRS)]
    by_step = [column(pairs + PAIRS * i) for i in range(PAIRS)]
    squares = [column(square_lanes(i)) for i in range(PAIRS)]
    curvs = column(pairs * (PAIRS + 1))
    steps_part = column(pairs + STEPS_GRADIENT)
    changes_part = column(pairs + CHANGES_GRADIENT)
    inverse = 1.0 / curvs
    scaling = element(curvs, PAIRS - 1) / element(squares[PAIRS - 1], PAIRS - 1)
    alphas = [None] * PAIRS
    for i in reversed(range(PAIRS)):
        alphas[i] = element(inverse * steps_part, i)
        steps_part = steps_part - alphas[i] * by_change[i]
        changes_part = changes_part - alphas[i] * squares[i]
    changes_part = scaling * changes_part
    weights = [None] * PAIRS
    for i in range(PAIRS):
        weights[i] = alphas[i] - element(inverse * changes_part, i)
        changes_part = changes_part + weights[i] * by_step[i]
    change_weights = [scaling * alpha for alpha in alphas]
    copies = []
    lons, pieces = gradient_ref.shape[0], 4
    for piece in range(pieces):
        at = slice(piece * lons // pieces, (piece + 1) * lons // pieces)
        for a, r, b in tiles(gradient_ref.shape):
            if at.start <= a < at.stop:
                value = -(scaling * gradient_ref[a, r, b])
                for i in range(PAIRS):
                    value = value + change_weights[i] * changes_ref[i, a, r, b]
                    value = value - weights[i] * steps_ref[i, a, r, b]
                direction_ref[a, r, b] = value
        if copies:
            copies[-1].start()
        copies.append(
            pltpu.make_async_copy(
                direction_ref.at[at], direction_out.at[at], semaphores.at[1 + piece]
            )
        )
    copies[-1].start()
    for copy in copies:
        copy.wait()
    written.wait()


def in_hbm(x):
    return pltpu.with_memory_space_constraint(x, pltpu.HBM)


def swapped(x, axis):
    return lax.ppermute(x, axis, [(0, 1), (1, 0)])


def cut_number():
    number = 0
    for axis in CUTS:
        number = number * lax.axis_size(axis) + lax.axis_index(axis)
    return number


def shards(kernels, steps, curvature):
    _, lons, rad_len, lats = kernels.shape
    rows = rad_len // 4
    block = ((lons, rows, lats), jnp.float32)
    size = lons * rows * lats
    keep, pass_on, send_keep, send_pass = call(
        radial_kernel,
        [block] * 4,
        2 * 4 * rad_len * kernels.size,
        8 * kernels.size,
        in_specs=[pl.BlockSpec(memory_space=pltpu.HBM)],
        scratch_shapes=[pltpu.VMEM(kernels.shape[1:], jnp.float32), pltpu.SemaphoreType.DMA((2,))],
    )(in_hbm(kernels))
    near_pass = swapped(send_pass, "event_1")
    passed = pass_on + near_pass
    far = swapped(passed, "event_0")
    near_keep = swapped(send_keep, "event_1")
    square = ((lats, lats), jnp.bfloat16)
    held_curvature, high, low = call(
        fetch_kernel,
        [(curvature.shape, jnp.float32), square, square],
        10 * lats * lats,
        8 * curvature.size,
        in_specs=[pl.BlockSpec(memory_space=pltpu.HBM)],
        scratch_shapes=[pltpu.SemaphoreType.DMA],
    )(in_hbm(curvature))
    cuts, last = lax.axis_size(CUTS), lax.axis_size(CUTS) - 1
    events = lax.axis_size(EVENT)
    inner = [(c * events + e, c * events + e) for c in range(1, last) for e in range(events)]
    side = ((RIM, rows, lats), jnp.float32)
    edge_own, edge_other = call(edge_kernel, [side, side], size, 12 * size)(keep, near_keep, passed)

    def wrapped(x, flip):
        ends = [(e, last * events + (e ^ flip)) for e in range(events)]
        return lax.ppermute(x, CUTS_EVENT, ends + [two[::-1] for two in ends] + inner)

    wrap_other = wrapped(edge_other, 2)
    wrap_own = wrapped(edge_own, 0)
    plane, first, second = call(
        latitude_kernel, [block, side, side], 2 * 4 * lats * size, 16 * size
    )(keep, near_keep, far, high, low)
    first = lax.ppermute(first, CUTS, [(c, c ^ 1) for c in range(cuts)])
    second = lax.ppermute(
        second, CUTS, [(0, 0), (last, last)] + [(c, ((c - 1) ^ 1) + 1) for c in range(1, last)]
    )
    changes, gram = call(
        gram_kernel,
        [(steps.shape, jnp.float32), ((8, LANES), jnp.float32)],
        2 * 100 * size,
        12 * steps.size,
    )(steps, held_curvature)
    gradient, outgoing = call(
        product_kernel,
        [block, ((cuts * events, 1, LANES), jnp.float32)],
        2 * 30 * size,
        4 * 20 * size,
        scratch_shapes=[pltpu.VMEM((2, RIM, rows, lats), jnp.float32)],
    )(plane, first, second, wrap_own, wrap_other, high, low, steps, changes, gram)
    arrived = lax.all_to_all(outgoing, CUTS_EVENT, 0, 0, tiled=True)
    return call(
        direction_kernel,
        [block] * 2,
        2 * 17 * size,
        4 * 18 * size,
        out_specs=[pl.BlockSpec(memory_space=pltpu.HBM)] * 2,
        scratch_shapes=[pltpu.VMEM((lons, rows, lats), jnp.float32), pltpu.SemaphoreType.DMA((5,))],
    )(arrived, gradient, steps, changes)


def solution(mesh):
    torus = Mesh(
        mesh.devices.reshape(2, 4, 4, 2, 2), ("cuts_0", "cuts_1", "cuts_2", "event_0", "event_1")
    )
    in_specs = (P(EVENT, CUTS, None, None), P(None, CUTS, EVENT, None), P(None, CUTS, EVENT, None))
    out_specs = (P(CUTS, EVENT, None), P(CUTS, EVENT, None))
    return jax.shard_map(
        shards, mesh=torus, in_specs=in_specs, out_specs=out_specs, check_vma=False
    )
```

```python
import functools
import math

import jax
import jax.numpy as jnp
from jax import lax
from jax.experimental import pallas as pl
from jax.experimental.pallas import tpu as pltpu
from jax.sharding import Mesh
from jax.sharding import PartitionSpec as P

PAIRS = 8
RIM = 4
CUTS = ("cuts_0", "cuts_1", "cuts_2")
EVENT = ("event_0", "event_1")
CUTS_EVENT = ("cuts_0", "cuts_1", "cuts_2", "event_0", "event_1")
LANES = 128
SQUARES, STEPS_GRADIENT, CHANGES_GRADIENT = 64, 100, 108


def cycle_weights():
    unscaled = [math.exp(-((column - RIM) ** 2) / 4.5) for column in range(2 * RIM + 1)]
    whole = sum(unscaled)
    return [weight / whole for weight in unscaled]


def split(x):
    high = x.astype(jnp.bfloat16)
    low = (x - high.astype(jnp.float32)).astype(jnp.bfloat16)
    return high, low


def dot(a, b):
    return jnp.dot(a, b, preferred_element_type=jnp.float32)


def call(kernel, outs, flops, moved, limit=16, **options):
    return pl.pallas_call(
        kernel,
        out_shape=[jax.ShapeDtypeStruct(*out) for out in outs],
        compiler_params=pltpu.CompilerParams(vmem_limit_bytes=limit << 20),
        cost_estimate=pl.CostEstimate(flops=flops, bytes_accessed=moved, transcendentals=0),
        **options,
    )


def gauss_rows(length, sigma, rows, axis):
    offset = (rows - lax.broadcasted_iota(jnp.int32, rows.shape, axis)).astype(jnp.float32)
    matrix = jnp.exp(-offset * offset / (2.0 * sigma * sigma))
    return matrix / jnp.sum(matrix, axis=axis, keepdims=True)


def gauss_rows(length, sigma, rows, axis):
    offset = (rows - lax.broadcasted_iota(jnp.int32, rows.shape, axis)).astype(jnp.float32)
    matrix = jnp.exp(-offset * offset / (2.0 * sigma * sigma))
    return matrix / jnp.sum(matrix, axis=axis, keepdims=True)


def radial_kernel(
    kernels_ref, keep_ref, pass_far_ref, pass_near_ref, send_keep_ref, send_pass_ref, held_ref, semaphores
):
    _, _, length, _ = kernels_ref.shape
    odd = lax.rem(cut_number(), 2)
    copies = []
    for piece in range(2):
        copies.append(
            pltpu.make_async_copy(
                kernels_ref.at[0, pl.ds(RIM * (odd ^ piece), RIM)],
                held_ref.at[pl.ds(RIM * piece, RIM)],
                semaphores.at[piece],
            )
        )
        copies[piece].start()
    part = 2 * lax.axis_index("event_0") + lax.axis_index("event_1")
    rows = length // 4
    local = lax.broadcasted_iota(jnp.int32, (rows, length), 0)
    order = [part, part ^ 2, part ^ 1, part ^ 3]
    matrix = jnp.concatenate(
        [gauss_rows(length, 3.0, local + rows * block, 1) for block in order], axis=0
    )
    weights = jnp.concatenate([jnp.concatenate([m, m], axis=1) for m in split(matrix)], axis=0)
    for piece in range(2):
        copies[piece].wait()
        for a in range(RIM):
            at = piece * RIM + a
            both = dot(weights, jnp.concatenate(split(held_ref[at]), axis=0))
            out = both[:length] + both[length:]
            keep_ref[at] = out[:rows]
            (pass_far_ref, pass_near_ref)[piece][a] = out[rows : 2 * rows]
            send_keep_ref[at] = out[2 * rows : 3 * rows]
            send_pass_ref[at] = out[3 * rows :]


def smoothed(field, high, low):
    count = field.shape[0]
    both = jnp.concatenate(split(field), axis=0)
    out = dot(both, high) + dot(both, low)
    return out[:count] + out[count:]


def fetch_kernel(curvature_ref, held_ref, high_ref, low_ref, semaphore):
    copy = pltpu.make_async_copy(curvature_ref, held_ref, semaphore)
    copy.start()
    lats = high_ref.shape[0]
    column = lax.broadcasted_iota(jnp.int32, (lats, lats), 1)
    high_ref[...], low_ref[...] = split(gauss_rows(lats, 4.0, column, 0))
    copy.wait()


def latitude_kernel(start, keep_ref, near_ref, far_ref, high_ref, low_ref, plane_ref):
    lons, rows, lats = plane_ref.shape
    at = slice(start, start + lons)
    summed = (keep_ref[at] + near_ref[at] + far_ref[...]).reshape(lons * rows, lats)
    plane_ref[...] = smoothed(summed, high_ref[...], low_ref[...]).reshape(lons, rows, lats)


def lane_numbers():
    return lax.broadcasted_iota(jnp.int32, (8, LANES), 1)


def tiles(shape):
    return [
        (a, slice(8 * r, 8 * r + 8), slice(LANES * b, LANES * (b + 1)))
        for r in range(shape[1] // 8)
        for b in range(shape[2] // LANES)
        for a in range(shape[0])
    ]


def placed(sums):
    lanes = lane_numbers()
    row = jnp.zeros((8, LANES), jnp.float32)
    for lane, value in sums:
        row = row + jnp.where(lanes == lane, jnp.sum(value, axis=1, keepdims=True), 0.0)
    return row


def gram_kernel(steps_ref, curvature_ref, changes_ref, row_ref):
    lons, rows, lats = steps_ref.shape[1:]
    spots = [
        (slice(8 * r, 8 * r + 8), slice(LANES * b, LANES * (b + 1)))
        for r in range(rows // 8)
        for b in range(lats // LANES)
    ]
    half = PAIRS // 2
    upper = [(i, j) for i in range(PAIRS) for j in range(i, PAIRS)]

    def first(a, sums):
        for at in spots:
            steps = [steps_ref[(i, a, *at)] for i in range(half)]
            changes = [None] * PAIRS
            for i in range(PAIRS):
                step = steps[i] if i < half else steps_ref[(i, a, *at)]
                changes[i] = curvature_ref[(i, a, *at)] * step
                changes_ref[(i, a, *at)] = changes[i]
            sums = [sums[k] + steps[k // PAIRS] * changes[k % PAIRS] for k in range(half * PAIRS)]
        return sums

    def second(a, sums):
        for at in spots:
            steps = [steps_ref[(i, a, *at)] for i in range(half, PAIRS)]
            changes = [changes_ref[(i, a, *at)] for i in range(PAIRS)]
            sums = [sums[k] + steps[k // PAIRS] * changes[k % PAIRS] for k in range(half * PAIRS)]
        return sums

    def third(a, sums):
        for at in spots:
            changes = [changes_ref[(i, a, *at)] for i in range(PAIRS)]
            sums = [value + changes[i] * changes[j] for value, (i, j) in zip(sums, upper)]
        return sums

    zero = jnp.zeros((8, LANES), jnp.float32)
    row = zero
    for start, step, size in ((0, first, 32), (32, second, 32), (SQUARES, third, len(upper))):
        sums = lax.fori_loop(0, lons, step, [zero] * size)
        row = row + placed([(start + k, value) for k, value in enumerate(sums)])
    row_ref[...] = row


def product_kernel(
    far_halo_ref, far_ref, near_ref, near_halo_ref,
    steps_ref, changes_ref, gram_ref, gradient_ref, rows_ref, padded_ref,
):
    lons, rows, lats = gradient_ref.shape
    weights = cycle_weights()
    mirror = 3 * lax.rem(cut_number(), 2)
    for k, ref in enumerate((far_halo_ref, far_ref, near_ref, near_halo_ref)):
        padded_ref[k ^ mirror] = ref[...]
    sums = [jnp.zeros((8, LANES), jnp.float32) for _ in range(2 * PAIRS)]
    for r in range(rows // 8):
        for b in range(lats // LANES):
            at = (slice(8 * r, 8 * r + 8), slice(LANES * b, LANES * (b + 1)))
            padded = [padded_ref[(k, a, *at)] for k in range(4) for a in range(RIM)]
            for a in range(lons):
                value = weights[RIM] * padded[a + RIM]
                for k in range(RIM):
                    value = value + weights[k] * (padded[a + k] + padded[a + 2 * RIM - k])
                gradient_ref[(a, *at)] = value
                for pair in range(PAIRS):
                    sums[pair] = sums[pair] + steps_ref[(pair, a, *at)] * value
                    sums[PAIRS + pair] = sums[PAIRS + pair] + changes_ref[(pair, a, *at)] * value
    row = gram_ref[...] + placed([(STEPS_GRADIENT + k, value) for k, value in enumerate(sums)])
    row = jnp.sum(row, axis=0, keepdims=True)
    rows_ref[...] = jnp.broadcast_to(row[None], rows_ref.shape)


def direction_kernel(
    rows_ref, gradient_ref, steps_ref, changes_ref, gradient_out, direction_out, direction_ref, semaphores
):
    written = pltpu.make_async_copy(gradient_ref, gradient_out, semaphores.at[0])
    written.start()
    row = jnp.broadcast_to(jnp.sum(rows_ref[...], axis=0), (8, LANES))
    lanes = lane_numbers()
    pairs = lax.broadcasted_iota(jnp.int32, (8, LANES), 0)

    def column(lane_of):
        picked = jnp.where(lanes == lane_of, row, 0.0)
        return jnp.broadcast_to(jnp.sum(picked, axis=1, keepdims=True), (8, LANES))

    def element(vector, i):
        return jnp.broadcast_to(vector[i : i + 1], (8, LANES))

    def square_lanes(j):
        low, high = jnp.minimum(pairs, j), jnp.maximum(pairs, j)
        return SQUARES + low * PAIRS - ((low * (low - 1)) >> 1) + high - low

    by_change = [column(pairs * PAIRS + i) for i in range(PAIRS)]
    by_step = [column(pairs + PAIRS * i) for i in range(PAIRS)]
    squares = [column(square_lanes(i)) for i in range(PAIRS)]
    curvs = column(pairs * (PAIRS + 1))
    steps_part = column(pairs + STEPS_GRADIENT)
    changes_part = column(pairs + CHANGES_GRADIENT)
    inverse = 1.0 / curvs
    scaling = element(curvs, PAIRS - 1) / element(squares[PAIRS - 1], PAIRS - 1)
    alphas = [None] * PAIRS
    for i in reversed(range(PAIRS)):
        alphas[i] = element(inverse * steps_part, i)
        steps_part = steps_part - alphas[i] * by_change[i]
        changes_part = changes_part - alphas[i] * squares[i]
    changes_part = scaling * changes_part
    weights = [None] * PAIRS
    for i in range(PAIRS):
        weights[i] = alphas[i] - element(inverse * changes_part, i)
        changes_part = changes_part + weights[i] * by_step[i]
    change_weights = [scaling * alpha for alpha in alphas]
    copies = []
    lons, pieces = gradient_ref.shape[0], 4
    for piece in range(pieces):
        at = slice(piece * lons // pieces, (piece + 1) * lons // pieces)
        for a, r, b in tiles(gradient_ref.shape):
            if at.start <= a < at.stop:
                value = -(scaling * gradient_ref[a, r, b])
                for i in range(PAIRS):
                    value = value + change_weights[i] * changes_ref[i, a, r, b]
                    value = value - weights[i] * steps_ref[i, a, r, b]
                direction_ref[a, r, b] = value
        if copies:
            copies[-1].start()
        copies.append(
            pltpu.make_async_copy(
                direction_ref.at[at], direction_out.at[at], semaphores.at[1 + piece]
            )
        )
    copies[-1].start()
    for copy in copies:
        copy.wait()
    written.wait()


def in_hbm(x):
    return pltpu.with_memory_space_constraint(x, pltpu.HBM)


def swapped(x, axis):
    return lax.ppermute(x, axis, [(0, 1), (1, 0)])


def cut_number():
    number = 0
    for axis in CUTS:
        number = number * lax.axis_size(axis) + lax.axis_index(axis)
    return number


def shards(kernels, steps, curvature):
    _, lons, rad_len, lats = kernels.shape
    rows = rad_len // 4
    block = ((lons, rows, lats), jnp.float32)
    size = lons * rows * lats
    half = ((RIM, rows, lats), jnp.float32)
    cuts, events = lax.axis_size(CUTS), lax.axis_size(EVENT)
    keep, pass_far, pass_near, send_keep, send_pass = call(
        radial_kernel,
        [block, half, half, block, block],
        2 * 4 * rad_len * kernels.size,
        8 * kernels.size,
        in_specs=[pl.BlockSpec(memory_space=pltpu.HBM)],
        scratch_shapes=[pltpu.VMEM(kernels.shape[1:], jnp.float32), pltpu.SemaphoreType.DMA((2,))],
    )(in_hbm(kernels))
    near_pass = swapped(send_pass, "event_1")
    square = ((lats, lats), jnp.bfloat16)
    held_curvature, high, low = call(
        fetch_kernel,
        [(curvature.shape, jnp.float32), square, square],
        10 * lats * lats,
        8 * curvature.size,
        in_specs=[pl.BlockSpec(memory_space=pltpu.HBM)],
        scratch_shapes=[pltpu.SemaphoreType.DMA],
    )(in_hbm(curvature))
    far_chunk = swapped(pass_far + near_pass[:RIM], "event_0")
    near_chunk = swapped(pass_near + near_pass[RIM:], "event_0")
    near_keep = swapped(send_keep, "event_1")
    changes, gram = call(
        gram_kernel,
        [(steps.shape, jnp.float32), ((8, LANES), jnp.float32)],
        2 * 100 * size,
        12 * steps.size,
    )(steps, held_curvature)

    def plane_of(start, chunk):
        return call(
            functools.partial(latitude_kernel, start), [half], 4 * lats * size, 8 * size
        )(keep, near_keep, chunk, high, low)[0]

    far_plane = plane_of(0, far_chunk)
    far_halo = lax.ppermute(
        far_plane, CUTS, [(c, (((c - 1) ^ 1) + 1) % cuts) for c in range(1, cuts)] + [(0, cuts - 1)]
    )
    near_plane = plane_of(RIM, near_chunk)
    near_halo = lax.ppermute(near_plane, CUTS, [(c, c ^ 1) for c in range(cuts)])
    gradient, outgoing = call(
        product_kernel,
        [block, ((cuts * events, 1, LANES), jnp.float32)],
        2 * 30 * size,
        4 * 20 * size,
        scratch_shapes=[pltpu.VMEM((4, RIM, rows, lats), jnp.float32)],
    )(far_halo, far_plane, near_plane, near_halo, steps, changes, gram)
    arrived = lax.all_to_all(outgoing, CUTS_EVENT, 0, 0, tiled=True)
    return call(
        direction_kernel,
        [block] * 2,
        2 * 17 * size,
        4 * 18 * size,
        out_specs=[pl.BlockSpec(memory_space=pltpu.HBM)] * 2,
        scratch_shapes=[pltpu.VMEM((lons, rows, lats), jnp.float32), pltpu.SemaphoreType.DMA((5,))],
    )(arrived, gradient, steps, changes)


def solution(mesh):
    torus = Mesh(
        mesh.devices.reshape(2, 4, 4, 2, 2), ("cuts_0", "cuts_1", "cuts_2", "event_0", "event_1")
    )
    in_specs = (P(EVENT, CUTS, None, None), P(None, CUTS, EVENT, None), P(None, CUTS, EVENT, None))
    out_specs = (P(CUTS, EVENT, None), P(CUTS, EVENT, None))
    return jax.shard_map(
        shards, mesh=torus, in_specs=in_specs, out_specs=out_specs, check_vma=False
    )
```

```python
import math

import jax
import jax.numpy as jnp
from jax import lax
from jax.experimental import pallas as pl
from jax.experimental.pallas import tpu as pltpu
from jax.sharding import Mesh
from jax.sharding import PartitionSpec as P

PAIRS = 8
RIM = 4
CUTS = ("cuts_0", "cuts_1", "cuts_2")
EVENT = ("event_0", "event_1")
CUTS_EVENT = ("cuts_0", "cuts_1", "cuts_2", "event_0", "event_1")
LANES = 128
SQUARES, STEPS_GRADIENT, CHANGES_GRADIENT = 64, 100, 108


def cycle_weights():
    unscaled = [math.exp(-((column - RIM) ** 2) / 4.5) for column in range(2 * RIM + 1)]
    whole = sum(unscaled)
    return [weight / whole for weight in unscaled]


def split(x):
    high = x.astype(jnp.bfloat16)
    low = (x - high.astype(jnp.float32)).astype(jnp.bfloat16)
    return high, low


def dot(a, b):
    return jnp.dot(a, b, preferred_element_type=jnp.float32)


def call(kernel, outs, flops, moved, limit=16, **options):
    return pl.pallas_call(
        kernel,
        out_shape=[jax.ShapeDtypeStruct(*out) for out in outs],
        compiler_params=pltpu.CompilerParams(vmem_limit_bytes=limit << 20),
        cost_estimate=pl.CostEstimate(flops=flops, bytes_accessed=moved, transcendentals=0),
        **options,
    )


def gauss_rows(length, sigma, rows, axis):
    offset = (rows - lax.broadcasted_iota(jnp.int32, rows.shape, axis)).astype(jnp.float32)
    matrix = jnp.exp(-offset * offset / (2.0 * sigma * sigma))
    return matrix / jnp.sum(matrix, axis=axis, keepdims=True)


def gauss_rows(length, sigma, rows, axis):
    offset = (rows - lax.broadcasted_iota(jnp.int32, rows.shape, axis)).astype(jnp.float32)
    matrix = jnp.exp(-offset * offset / (2.0 * sigma * sigma))
    return matrix / jnp.sum(matrix, axis=axis, keepdims=True)


def radial_products(field_ref, weights, keep_ref, pass_ref, send_keep_ref, send_pass_ref):
    for a in range(field_ref.shape[0]):
        both = dot(weights, jnp.concatenate(split(field_ref[a]), axis=0))
        length = both.shape[0] // 2
        rows = length // 4
        out = both[:length] + both[length:]
        for k, ref in enumerate((keep_ref, pass_ref, send_keep_ref, send_pass_ref)):
            ref[a] = out[k * rows : (k + 1) * rows]


def far_radial_kernel(
    kernels_ref, keep_ref, pass_ref, send_keep_ref, send_pass_ref, near_ref, weights_ref, far_ref, semaphores
):
    length = kernels_ref.shape[2]
    odd = lax.rem(cut_number(), 2)
    copies = []
    for piece, ref in enumerate((far_ref, near_ref)):
        source = kernels_ref.at[0, pl.ds(RIM * (odd ^ piece), RIM)]
        copies.append(pltpu.make_async_copy(source, ref, semaphores.at[piece]))
        copies[piece].start()
    part = 2 * lax.axis_index("event_0") + lax.axis_index("event_1")
    rows = length // 4
    local = lax.broadcasted_iota(jnp.int32, (rows, length), 0)
    order = [part, part ^ 2, part ^ 1, part ^ 3]
    matrix = jnp.concatenate(
        [gauss_rows(length, 3.0, local + rows * block, 1) for block in order], axis=0
    )
    weights = jnp.concatenate([jnp.concatenate([m, m], axis=1) for m in split(matrix)], axis=0)
    weights_ref[...] = weights
    copies[0].wait()
    radial_products(far_ref, weights, keep_ref, pass_ref, send_keep_ref, send_pass_ref)
    copies[1].wait()


def near_radial_kernel(near_ref, weights_ref, keep_ref, pass_ref, send_keep_ref, send_pass_ref):
    radial_products(near_ref, weights_ref[...], keep_ref, pass_ref, send_keep_ref, send_pass_ref)


def smoothed(field, high, low):
    count = field.shape[0]
    both = jnp.concatenate(split(field), axis=0)
    out = dot(both, high) + dot(both, low)
    return out[:count] + out[count:]


def fetch_kernel(curvature_ref, held_ref, high_ref, low_ref, semaphore):
    copy = pltpu.make_async_copy(curvature_ref, held_ref, semaphore)
    copy.start()
    lats = high_ref.shape[0]
    column = lax.broadcasted_iota(jnp.int32, (lats, lats), 1)
    high_ref[...], low_ref[...] = split(gauss_rows(lats, 4.0, column, 0))
    copy.wait()


def latitude_kernel(keep_ref, core_ref, chip_ref, high_ref, low_ref, plane_ref):
    lons, rows, lats = plane_ref.shape
    summed = (keep_ref[...] + core_ref[...] + chip_ref[...]).reshape(lons * rows, lats)
    plane_ref[...] = smoothed(summed, high_ref[...], low_ref[...]).reshape(lons, rows, lats)


def lane_numbers():
    return lax.broadcasted_iota(jnp.int32, (8, LANES), 1)


def tiles(shape):
    return [
        (a, slice(8 * r, 8 * r + 8), slice(LANES * b, LANES * (b + 1)))
        for r in range(shape[1] // 8)
        for b in range(shape[2] // LANES)
        for a in range(shape[0])
    ]


def placed(sums):
    lanes = lane_numbers()
    row = jnp.zeros((8, LANES), jnp.float32)
    for lane, value in sums:
        row = row + jnp.where(lanes == lane, jnp.sum(value, axis=1, keepdims=True), 0.0)
    return row


def gram_kernel(steps_ref, curvature_ref, changes_ref, row_ref):
    lons, rows, lats = steps_ref.shape[1:]
    spots = [
        (slice(8 * r, 8 * r + 8), slice(LANES * b, LANES * (b + 1)))
        for r in range(rows // 8)
        for b in range(lats // LANES)
    ]
    half = PAIRS // 2
    upper = [(i, j) for i in range(PAIRS) for j in range(i, PAIRS)]

    def first(a, sums):
        for at in spots:
            steps = [steps_ref[(i, a, *at)] for i in range(half)]
            changes = [None] * PAIRS
            for i in range(PAIRS):
                step = steps[i] if i < half else steps_ref[(i, a, *at)]
                changes[i] = curvature_ref[(i, a, *at)] * step
                changes_ref[(i, a, *at)] = changes[i]
            sums = [sums[k] + steps[k // PAIRS] * changes[k % PAIRS] for k in range(half * PAIRS)]
        return sums

    def second(a, sums):
        for at in spots:
            steps = [steps_ref[(i, a, *at)] for i in range(half, PAIRS)]
            changes = [changes_ref[(i, a, *at)] for i in range(PAIRS)]
            sums = [sums[k] + steps[k // PAIRS] * changes[k % PAIRS] for k in range(half * PAIRS)]
        return sums

    def third(a, sums):
        for at in spots:
            changes = [changes_ref[(i, a, *at)] for i in range(PAIRS)]
            sums = [value + changes[i] * changes[j] for value, (i, j) in zip(sums, upper)]
        return sums

    zero = jnp.zeros((8, LANES), jnp.float32)
    row = zero
    for start, step, size in ((0, first, 32), (32, second, 32), (SQUARES, third, len(upper))):
        sums = lax.fori_loop(0, lons, step, [zero] * size)
        row = row + placed([(start + k, value) for k, value in enumerate(sums)])
    row_ref[...] = row


def product_kernel(
    far_halo_ref, far_ref, near_ref, near_halo_ref,
    steps_ref, changes_ref, gram_ref, gradient_ref, rows_ref, padded_ref,
):
    lons, rows, lats = gradient_ref.shape
    weights = cycle_weights()
    mirror = 3 * lax.rem(cut_number(), 2)
    for k, ref in enumerate((far_halo_ref, far_ref, near_ref, near_halo_ref)):
        padded_ref[k ^ mirror] = ref[...]
    sums = [jnp.zeros((8, LANES), jnp.float32) for _ in range(2 * PAIRS)]
    for r in range(rows // 8):
        for b in range(lats // LANES):
            at = (slice(8 * r, 8 * r + 8), slice(LANES * b, LANES * (b + 1)))
            padded = [padded_ref[(k, a, *at)] for k in range(4) for a in range(RIM)]
            for a in range(lons):
                value = weights[RIM] * padded[a + RIM]
                for k in range(RIM):
                    value = value + weights[k] * (padded[a + k] + padded[a + 2 * RIM - k])
                gradient_ref[(a, *at)] = value
                for pair in range(PAIRS):
                    sums[pair] = sums[pair] + steps_ref[(pair, a, *at)] * value
                    sums[PAIRS + pair] = sums[PAIRS + pair] + changes_ref[(pair, a, *at)] * value
    row = gram_ref[...] + placed([(STEPS_GRADIENT + k, value) for k, value in enumerate(sums)])
    row = jnp.sum(row, axis=0, keepdims=True)
    rows_ref[...] = jnp.broadcast_to(row[None], rows_ref.shape)


def direction_kernel(
    rows_ref, gradient_ref, steps_ref, changes_ref, gradient_out, direction_out, direction_ref, semaphores
):
    written = pltpu.make_async_copy(gradient_ref, gradient_out, semaphores.at[0])
    written.start()
    row = jnp.broadcast_to(jnp.sum(rows_ref[...], axis=0), (8, LANES))
    lanes = lane_numbers()
    pairs = lax.broadcasted_iota(jnp.int32, (8, LANES), 0)

    def column(lane_of):
        picked = jnp.where(lanes == lane_of, row, 0.0)
        return jnp.broadcast_to(jnp.sum(picked, axis=1, keepdims=True), (8, LANES))

    def element(vector, i):
        return jnp.broadcast_to(vector[i : i + 1], (8, LANES))

    def square_lanes(j):
        low, high = jnp.minimum(pairs, j), jnp.maximum(pairs, j)
        return SQUARES + low * PAIRS - ((low * (low - 1)) >> 1) + high - low

    by_change = [column(pairs * PAIRS + i) for i in range(PAIRS)]
    by_step = [column(pairs + PAIRS * i) for i in range(PAIRS)]
    squares = [column(square_lanes(i)) for i in range(PAIRS)]
    curvs = column(pairs * (PAIRS + 1))
    steps_part = column(pairs + STEPS_GRADIENT)
    changes_part = column(pairs + CHANGES_GRADIENT)
    inverse = 1.0 / curvs
    scaling = element(curvs, PAIRS - 1) / element(squares[PAIRS - 1], PAIRS - 1)
    alphas = [None] * PAIRS
    for i in reversed(range(PAIRS)):
        alphas[i] = element(inverse * steps_part, i)
        steps_part = steps_part - alphas[i] * by_change[i]
        changes_part = changes_part - alphas[i] * squares[i]
    changes_part = scaling * changes_part
    weights = [None] * PAIRS
    for i in range(PAIRS):
        weights[i] = alphas[i] - element(inverse * changes_part, i)
        changes_part = changes_part + weights[i] * by_step[i]
    change_weights = [scaling * alpha for alpha in alphas]
    copies = []
    lons, pieces = gradient_ref.shape[0], 4
    for piece in range(pieces):
        at = slice(piece * lons // pieces, (piece + 1) * lons // pieces)
        for a, r, b in tiles(gradient_ref.shape):
            if at.start <= a < at.stop:
                value = -(scaling * gradient_ref[a, r, b])
                for i in range(PAIRS):
                    value = value + change_weights[i] * changes_ref[i, a, r, b]
                    value = value - weights[i] * steps_ref[i, a, r, b]
                direction_ref[a, r, b] = value
        if copies:
            copies[-1].start()
        copies.append(
            pltpu.make_async_copy(
                direction_ref.at[at], direction_out.at[at], semaphores.at[1 + piece]
            )
        )
    copies[-1].start()
    for copy in copies:
        copy.wait()
    written.wait()


def in_hbm(x):
    return pltpu.with_memory_space_constraint(x, pltpu.HBM)


def swapped(x, axis):
    return lax.ppermute(x, axis, [(0, 1), (1, 0)])


def cut_number():
    number = 0
    for axis in CUTS:
        number = number * lax.axis_size(axis) + lax.axis_index(axis)
    return number


def shards(kernels, steps, curvature):
    _, lons, rad_len, lats = kernels.shape
    rows = rad_len // 4
    block = ((lons, rows, lats), jnp.float32)
    size = lons * rows * lats
    half = ((RIM, rows, lats), jnp.float32)
    cuts, events = lax.axis_size(CUTS), lax.axis_size(EVENT)
    table = ((2 * rad_len, 2 * rad_len), jnp.bfloat16)
    flops = 4 * rad_len * kernels.size
    far_keep, far_pass, far_send_keep, far_send_pass, near_field, weights = call(
        far_radial_kernel,
        [half] * 4 + [((RIM, rad_len, lats), jnp.float32), table],
        flops,
        8 * kernels.size,
        in_specs=[pl.BlockSpec(memory_space=pltpu.HBM)],
        scratch_shapes=[
            pltpu.VMEM((RIM, rad_len, lats), jnp.float32),
            pltpu.SemaphoreType.DMA((2,)),
        ],
    )(in_hbm(kernels))
    far_core_pass = swapped(far_send_pass, "event_1")
    near_keep, near_pass, near_send_keep, near_send_pass = call(
        near_radial_kernel, [half] * 4, flops, 4 * kernels.size
    )(near_field, weights)
    far_chip = swapped(far_pass + far_core_pass, "event_0")
    near_core_pass = swapped(near_send_pass, "event_1")
    square = ((lats, lats), jnp.bfloat16)
    held_curvature, high, low = call(
        fetch_kernel,
        [(curvature.shape, jnp.float32), square, square],
        10 * lats * lats,
        8 * curvature.size,
        in_specs=[pl.BlockSpec(memory_space=pltpu.HBM)],
        scratch_shapes=[pltpu.SemaphoreType.DMA],
    )(in_hbm(curvature))
    near_chip = swapped(near_pass + near_core_pass, "event_0")
    far_core = swapped(far_send_keep, "event_1")
    near_core = swapped(near_send_keep, "event_1")
    changes, gram = call(
        gram_kernel,
        [(steps.shape, jnp.float32), ((8, LANES), jnp.float32)],
        2 * 100 * size,
        12 * steps.size,
    )(steps, held_curvature)

    def plane_of(*parts):
        return call(latitude_kernel, [half], 4 * lats * size, 8 * size)(*parts, high, low)[0]

    far_plane = plane_of(far_keep, far_core, far_chip)
    far_halo = lax.ppermute(
        far_plane, CUTS, [(c, (((c - 1) ^ 1) + 1) % cuts) for c in range(1, cuts)] + [(0, cuts - 1)]
    )
    near_plane = plane_of(near_keep, near_core, near_chip)
    near_halo = lax.ppermute(near_plane, CUTS, [(c, c ^ 1) for c in range(cuts)])
    gradient, outgoing = call(
        product_kernel,
        [block, ((cuts * events, 1, LANES), jnp.float32)],
        2 * 30 * size,
        4 * 20 * size,
        scratch_shapes=[pltpu.VMEM((4, RIM, rows, lats), jnp.float32)],
    )(far_halo, far_plane, near_plane, near_halo, steps, changes, gram)
    arrived = lax.all_to_all(outgoing, CUTS_EVENT, 0, 0, tiled=True)
    return call(
        direction_kernel,
        [block] * 2,
        2 * 17 * size,
        4 * 18 * size,
        out_specs=[pl.BlockSpec(memory_space=pltpu.HBM)] * 2,
        scratch_shapes=[pltpu.VMEM((lons, rows, lats), jnp.float32), pltpu.SemaphoreType.DMA((5,))],
    )(arrived, gradient, steps, changes)


def solution(mesh):
    torus = Mesh(
        mesh.devices.reshape(2, 4, 4, 2, 2), ("cuts_0", "cuts_1", "cuts_2", "event_0", "event_1")
    )
    in_specs = (P(EVENT, CUTS, None, None), P(None, CUTS, EVENT, None), P(None, CUTS, EVENT, None))
    out_specs = (P(CUTS, EVENT, None), P(CUTS, EVENT, None))
    return jax.shard_map(
        shards, mesh=torus, in_specs=in_specs, out_specs=out_specs, check_vma=False
    )
```

```python
import math

import jax
import jax.numpy as jnp
from jax import lax
from jax.experimental import pallas as pl
from jax.experimental.pallas import tpu as pltpu
from jax.sharding import Mesh
from jax.sharding import PartitionSpec as P

PAIRS = 8
RIM = 4
CUTS = ("cuts_0", "cuts_1", "cuts_2")
EVENT = ("event_0", "event_1")
CUTS_EVENT = ("cuts_0", "cuts_1", "cuts_2", "event_0", "event_1")
LANES = 128
SQUARES, STEPS_GRADIENT, CHANGES_GRADIENT = 64, 100, 108


def cycle_weights():
    unscaled = [math.exp(-((column - RIM) ** 2) / 4.5) for column in range(2 * RIM + 1)]
    whole = sum(unscaled)
    return [weight / whole for weight in unscaled]


def split(x):
    high = x.astype(jnp.bfloat16)
    low = (x - high.astype(jnp.float32)).astype(jnp.bfloat16)
    return high, low


def dot(a, b):
    return jnp.dot(a, b, preferred_element_type=jnp.float32)


def call(kernel, outs, flops, moved, limit=16, **options):
    return pl.pallas_call(
        kernel,
        out_shape=[jax.ShapeDtypeStruct(*out) for out in outs],
        compiler_params=pltpu.CompilerParams(vmem_limit_bytes=limit << 20),
        cost_estimate=pl.CostEstimate(flops=flops, bytes_accessed=moved, transcendentals=0),
        **options,
    )


def gauss_rows(length, sigma, rows, axis):
    offset = (rows - lax.broadcasted_iota(jnp.int32, rows.shape, axis)).astype(jnp.float32)
    matrix = jnp.exp(-offset * offset / (2.0 * sigma * sigma))
    return matrix / jnp.sum(matrix, axis=axis, keepdims=True)


def gauss_rows(length, sigma, rows, axis):
    offset = (rows - lax.broadcasted_iota(jnp.int32, rows.shape, axis)).astype(jnp.float32)
    matrix = jnp.exp(-offset * offset / (2.0 * sigma * sigma))
    return matrix / jnp.sum(matrix, axis=axis, keepdims=True)


def radial_products(field_ref, weights, keep_ref, pass_ref, send_keep_ref, send_pass_ref):
    for a in range(field_ref.shape[0]):
        both = dot(weights, jnp.concatenate(split(field_ref[a]), axis=0))
        length = both.shape[0] // 2
        rows = length // 4
        out = both[:length] + both[length:]
        for k, ref in enumerate((keep_ref, pass_ref, send_keep_ref, send_pass_ref)):
            ref[a] = out[k * rows : (k + 1) * rows]


def far_radial_kernel(
    kernels_ref, keep_ref, pass_ref, send_keep_ref, send_pass_ref, near_ref, weights_ref, far_ref, semaphores
):
    length = kernels_ref.shape[2]
    odd = lax.rem(cut_number(), 2)
    copies = []
    for piece, ref in enumerate((far_ref, near_ref)):
        source = kernels_ref.at[0, pl.ds(RIM * (odd ^ piece), RIM)]
        copies.append(pltpu.make_async_copy(source, ref, semaphores.at[piece]))
        copies[piece].start()
    part = 2 * lax.axis_index("event_0") + lax.axis_index("event_1")
    rows = length // 4
    local = lax.broadcasted_iota(jnp.int32, (rows, length), 0)
    order = [part, part ^ 2, part ^ 1, part ^ 3]
    matrix = jnp.concatenate(
        [gauss_rows(length, 3.0, local + rows * block, 1) for block in order], axis=0
    )
    weights = jnp.concatenate([jnp.concatenate([m, m], axis=1) for m in split(matrix)], axis=0)
    weights_ref[...] = weights
    copies[0].wait()
    radial_products(far_ref, weights, keep_ref, pass_ref, send_keep_ref, send_pass_ref)
    copies[1].wait()


def near_radial_kernel(
    near_ref, weights_ref, keep_ref, pass_ref, send_keep_ref, send_pass_ref, high_ref, low_ref
):
    radial_products(near_ref, weights_ref[...], keep_ref, pass_ref, send_keep_ref, send_pass_ref)
    lats = high_ref.shape[0]
    column = lax.broadcasted_iota(jnp.int32, (lats, lats), 1)
    high_ref[...], low_ref[...] = split(gauss_rows(lats, 4.0, column, 0))


def smoothed(field, high, low):
    count = field.shape[0]
    both = jnp.concatenate(split(field), axis=0)
    out = dot(both, high) + dot(both, low)
    return out[:count] + out[count:]


def fetch_kernel(curvature_ref, held_ref, semaphore):
    copy = pltpu.make_async_copy(curvature_ref, held_ref, semaphore)
    copy.start()
    copy.wait()


def plane_of(parts, high_ref, low_ref):
    summed = sum(ref[...] for ref in parts)
    lons, rows, lats = summed.shape
    plane = smoothed(summed.reshape(lons * rows, lats), high_ref[...], low_ref[...])
    return plane.reshape(lons, rows, lats)


def far_latitude_kernel(
    keep_ref, core_ref, chip_ref, passed_ref, cross_ref, high_ref, low_ref, plane_ref, out_ref
):
    plane = plane_of((keep_ref, core_ref, chip_ref), high_ref, low_ref)
    plane_ref[...] = plane
    first = cut_number() == 0

    @pl.when(first)
    def _():
        out_ref[...] = plane_of((passed_ref, cross_ref), high_ref, low_ref)

    @pl.when(jnp.logical_not(first))
    def _():
        out_ref[...] = plane


def near_latitude_kernel(keep_ref, core_ref, chip_ref, high_ref, low_ref, plane_ref):
    plane_ref[...] = plane_of((keep_ref, core_ref, chip_ref), high_ref, low_ref)


def lane_numbers():
    return lax.broadcasted_iota(jnp.int32, (8, LANES), 1)


def tiles(shape):
    return [
        (a, slice(8 * r, 8 * r + 8), slice(LANES * b, LANES * (b + 1)))
        for r in range(shape[1] // 8)
        for b in range(shape[2] // LANES)
        for a in range(shape[0])
    ]


def placed(sums):
    lanes = lane_numbers()
    row = jnp.zeros((8, LANES), jnp.float32)
    for lane, value in sums:
        row = row + jnp.where(lanes == lane, jnp.sum(value, axis=1, keepdims=True), 0.0)
    return row


def gram_kernel(steps_ref, curvature_ref, changes_ref, row_ref):
    lons, rows, lats = steps_ref.shape[1:]
    spots = [
        (slice(8 * r, 8 * r + 8), slice(LANES * b, LANES * (b + 1)))
        for r in range(rows // 8)
        for b in range(lats // LANES)
    ]
    half = PAIRS // 2
    upper = [(i, j) for i in range(PAIRS) for j in range(i, PAIRS)]

    def first(a, sums):
        for at in spots:
            steps = [steps_ref[(i, a, *at)] for i in range(half)]
            changes = [None] * PAIRS
            for i in range(PAIRS):
                step = steps[i] if i < half else steps_ref[(i, a, *at)]
                changes[i] = curvature_ref[(i, a, *at)] * step
                changes_ref[(i, a, *at)] = changes[i]
            sums = [sums[k] + steps[k // PAIRS] * changes[k % PAIRS] for k in range(half * PAIRS)]
        return sums

    def second(a, sums):
        for at in spots:
            steps = [steps_ref[(i, a, *at)] for i in range(half, PAIRS)]
            changes = [changes_ref[(i, a, *at)] for i in range(PAIRS)]
            sums = [sums[k] + steps[k // PAIRS] * changes[k % PAIRS] for k in range(half * PAIRS)]
        return sums

    def third(a, sums):
        for at in spots:
            changes = [changes_ref[(i, a, *at)] for i in range(PAIRS)]
            sums = [value + changes[i] * changes[j] for value, (i, j) in zip(sums, upper)]
        return sums

    zero = jnp.zeros((8, LANES), jnp.float32)
    row = zero
    for start, step, size in ((0, first, 32), (32, second, 32), (SQUARES, third, len(upper))):
        sums = lax.fori_loop(0, lons, step, [zero] * size)
        row = row + placed([(start + k, value) for k, value in enumerate(sums)])
    row_ref[...] = row


def product_kernel(
    far_halo_ref, far_ref, near_ref, near_halo_ref,
    steps_ref, changes_ref, gram_ref, gradient_ref, rows_ref, padded_ref,
):
    lons, rows, lats = gradient_ref.shape
    weights = cycle_weights()
    mirror = 3 * lax.rem(cut_number(), 2)
    for k, ref in enumerate((far_halo_ref, far_ref, near_ref, near_halo_ref)):
        padded_ref[k ^ mirror] = ref[...]
    sums = [jnp.zeros((8, LANES), jnp.float32) for _ in range(2 * PAIRS)]
    for r in range(rows // 8):
        for b in range(lats // LANES):
            at = (slice(8 * r, 8 * r + 8), slice(LANES * b, LANES * (b + 1)))
            padded = [padded_ref[(k, a, *at)] for k in range(4) for a in range(RIM)]
            for a in range(lons):
                value = weights[RIM] * padded[a + RIM]
                for k in range(RIM):
                    value = value + weights[k] * (padded[a + k] + padded[a + 2 * RIM - k])
                gradient_ref[(a, *at)] = value
                for pair in range(PAIRS):
                    sums[pair] = sums[pair] + steps_ref[(pair, a, *at)] * value
                    sums[PAIRS + pair] = sums[PAIRS + pair] + changes_ref[(pair, a, *at)] * value
    row = gram_ref[...] + placed([(STEPS_GRADIENT + k, value) for k, value in enumerate(sums)])
    row = jnp.sum(row, axis=0, keepdims=True)
    rows_ref[...] = jnp.broadcast_to(row[None], rows_ref.shape)


def direction_kernel(
    rows_ref, gradient_ref, steps_ref, changes_ref, gradient_out, direction_out, direction_ref, semaphores
):
    written = pltpu.make_async_copy(gradient_ref, gradient_out, semaphores.at[0])
    written.start()
    row = jnp.broadcast_to(jnp.sum(rows_ref[...], axis=0), (8, LANES))
    lanes = lane_numbers()
    pairs = lax.broadcasted_iota(jnp.int32, (8, LANES), 0)

    def column(lane_of):
        picked = jnp.where(lanes == lane_of, row, 0.0)
        return jnp.broadcast_to(jnp.sum(picked, axis=1, keepdims=True), (8, LANES))

    def element(vector, i):
        return jnp.broadcast_to(vector[i : i + 1], (8, LANES))

    def square_lanes(j):
        low, high = jnp.minimum(pairs, j), jnp.maximum(pairs, j)
        return SQUARES + low * PAIRS - ((low * (low - 1)) >> 1) + high - low

    by_change = [column(pairs * PAIRS + i) for i in range(PAIRS)]
    by_step = [column(pairs + PAIRS * i) for i in range(PAIRS)]
    squares = [column(square_lanes(i)) for i in range(PAIRS)]
    curvs = column(pairs * (PAIRS + 1))
    steps_part = column(pairs + STEPS_GRADIENT)
    changes_part = column(pairs + CHANGES_GRADIENT)
    inverse = 1.0 / curvs
    scaling = element(curvs, PAIRS - 1) / element(squares[PAIRS - 1], PAIRS - 1)
    alphas = [None] * PAIRS
    for i in reversed(range(PAIRS)):
        alphas[i] = element(inverse * steps_part, i)
        steps_part = steps_part - alphas[i] * by_change[i]
        changes_part = changes_part - alphas[i] * squares[i]
    changes_part = scaling * changes_part
    weights = [None] * PAIRS
    for i in range(PAIRS):
        weights[i] = alphas[i] - element(inverse * changes_part, i)
        changes_part = changes_part + weights[i] * by_step[i]
    change_weights = [scaling * alpha for alpha in alphas]
    copies = []
    lons, pieces = gradient_ref.shape[0], 4
    for piece in range(pieces):
        at = slice(piece * lons // pieces, (piece + 1) * lons // pieces)
        for a, r, b in tiles(gradient_ref.shape):
            if at.start <= a < at.stop:
                value = -(scaling * gradient_ref[a, r, b])
                for i in range(PAIRS):
                    value = value + change_weights[i] * changes_ref[i, a, r, b]
                    value = value - weights[i] * steps_ref[i, a, r, b]
                direction_ref[a, r, b] = value
        if copies:
            copies[-1].start()
        copies.append(
            pltpu.make_async_copy(
                direction_ref.at[at], direction_out.at[at], semaphores.at[1 + piece]
            )
        )
    copies[-1].start()
    for copy in copies:
        copy.wait()
    written.wait()


def in_hbm(x):
    return pltpu.with_memory_space_constraint(x, pltpu.HBM)


def swapped(x, axis):
    return lax.ppermute(x, axis, [(0, 1), (1, 0)])


def cut_number():
    number = 0
    for axis in CUTS:
        number = number * lax.axis_size(axis) + lax.axis_index(axis)
    return number


def shards(kernels, steps, curvature):
    _, lons, rad_len, lats = kernels.shape
    rows = rad_len // 4
    block = ((lons, rows, lats), jnp.float32)
    size = lons * rows * lats
    half = ((RIM, rows, lats), jnp.float32)
    cuts, events = lax.axis_size(CUTS), lax.axis_size(EVENT)
    table = ((2 * rad_len, 2 * rad_len), jnp.bfloat16)
    flops = 4 * rad_len * kernels.size
    far_keep, far_pass, far_send_keep, far_send_pass, near_field, weights = call(
        far_radial_kernel,
        [half] * 4 + [((RIM, rad_len, lats), jnp.float32), table],
        flops,
        8 * kernels.size,
        in_specs=[pl.BlockSpec(memory_space=pltpu.HBM)],
        scratch_shapes=[
            pltpu.VMEM((RIM, rad_len, lats), jnp.float32),
            pltpu.SemaphoreType.DMA((2,)),
        ],
    )(in_hbm(kernels))
    far_core_pass = swapped(far_send_pass, "event_1")
    square = ((lats, lats), jnp.bfloat16)
    near_keep, near_pass, near_send_keep, near_send_pass, high, low = call(
        near_radial_kernel, [half] * 4 + [square] * 2, flops, 4 * kernels.size
    )(near_field, weights)
    far_passed = far_pass + far_core_pass
    far_chip = swapped(far_passed, "event_0")
    near_core_pass = swapped(near_send_pass, "event_1")
    near_chip = swapped(near_pass + near_core_pass, "event_0")
    far_core = swapped(far_send_keep, "event_1")
    near_core = swapped(near_send_keep, "event_1")
    (held_curvature,) = call(
        fetch_kernel,
        [(curvature.shape, jnp.float32)],
        0,
        8 * curvature.size,
        in_specs=[pl.BlockSpec(memory_space=pltpu.HBM)],
        scratch_shapes=[pltpu.SemaphoreType.DMA],
    )(in_hbm(curvature))
    cross = lax.ppermute(
        far_keep + far_core,
        CUTS_EVENT,
        [(e, e ^ 2) for e in range(events)] + [(d, d) for d in range(events, cuts * events)],
    )
    changes, gram = call(
        gram_kernel,
        [(steps.shape, jnp.float32), ((8, LANES), jnp.float32)],
        2 * 100 * size,
        12 * steps.size,
    )(steps, held_curvature)

    far_plane, far_out = call(far_latitude_kernel, [half] * 2, 4 * lats * size, 8 * size)(
        far_keep, far_core, far_chip, far_passed, cross, high, low
    )
    pairs = []
    for c in range(cuts):
        other, flip = (((c - 1) ^ 1) + 1) % cuts if c else cuts - 1, 2 if c == 0 else 0
        pairs += [(c * events + e, other * events + (e ^ flip)) for e in range(events)]
    far_halo = lax.ppermute(far_out, CUTS_EVENT, pairs)
    (near_plane,) = call(near_latitude_kernel, [half], 4 * lats * size, 8 * size)(
        near_keep, near_core, near_chip, high, low
    )
    near_halo = lax.ppermute(near_plane, CUTS, [(c, c ^ 1) for c in range(cuts)])
    gradient, outgoing = call(
        product_kernel,
        [block, ((cuts * events, 1, LANES), jnp.float32)],
        2 * 30 * size,
        4 * 20 * size,
        scratch_shapes=[pltpu.VMEM((4, RIM, rows, lats), jnp.float32)],
    )(far_halo, far_plane, near_plane, near_halo, steps, changes, gram)
    arrived = lax.all_to_all(outgoing, CUTS_EVENT, 0, 0, tiled=True)
    return call(
        direction_kernel,
        [block] * 2,
        2 * 17 * size,
        4 * 18 * size,
        out_specs=[pl.BlockSpec(memory_space=pltpu.HBM)] * 2,
        scratch_shapes=[pltpu.VMEM((lons, rows, lats), jnp.float32), pltpu.SemaphoreType.DMA((5,))],
    )(arrived, gradient, steps, changes)


def solution(mesh):
    torus = Mesh(
        mesh.devices.reshape(2, 4, 4, 2, 2), ("cuts_0", "cuts_1", "cuts_2", "event_0", "event_1")
    )
    in_specs = (P(EVENT, CUTS, None, None), P(None, CUTS, EVENT, None), P(None, CUTS, EVENT, None))
    out_specs = (P(CUTS, EVENT, None), P(CUTS, EVENT, None))
    return jax.shard_map(
        shards, mesh=torus, in_specs=in_specs, out_specs=out_specs, check_vma=False
    )
```

```python
import math

import jax
import jax.numpy as jnp
from jax import lax
from jax.experimental import pallas as pl
from jax.experimental.pallas import tpu as pltpu
from jax.sharding import Mesh
from jax.sharding import PartitionSpec as P

PAIRS = 8
RIM = 4
CUTS = ("cuts_0", "cuts_1", "cuts_2")
EVENT = ("event_0", "event_1")
CUTS_EVENT = ("cuts_0", "cuts_1", "cuts_2", "event_0", "event_1")
LANES = 128
SQUARES, STEPS_GRADIENT, CHANGES_GRADIENT = 64, 100, 108


def cycle_weights():
    unscaled = [math.exp(-((column - RIM) ** 2) / 4.5) for column in range(2 * RIM + 1)]
    whole = sum(unscaled)
    return [weight / whole for weight in unscaled]


def split(x):
    high = x.astype(jnp.bfloat16)
    low = (x - high.astype(jnp.float32)).astype(jnp.bfloat16)
    return high, low


def dot(a, b):
    return jnp.dot(a, b, preferred_element_type=jnp.float32)


def call(kernel, outs, flops, moved, limit=16, **options):
    return pl.pallas_call(
        kernel,
        out_shape=[jax.ShapeDtypeStruct(*out) for out in outs],
        compiler_params=pltpu.CompilerParams(vmem_limit_bytes=limit << 20),
        cost_estimate=pl.CostEstimate(flops=flops, bytes_accessed=moved, transcendentals=0),
        **options,
    )


def gauss_rows(length, sigma, rows, axis):
    offset = (rows - lax.broadcasted_iota(jnp.int32, rows.shape, axis)).astype(jnp.float32)
    matrix = jnp.exp(-offset * offset / (2.0 * sigma * sigma))
    return matrix / jnp.sum(matrix, axis=axis, keepdims=True)


def gauss_rows(length, sigma, rows, axis):
    offset = (rows - lax.broadcasted_iota(jnp.int32, rows.shape, axis)).astype(jnp.float32)
    matrix = jnp.exp(-offset * offset / (2.0 * sigma * sigma))
    return matrix / jnp.sum(matrix, axis=axis, keepdims=True)


def radial_products(field_ref, weights, keep_ref, pass_ref, send_keep_ref, send_pass_ref):
    for a in range(field_ref.shape[0]):
        both = dot(weights, jnp.concatenate(split(field_ref[a]), axis=0))
        length = both.shape[0] // 2
        rows = length // 4
        out = both[:length] + both[length:]
        for k, ref in enumerate((keep_ref, pass_ref, send_keep_ref, send_pass_ref)):
            ref[a] = out[k * rows : (k + 1) * rows]


def far_radial_kernel(
    kernels_ref, keep_ref, pass_ref, send_keep_ref, send_pass_ref, near_ref, weights_ref, far_ref, semaphores
):
    length = kernels_ref.shape[2]
    odd = lax.rem(cut_number(), 2)
    copies = []
    for piece, ref in enumerate((far_ref, near_ref)):
        source = kernels_ref.at[0, pl.ds(RIM * (odd ^ piece), RIM)]
        copies.append(pltpu.make_async_copy(source, ref, semaphores.at[piece]))
        copies[piece].start()
    part = 2 * lax.axis_index("event_0") + lax.axis_index("event_1")
    rows = length // 4
    local = lax.broadcasted_iota(jnp.int32, (rows, length), 0)

    def weights_of(first):
        order = [first, first ^ 2, first ^ 1, first ^ 3]
        matrix = jnp.concatenate(
            [gauss_rows(length, 3.0, local + rows * block, 1) for block in order], axis=0
        )
        return jnp.concatenate([jnp.concatenate([m, m], axis=1) for m in split(matrix)], axis=0)

    weights = weights_of(jnp.where(cut_number() == 0, part ^ 2, part))
    weights_ref[...] = weights_of(part)
    copies[0].wait()
    radial_products(far_ref, weights, keep_ref, pass_ref, send_keep_ref, send_pass_ref)
    copies[1].wait()


def near_radial_kernel(near_ref, weights_ref, keep_ref, pass_ref, send_keep_ref, send_pass_ref):
    radial_products(near_ref, weights_ref[...], keep_ref, pass_ref, send_keep_ref, send_pass_ref)


def smoothed(field, high, low):
    count = field.shape[0]
    both = jnp.concatenate(split(field), axis=0)
    out = dot(both, high) + dot(both, low)
    return out[:count] + out[count:]


def fetch_kernel(curvature_ref, held_ref, high_ref, low_ref, semaphore):
    copy = pltpu.make_async_copy(curvature_ref, held_ref, semaphore)
    copy.start()
    lats = high_ref.shape[0]
    column = lax.broadcasted_iota(jnp.int32, (lats, lats), 1)
    high_ref[...], low_ref[...] = split(gauss_rows(lats, 4.0, column, 0))
    copy.wait()


def latitude_kernel(keep_ref, core_ref, chip_ref, high_ref, low_ref, plane_ref):
    lons, rows, lats = plane_ref.shape
    summed = (keep_ref[...] + core_ref[...] + chip_ref[...]).reshape(lons * rows, lats)
    plane_ref[...] = smoothed(summed, high_ref[...], low_ref[...]).reshape(lons, rows, lats)


def lane_numbers():
    return lax.broadcasted_iota(jnp.int32, (8, LANES), 1)


def tiles(shape):
    return [
        (a, slice(8 * r, 8 * r + 8), slice(LANES * b, LANES * (b + 1)))
        for r in range(shape[1] // 8)
        for b in range(shape[2] // LANES)
        for a in range(shape[0])
    ]


def placed(sums):
    lanes = lane_numbers()
    row = jnp.zeros((8, LANES), jnp.float32)
    for lane, value in sums:
        row = row + jnp.where(lanes == lane, jnp.sum(value, axis=1, keepdims=True), 0.0)
    return row


def gram_kernel(steps_ref, curvature_ref, changes_ref, row_ref):
    lons, rows, lats = steps_ref.shape[1:]
    spots = [
        (slice(8 * r, 8 * r + 8), slice(LANES * b, LANES * (b + 1)))
        for r in range(rows // 8)
        for b in range(lats // LANES)
    ]
    half = PAIRS // 2
    upper = [(i, j) for i in range(PAIRS) for j in range(i, PAIRS)]

    def first(a, sums):
        for at in spots:
            steps = [steps_ref[(i, a, *at)] for i in range(half)]
            changes = [None] * PAIRS
            for i in range(PAIRS):
                step = steps[i] if i < half else steps_ref[(i, a, *at)]
                changes[i] = curvature_ref[(i, a, *at)] * step
                changes_ref[(i, a, *at)] = changes[i]
            sums = [sums[k] + steps[k // PAIRS] * changes[k % PAIRS] for k in range(half * PAIRS)]
        return sums

    def second(a, sums):
        for at in spots:
            steps = [steps_ref[(i, a, *at)] for i in range(half, PAIRS)]
            changes = [changes_ref[(i, a, *at)] for i in range(PAIRS)]
            sums = [sums[k] + steps[k // PAIRS] * changes[k % PAIRS] for k in range(half * PAIRS)]
        return sums

    def third(a, sums):
        for at in spots:
            changes = [changes_ref[(i, a, *at)] for i in range(PAIRS)]
            sums = [value + changes[i] * changes[j] for value, (i, j) in zip(sums, upper)]
        return sums

    zero = jnp.zeros((8, LANES), jnp.float32)
    row = zero
    for start, step, size in ((0, first, 32), (32, second, 32), (SQUARES, third, len(upper))):
        sums = lax.fori_loop(0, lons, step, [zero] * size)
        row = row + placed([(start + k, value) for k, value in enumerate(sums)])
    row_ref[...] = row


def product_kernel(
    far_halo_ref, far_ref, near_ref, near_halo_ref,
    steps_ref, changes_ref, gram_ref, gradient_ref, rows_ref, padded_ref,
):
    lons, rows, lats = gradient_ref.shape
    weights = cycle_weights()
    mirror = 3 * lax.rem(cut_number(), 2)
    for k, ref in enumerate((far_halo_ref, far_ref, near_ref, near_halo_ref)):
        padded_ref[k ^ mirror] = ref[...]
    sums = [jnp.zeros((8, LANES), jnp.float32) for _ in range(2 * PAIRS)]
    for r in range(rows // 8):
        for b in range(lats // LANES):
            at = (slice(8 * r, 8 * r + 8), slice(LANES * b, LANES * (b + 1)))
            padded = [padded_ref[(k, a, *at)] for k in range(4) for a in range(RIM)]
            for a in range(lons):
                value = weights[RIM] * padded[a + RIM]
                for k in range(RIM):
                    value = value + weights[k] * (padded[a + k] + padded[a + 2 * RIM - k])
                gradient_ref[(a, *at)] = value
                for pair in range(PAIRS):
                    sums[pair] = sums[pair] + steps_ref[(pair, a, *at)] * value
                    sums[PAIRS + pair] = sums[PAIRS + pair] + changes_ref[(pair, a, *at)] * value
    row = gram_ref[...] + placed([(STEPS_GRADIENT + k, value) for k, value in enumerate(sums)])
    row = jnp.sum(row, axis=0, keepdims=True)
    rows_ref[...] = jnp.broadcast_to(row[None], rows_ref.shape)


def direction_kernel(
    rows_ref, gradient_ref, steps_ref, changes_ref, gradient_out, direction_out, direction_ref, semaphores
):
    written = pltpu.make_async_copy(gradient_ref, gradient_out, semaphores.at[0])
    written.start()
    row = jnp.broadcast_to(jnp.sum(rows_ref[...], axis=0), (8, LANES))
    lanes = lane_numbers()
    pairs = lax.broadcasted_iota(jnp.int32, (8, LANES), 0)

    def column(lane_of):
        picked = jnp.where(lanes == lane_of, row, 0.0)
        return jnp.broadcast_to(jnp.sum(picked, axis=1, keepdims=True), (8, LANES))

    def element(vector, i):
        return jnp.broadcast_to(vector[i : i + 1], (8, LANES))

    def square_lanes(j):
        low, high = jnp.minimum(pairs, j), jnp.maximum(pairs, j)
        return SQUARES + low * PAIRS - ((low * (low - 1)) >> 1) + high - low

    by_change = [column(pairs * PAIRS + i) for i in range(PAIRS)]
    by_step = [column(pairs + PAIRS * i) for i in range(PAIRS)]
    squares = [column(square_lanes(i)) for i in range(PAIRS)]
    curvs = column(pairs * (PAIRS + 1))
    steps_part = column(pairs + STEPS_GRADIENT)
    changes_part = column(pairs + CHANGES_GRADIENT)
    inverse = 1.0 / curvs
    scaling = element(curvs, PAIRS - 1) / element(squares[PAIRS - 1], PAIRS - 1)
    alphas = [None] * PAIRS
    for i in reversed(range(PAIRS)):
        alphas[i] = element(inverse * steps_part, i)
        steps_part = steps_part - alphas[i] * by_change[i]
        changes_part = changes_part - alphas[i] * squares[i]
    changes_part = scaling * changes_part
    weights = [None] * PAIRS
    for i in range(PAIRS):
        weights[i] = alphas[i] - element(inverse * changes_part, i)
        changes_part = changes_part + weights[i] * by_step[i]
    change_weights = [scaling * alpha for alpha in alphas]
    copies = []
    lons, pieces = gradient_ref.shape[0], 4
    for piece in range(pieces):
        at = slice(piece * lons // pieces, (piece + 1) * lons // pieces)
        for a, r, b in tiles(gradient_ref.shape):
            if at.start <= a < at.stop:
                value = -(scaling * gradient_ref[a, r, b])
                for i in range(PAIRS):
                    value = value + change_weights[i] * changes_ref[i, a, r, b]
                    value = value - weights[i] * steps_ref[i, a, r, b]
                direction_ref[a, r, b] = value
        if copies:
            copies[-1].start()
        copies.append(
            pltpu.make_async_copy(
                direction_ref.at[at], direction_out.at[at], semaphores.at[1 + piece]
            )
        )
    copies[-1].start()
    for copy in copies:
        copy.wait()
    written.wait()


def in_hbm(x):
    return pltpu.with_memory_space_constraint(x, pltpu.HBM)


def swapped(x, axis):
    return lax.ppermute(x, axis, [(0, 1), (1, 0)])


def cut_number():
    number = 0
    for axis in CUTS:
        number = number * lax.axis_size(axis) + lax.axis_index(axis)
    return number


def shards(kernels, steps, curvature):
    _, lons, rad_len, lats = kernels.shape
    rows = rad_len // 4
    block = ((lons, rows, lats), jnp.float32)
    size = lons * rows * lats
    half = ((RIM, rows, lats), jnp.float32)
    cuts, events = lax.axis_size(CUTS), lax.axis_size(EVENT)
    table = ((2 * rad_len, 2 * rad_len), jnp.bfloat16)
    flops = 4 * rad_len * kernels.size
    far_keep, far_pass, far_send_keep, far_send_pass, near_field, weights = call(
        far_radial_kernel,
        [half] * 4 + [((RIM, rad_len, lats), jnp.float32), table],
        flops,
        8 * kernels.size,
        in_specs=[pl.BlockSpec(memory_space=pltpu.HBM)],
        scratch_shapes=[
            pltpu.VMEM((RIM, rad_len, lats), jnp.float32),
            pltpu.SemaphoreType.DMA((2,)),
        ],
    )(in_hbm(kernels))
    far_core_pass = swapped(far_send_pass, "event_1")
    near_keep, near_pass, near_send_keep, near_send_pass = call(
        near_radial_kernel, [half] * 4, flops, 4 * kernels.size
    )(near_field, weights)
    far_chip = swapped(far_pass + far_core_pass, "event_0")
    near_core_pass = swapped(near_send_pass, "event_1")
    square = ((lats, lats), jnp.bfloat16)
    held_curvature, high, low = call(
        fetch_kernel,
        [(curvature.shape, jnp.float32), square, square],
        10 * lats * lats,
        8 * curvature.size,
        in_specs=[pl.BlockSpec(memory_space=pltpu.HBM)],
        scratch_shapes=[pltpu.SemaphoreType.DMA],
    )(in_hbm(curvature))
    near_chip = swapped(near_pass + near_core_pass, "event_0")
    far_core = swapped(far_send_keep, "event_1")
    near_core = swapped(near_send_keep, "event_1")
    changes, gram = call(
        gram_kernel,
        [(steps.shape, jnp.float32), ((8, LANES), jnp.float32)],
        2 * 100 * size,
        12 * steps.size,
    )(steps, held_curvature)

    def plane_of(*parts):
        return call(latitude_kernel, [half], 4 * lats * size, 8 * size)(*parts, high, low)[0]

    far_plane = plane_of(far_keep, far_core, far_chip)
    pairs = []
    for c in range(cuts):
        other, flip = (((c - 1) ^ 1) + 1) % cuts if c else cuts - 1, 2 if c == 0 else 0
        pairs += [(c * events + e, other * events + (e ^ flip)) for e in range(events)]
    far_halo = lax.ppermute(far_plane, CUTS_EVENT, pairs)
    far_plane = lax.ppermute(
        far_plane,
        CUTS_EVENT,
        [(e, e ^ 2) for e in range(events)] + [(d, d) for d in range(events, cuts * events)],
    )
    near_plane = plane_of(near_keep, near_core, near_chip)
    near_halo = lax.ppermute(near_plane, CUTS, [(c, c ^ 1) for c in range(cuts)])
    gradient, outgoing = call(
        product_kernel,
        [block, ((cuts * events, 1, LANES), jnp.float32)],
        2 * 30 * size,
        4 * 20 * size,
        scratch_shapes=[pltpu.VMEM((4, RIM, rows, lats), jnp.float32)],
    )(far_halo, far_plane, near_plane, near_halo, steps, changes, gram)
    arrived = lax.all_to_all(outgoing, CUTS_EVENT, 0, 0, tiled=True)
    return call(
        direction_kernel,
        [block] * 2,
        2 * 17 * size,
        4 * 18 * size,
        out_specs=[pl.BlockSpec(memory_space=pltpu.HBM)] * 2,
        scratch_shapes=[pltpu.VMEM((lons, rows, lats), jnp.float32), pltpu.SemaphoreType.DMA((5,))],
    )(arrived, gradient, steps, changes)


def solution(mesh):
    torus = Mesh(
        mesh.devices.reshape(2, 4, 4, 2, 2), ("cuts_0", "cuts_1", "cuts_2", "event_0", "event_1")
    )
    in_specs = (P(EVENT, CUTS, None, None), P(None, CUTS, EVENT, None), P(None, CUTS, EVENT, None))
    out_specs = (P(CUTS, EVENT, None), P(CUTS, EVENT, None))
    return jax.shard_map(
        shards, mesh=torus, in_specs=in_specs, out_specs=out_specs, check_vma=False
    )
```

```python
import functools
import math

import jax
import jax.numpy as jnp
from jax import lax
from jax.experimental import pallas as pl
from jax.experimental.pallas import tpu as pltpu
from jax.sharding import Mesh
from jax.sharding import PartitionSpec as P

PAIRS = 8
RIM = 4
CUTS = ("cuts_0", "cuts_1", "cuts_2")
EVENT = ("event_0", "event_1")
CUTS_EVENT = ("cuts_0", "cuts_1", "cuts_2", "event_0", "event_1")
LANES = 128
SQUARES, STEPS_GRADIENT, CHANGES_GRADIENT = 64, 100, 108


def cycle_weights():
    unscaled = [math.exp(-((column - RIM) ** 2) / 4.5) for column in range(2 * RIM + 1)]
    whole = sum(unscaled)
    return [weight / whole for weight in unscaled]


def split(x):
    high = x.astype(jnp.bfloat16)
    low = (x - high.astype(jnp.float32)).astype(jnp.bfloat16)
    return high, low


def dot(a, b):
    return jnp.dot(a, b, preferred_element_type=jnp.float32)


def call(kernel, outs, flops, moved, limit=16, **options):
    return pl.pallas_call(
        kernel,
        out_shape=[jax.ShapeDtypeStruct(*out) for out in outs],
        compiler_params=pltpu.CompilerParams(vmem_limit_bytes=limit << 20),
        cost_estimate=pl.CostEstimate(flops=flops, bytes_accessed=moved, transcendentals=0),
        **options,
    )


def gauss_rows(length, sigma, rows, axis):
    offset = (rows - lax.broadcasted_iota(jnp.int32, rows.shape, axis)).astype(jnp.float32)
    matrix = jnp.exp(-offset * offset / (2.0 * sigma * sigma))
    return matrix / jnp.sum(matrix, axis=axis, keepdims=True)


def gauss_rows(length, sigma, rows, axis):
    offset = (rows - lax.broadcasted_iota(jnp.int32, rows.shape, axis)).astype(jnp.float32)
    matrix = jnp.exp(-offset * offset / (2.0 * sigma * sigma))
    return matrix / jnp.sum(matrix, axis=axis, keepdims=True)


def radial_products(field_ref, weights, keep_ref, pass_ref, send_keep_ref, send_pass_ref):
    for a in range(field_ref.shape[0]):
        both = dot(weights, jnp.concatenate(split(field_ref[a]), axis=0))
        length = both.shape[0] // 2
        rows = length // 4
        out = both[:length] + both[length:]
        for k, ref in enumerate((keep_ref, pass_ref, send_keep_ref, send_pass_ref)):
            ref[a] = out[k * rows : (k + 1) * rows]


def far_radial_kernel(
    kernels_ref, keep_ref, pass_ref, send_keep_ref, send_pass_ref, near_ref, weights_ref, far_ref, semaphores
):
    length = kernels_ref.shape[2]
    odd = lax.rem(cut_number(), 2)
    copies = []
    for piece, ref in enumerate((far_ref, near_ref)):
        source = kernels_ref.at[0, pl.ds(RIM * (odd ^ piece), RIM)]
        copies.append(pltpu.make_async_copy(source, ref, semaphores.at[piece]))
        copies[piece].start()
    part = 2 * lax.axis_index("event_0") + lax.axis_index("event_1")
    rows = length // 4
    local = lax.broadcasted_iota(jnp.int32, (rows, length), 0)

    def weights_of(first):
        order = [first, first ^ 2, first ^ 1, first ^ 3]
        matrix = jnp.concatenate(
            [gauss_rows(length, 3.0, local + rows * block, 1) for block in order], axis=0
        )
        return jnp.concatenate([jnp.concatenate([m, m], axis=1) for m in split(matrix)], axis=0)

    weights = weights_of(jnp.where(cut_number() == 0, part ^ 2, part))
    weights_ref[...] = weights_of(part)
    copies[0].wait()
    radial_products(far_ref, weights, keep_ref, pass_ref, send_keep_ref, send_pass_ref)
    copies[1].wait()


def near_radial_kernel(
    near_ref, weights_ref, far_send_keep_ref, keep_ref, pass_ref, rest_ref, high_ref, low_ref
):
    rest_ref[2] = far_send_keep_ref[...]
    parts = (keep_ref, pass_ref, rest_ref.at[1], rest_ref.at[0])
    radial_products(near_ref, weights_ref[...], *parts)
    lats = high_ref.shape[0]
    column = lax.broadcasted_iota(jnp.int32, (lats, lats), 1)
    high_ref[...], low_ref[...] = split(gauss_rows(lats, 4.0, column, 0))


def smoothed(field, high, low):
    count = field.shape[0]
    both = jnp.concatenate(split(field), axis=0)
    out = dot(both, high) + dot(both, low)
    return out[:count] + out[count:]


def latitude_kernel(slot, keep_ref, rest_ref, chip_ref, high_ref, low_ref, plane_ref):
    lons, rows, lats = plane_ref.shape
    summed = (keep_ref[...] + rest_ref[slot] + chip_ref[...]).reshape(lons * rows, lats)
    plane_ref[...] = smoothed(summed, high_ref[...], low_ref[...]).reshape(lons, rows, lats)


def lane_numbers():
    return lax.broadcasted_iota(jnp.int32, (8, LANES), 1)


def tiles(shape):
    return [
        (a, slice(8 * r, 8 * r + 8), slice(LANES * b, LANES * (b + 1)))
        for r in range(shape[1] // 8)
        for b in range(shape[2] // LANES)
        for a in range(shape[0])
    ]


def placed(sums):
    lanes = lane_numbers()
    row = jnp.zeros((8, LANES), jnp.float32)
    for lane, value in sums:
        row = row + jnp.where(lanes == lane, jnp.sum(value, axis=1, keepdims=True), 0.0)
    return row


def gram_kernel(steps_ref, curvature_hbm, changes_ref, row_ref, curvature_ref, semaphores):
    lons, rows, lats = steps_ref.shape[1:]

    def fetch(a):
        return pltpu.make_async_copy(
            curvature_hbm.at[:, a], curvature_ref.at[:, a], semaphores.at[a]
        )

    for a in range(lons):
        fetch(a).start()
    spots = [
        (slice(8 * r, 8 * r + 8), slice(LANES * b, LANES * (b + 1)))
        for r in range(rows // 8)
        for b in range(lats // LANES)
    ]
    half = PAIRS // 2
    upper = [(i, j) for i in range(PAIRS) for j in range(i, PAIRS)]

    def first(a, sums):
        fetch(a).wait()
        for at in spots:
            steps = [steps_ref[(i, a, *at)] for i in range(half)]
            changes = [None] * PAIRS
            for i in range(PAIRS):
                step = steps[i] if i < half else steps_ref[(i, a, *at)]
                changes[i] = curvature_ref[(i, a, *at)] * step
                changes_ref[(i, a, *at)] = changes[i]
            sums = [sums[k] + steps[k // PAIRS] * changes[k % PAIRS] for k in range(half * PAIRS)]
        return sums

    def second(a, sums):
        for at in spots:
            steps = [steps_ref[(i, a, *at)] for i in range(half, PAIRS)]
            changes = [changes_ref[(i, a, *at)] for i in range(PAIRS)]
            sums = [sums[k] + steps[k // PAIRS] * changes[k % PAIRS] for k in range(half * PAIRS)]
        return sums

    def third(a, sums):
        for at in spots:
            changes = [changes_ref[(i, a, *at)] for i in range(PAIRS)]
            sums = [value + changes[i] * changes[j] for value, (i, j) in zip(sums, upper)]
        return sums

    zero = jnp.zeros((8, LANES), jnp.float32)
    row = zero
    for start, step, size in ((0, first, 32), (32, second, 32), (SQUARES, third, len(upper))):
        sums = lax.fori_loop(0, lons, step, [zero] * size)
        row = row + placed([(start + k, value) for k, value in enumerate(sums)])
    row_ref[...] = row


def product_kernel(
    far_halo_ref, far_ref, near_ref, near_halo_ref,
    steps_ref, changes_ref, gram_ref, gradient_ref, rows_ref, padded_ref,
):
    lons, rows, lats = gradient_ref.shape
    weights = cycle_weights()
    mirror = 3 * lax.rem(cut_number(), 2)
    for k, ref in enumerate((far_halo_ref, far_ref, near_ref, near_halo_ref)):
        padded_ref[k ^ mirror] = ref[...]
    sums = [jnp.zeros((8, LANES), jnp.float32) for _ in range(2 * PAIRS)]
    for r in range(rows // 8):
        for b in range(lats // LANES):
            at = (slice(8 * r, 8 * r + 8), slice(LANES * b, LANES * (b + 1)))
            padded = [padded_ref[(k, a, *at)] for k in range(4) for a in range(RIM)]
            for a in range(lons):
                value = weights[RIM] * padded[a + RIM]
                for k in range(RIM):
                    value = value + weights[k] * (padded[a + k] + padded[a + 2 * RIM - k])
                gradient_ref[(a, *at)] = value
                for pair in range(PAIRS):
                    sums[pair] = sums[pair] + steps_ref[(pair, a, *at)] * value
                    sums[PAIRS + pair] = sums[PAIRS + pair] + changes_ref[(pair, a, *at)] * value
    row = gram_ref[...] + placed([(STEPS_GRADIENT + k, value) for k, value in enumerate(sums)])
    row = jnp.sum(row, axis=0, keepdims=True)
    rows_ref[...] = jnp.broadcast_to(row[None], rows_ref.shape)


def direction_kernel(
    rows_ref, gradient_ref, steps_ref, changes_ref, gradient_out, direction_out, direction_ref, semaphores
):
    written = pltpu.make_async_copy(gradient_ref, gradient_out, semaphores.at[0])
    written.start()
    row = jnp.broadcast_to(jnp.sum(rows_ref[...], axis=0), (8, LANES))
    lanes = lane_numbers()
    pairs = lax.broadcasted_iota(jnp.int32, (8, LANES), 0)

    def column(lane_of):
        picked = jnp.where(lanes == lane_of, row, 0.0)
        return jnp.broadcast_to(jnp.sum(picked, axis=1, keepdims=True), (8, LANES))

    def element(vector, i):
        return jnp.broadcast_to(vector[i : i + 1], (8, LANES))

    def square_lanes(j):
        low, high = jnp.minimum(pairs, j), jnp.maximum(pairs, j)
        return SQUARES + low * PAIRS - ((low * (low - 1)) >> 1) + high - low

    by_change = [column(pairs * PAIRS + i) for i in range(PAIRS)]
    by_step = [column(pairs + PAIRS * i) for i in range(PAIRS)]
    squares = [column(square_lanes(i)) for i in range(PAIRS)]
    curvs = column(pairs * (PAIRS + 1))
    steps_part = column(pairs + STEPS_GRADIENT)
    changes_part = column(pairs + CHANGES_GRADIENT)
    inverse = 1.0 / curvs
    scaling = element(curvs, PAIRS - 1) / element(squares[PAIRS - 1], PAIRS - 1)
    alphas = [None] * PAIRS
    for i in reversed(range(PAIRS)):
        alphas[i] = element(inverse * steps_part, i)
        steps_part = steps_part - alphas[i] * by_change[i]
        changes_part = changes_part - alphas[i] * squares[i]
    changes_part = scaling * changes_part
    weights = [None] * PAIRS
    for i in range(PAIRS):
        weights[i] = alphas[i] - element(inverse * changes_part, i)
        changes_part = changes_part + weights[i] * by_step[i]
    change_weights = [scaling * alpha for alpha in alphas]
    copies = []
    lons, pieces = gradient_ref.shape[0], 4
    for piece in range(pieces):
        at = slice(piece * lons // pieces, (piece + 1) * lons // pieces)
        for a, r, b in tiles(gradient_ref.shape):
            if at.start <= a < at.stop:
                value = -(scaling * gradient_ref[a, r, b])
                for i in range(PAIRS):
                    value = value + change_weights[i] * changes_ref[i, a, r, b]
                    value = value - weights[i] * steps_ref[i, a, r, b]
                direction_ref[a, r, b] = value
        if copies:
            copies[-1].start()
        copies.append(
            pltpu.make_async_copy(
                direction_ref.at[at], direction_out.at[at], semaphores.at[1 + piece]
            )
        )
    copies[-1].start()
    for copy in copies:
        copy.wait()
    written.wait()


def in_hbm(x):
    return pltpu.with_memory_space_constraint(x, pltpu.HBM)


def swapped(x, axis):
    return lax.ppermute(x, axis, [(0, 1), (1, 0)])


def cut_number():
    number = 0
    for axis in CUTS:
        number = number * lax.axis_size(axis) + lax.axis_index(axis)
    return number


def shards(kernels, steps, curvature):
    _, lons, rad_len, lats = kernels.shape
    rows = rad_len // 4
    block = ((lons, rows, lats), jnp.float32)
    size = lons * rows * lats
    half = ((RIM, rows, lats), jnp.float32)
    cuts, events = lax.axis_size(CUTS), lax.axis_size(EVENT)
    table = ((2 * rad_len, 2 * rad_len), jnp.bfloat16)
    flops = 4 * rad_len * kernels.size
    far_keep, far_pass, far_send_keep, far_send_pass, near_field, weights = call(
        far_radial_kernel,
        [half] * 4 + [((RIM, rad_len, lats), jnp.float32), table],
        flops,
        8 * kernels.size,
        in_specs=[pl.BlockSpec(memory_space=pltpu.HBM)],
        scratch_shapes=[
            pltpu.VMEM((RIM, rad_len, lats), jnp.float32),
            pltpu.SemaphoreType.DMA((2,)),
        ],
    )(in_hbm(kernels))
    far_core_pass = swapped(far_send_pass, "event_1")
    square = ((lats, lats), jnp.bfloat16)
    near_keep, near_pass, rest, high, low = call(
        near_radial_kernel,
        [half, half, ((3, RIM, rows, lats), jnp.float32), square, square],
        flops,
        4 * kernels.size,
    )(near_field, weights, far_send_keep)
    far_chip = swapped(far_pass + far_core_pass, "event_0")
    rest = swapped(rest, "event_1")
    near_chip = swapped(near_pass + rest[0], "event_0")
    changes, gram = call(
        gram_kernel,
        [(steps.shape, jnp.float32), ((8, LANES), jnp.float32)],
        2 * 100 * size,
        12 * steps.size,
        in_specs=[pl.BlockSpec(memory_space=pltpu.VMEM), pl.BlockSpec(memory_space=pltpu.HBM)],
        scratch_shapes=[pltpu.VMEM(curvature.shape, jnp.float32), pltpu.SemaphoreType.DMA((lons,))],
    )(steps, in_hbm(curvature))

    def plane_of(slot, *parts):
        kernel = functools.partial(latitude_kernel, slot)
        return call(kernel, [half], 4 * lats * size, 8 * size)(*parts, high, low)[0]

    far_plane = plane_of(2, far_keep, rest, far_chip)
    pairs = []
    for c in range(cuts):
        other, flip = (((c - 1) ^ 1) + 1) % cuts if c else cuts - 1, 2 if c == 0 else 0
        pairs += [(c * events + e, other * events + (e ^ flip)) for e in range(events)]
    far_halo = lax.ppermute(far_plane, CUTS_EVENT, pairs)
    far_plane = lax.ppermute(
        far_plane,
        CUTS_EVENT,
        [(e, e ^ 2) for e in range(events)] + [(d, d) for d in range(events, cuts * events)],
    )
    near_plane = plane_of(1, near_keep, rest, near_chip)
    near_halo = lax.ppermute(near_plane, CUTS, [(c, c ^ 1) for c in range(cuts)])
    gradient, outgoing = call(
        product_kernel,
        [block, ((cuts * events, 1, LANES), jnp.float32)],
        2 * 30 * size,
        4 * 20 * size,
        scratch_shapes=[pltpu.VMEM((4, RIM, rows, lats), jnp.float32)],
    )(far_halo, far_plane, near_plane, near_halo, steps, changes, gram)
    arrived = lax.all_to_all(outgoing, CUTS_EVENT, 0, 0, tiled=True)
    return call(
        direction_kernel,
        [block] * 2,
        2 * 17 * size,
        4 * 18 * size,
        out_specs=[pl.BlockSpec(memory_space=pltpu.HBM)] * 2,
        scratch_shapes=[pltpu.VMEM((lons, rows, lats), jnp.float32), pltpu.SemaphoreType.DMA((5,))],
    )(arrived, gradient, steps, changes)


def solution(mesh):
    torus = Mesh(
        mesh.devices.reshape(2, 4, 4, 2, 2), ("cuts_0", "cuts_1", "cuts_2", "event_0", "event_1")
    )
    in_specs = (P(EVENT, CUTS, None, None), P(None, CUTS, EVENT, None), P(None, CUTS, EVENT, None))
    out_specs = (P(CUTS, EVENT, None), P(CUTS, EVENT, None))
    return jax.shard_map(
        shards, mesh=torus, in_specs=in_specs, out_specs=out_specs, check_vma=False
    )
```

```python
import functools
import math

import jax
import jax.numpy as jnp
from jax import lax
from jax.experimental import pallas as pl
from jax.experimental.pallas import tpu as pltpu
from jax.sharding import Mesh
from jax.sharding import PartitionSpec as P

PAIRS = 8
RIM = 4
CUTS = ("cuts_0", "cuts_1", "cuts_2")
EVENT = ("event_0", "event_1")
CUTS_EVENT = ("cuts_0", "cuts_1", "cuts_2", "event_0", "event_1")
LANES = 128
SQUARES, STEPS_GRADIENT, CHANGES_GRADIENT = 64, 100, 108


def cycle_weights():
    unscaled = [math.exp(-((column - RIM) ** 2) / 4.5) for column in range(2 * RIM + 1)]
    whole = sum(unscaled)
    return [weight / whole for weight in unscaled]


def split(x):
    high = x.astype(jnp.bfloat16)
    low = (x - high.astype(jnp.float32)).astype(jnp.bfloat16)
    return high, low


def dot(a, b):
    return jnp.dot(a, b, preferred_element_type=jnp.float32)


def call(kernel, outs, flops, moved, limit=16, **options):
    return pl.pallas_call(
        kernel,
        out_shape=[jax.ShapeDtypeStruct(*out) for out in outs],
        compiler_params=pltpu.CompilerParams(vmem_limit_bytes=limit << 20),
        cost_estimate=pl.CostEstimate(flops=flops, bytes_accessed=moved, transcendentals=0),
        **options,
    )


def gauss_rows(length, sigma, rows, axis):
    offset = (rows - lax.broadcasted_iota(jnp.int32, rows.shape, axis)).astype(jnp.float32)
    matrix = jnp.exp(-offset * offset / (2.0 * sigma * sigma))
    return matrix / jnp.sum(matrix, axis=axis, keepdims=True)


def gauss_rows(length, sigma, rows, axis):
    offset = (rows - lax.broadcasted_iota(jnp.int32, rows.shape, axis)).astype(jnp.float32)
    matrix = jnp.exp(-offset * offset / (2.0 * sigma * sigma))
    return matrix / jnp.sum(matrix, axis=axis, keepdims=True)


def radial_products(field_ref, weights, keep_ref, pass_ref, send_keep_ref, send_pass_ref):
    for a in range(field_ref.shape[0]):
        both = dot(weights, jnp.concatenate(split(field_ref[a]), axis=0))
        length = both.shape[0] // 2
        rows = length // 4
        out = both[:length] + both[length:]
        for k, ref in enumerate((keep_ref, pass_ref, send_keep_ref, send_pass_ref)):
            ref[a] = out[k * rows : (k + 1) * rows]


def far_radial_kernel(
    kernels_ref, keep_ref, pass_ref, send_keep_ref, send_pass_ref, near_ref, weights_ref, far_ref, semaphores
):
    length = kernels_ref.shape[2]
    odd = lax.rem(cut_number(), 2)
    copies = []
    for piece, ref in enumerate((far_ref, near_ref)):
        source = kernels_ref.at[0, pl.ds(RIM * (odd ^ piece), RIM)]
        copies.append(pltpu.make_async_copy(source, ref, semaphores.at[piece]))
        copies[piece].start()
    part = 2 * lax.axis_index("event_0") + lax.axis_index("event_1")
    rows = length // 4
    local = lax.broadcasted_iota(jnp.int32, (rows, length), 0)

    def weights_of(first):
        order = [first, first ^ 2, first ^ 1, first ^ 3]
        matrix = jnp.concatenate(
            [gauss_rows(length, 3.0, local + rows * block, 1) for block in order], axis=0
        )
        return jnp.concatenate([jnp.concatenate([m, m], axis=1) for m in split(matrix)], axis=0)

    weights = weights_of(jnp.where(cut_number() == 0, part ^ 2, part))
    weights_ref[...] = weights_of(part)
    copies[0].wait()
    radial_products(far_ref, weights, keep_ref, pass_ref, send_keep_ref, send_pass_ref)
    copies[1].wait()


def near_radial_kernel(
    near_ref, weights_ref, far_send_keep_ref, keep_ref, pass_ref, rest_ref, high_ref, low_ref
):
    rest_ref[2] = far_send_keep_ref[...]
    parts = (keep_ref, pass_ref, rest_ref.at[1], rest_ref.at[0])
    radial_products(near_ref, weights_ref[...], *parts)
    lats = high_ref.shape[0]
    column = lax.broadcasted_iota(jnp.int32, (lats, lats), 1)
    high_ref[...], low_ref[...] = split(gauss_rows(lats, 4.0, column, 0))


def smoothed(field, high, low):
    count = field.shape[0]
    both = jnp.concatenate(split(field), axis=0)
    out = dot(both, high) + dot(both, low)
    return out[:count] + out[count:]


def latitude_kernel(slot, keep_ref, rest_ref, chip_ref, high_ref, low_ref, plane_ref):
    lons, rows, lats = plane_ref.shape
    summed = (keep_ref[...] + rest_ref[slot] + chip_ref[...]).reshape(lons * rows, lats)
    plane_ref[...] = smoothed(summed, high_ref[...], low_ref[...]).reshape(lons, rows, lats)


def lane_numbers():
    return lax.broadcasted_iota(jnp.int32, (8, LANES), 1)


def tiles(shape):
    return [
        (a, slice(8 * r, 8 * r + 8), slice(LANES * b, LANES * (b + 1)))
        for r in range(shape[1] // 8)
        for b in range(shape[2] // LANES)
        for a in range(shape[0])
    ]


def placed(sums):
    lanes = lane_numbers()
    row = jnp.zeros((8, LANES), jnp.float32)
    for lane, value in sums:
        row = row + jnp.where(lanes == lane, jnp.sum(value, axis=1, keepdims=True), 0.0)
    return row


def spots(shape):
    return [
        (slice(8 * r, 8 * r + 8), slice(LANES * b, LANES * (b + 1)))
        for r in range(shape[0] // 8)
        for b in range(shape[1] // LANES)
    ]


def summed_over(lons, step, size):
    return lax.fori_loop(0, lons, step, [jnp.zeros((8, LANES), jnp.float32)] * size)


def first_gram_kernel(steps_ref, curvature_hbm, changes_ref, row_ref, curvature_ref, semaphores):
    lons, *plane = steps_ref.shape[1:]

    def fetch(a):
        return pltpu.make_async_copy(
            curvature_hbm.at[:, a], curvature_ref.at[:, a], semaphores.at[a]
        )

    for a in range(lons):
        fetch(a).start()
    half = PAIRS // 2

    def step(a, sums):
        fetch(a).wait()
        for at in spots(plane):
            steps = [steps_ref[(i, a, *at)] for i in range(half)]
            changes = [None] * PAIRS
            for i in range(PAIRS):
                value = steps[i] if i < half else steps_ref[(i, a, *at)]
                changes[i] = curvature_ref[(i, a, *at)] * value
                changes_ref[(i, a, *at)] = changes[i]
            sums = [sums[k] + steps[k // PAIRS] * changes[k % PAIRS] for k in range(half * PAIRS)]
        return sums

    row_ref[...] = placed(enumerate(summed_over(lons, step, half * PAIRS)))


def second_gram_kernel(steps_ref, changes_ref, first_ref, row_ref):
    lons, *plane = steps_ref.shape[1:]
    half = PAIRS // 2
    upper = [(i, j) for i in range(PAIRS) for j in range(i, PAIRS)]

    def mixed(a, sums):
        for at in spots(plane):
            steps = [steps_ref[(i, a, *at)] for i in range(half, PAIRS)]
            changes = [changes_ref[(i, a, *at)] for i in range(PAIRS)]
            sums = [sums[k] + steps[k // PAIRS] * changes[k % PAIRS] for k in range(half * PAIRS)]
        return sums

    def squares(a, sums):
        for at in spots(plane):
            changes = [changes_ref[(i, a, *at)] for i in range(PAIRS)]
            sums = [value + changes[i] * changes[j] for value, (i, j) in zip(sums, upper)]
        return sums

    row = first_ref[...] + placed(enumerate(summed_over(lons, mixed, half * PAIRS), half * PAIRS))
    row_ref[...] = row + placed(enumerate(summed_over(lons, squares, len(upper)), SQUARES))


def product_kernel(
    far_halo_ref, far_ref, near_ref, near_halo_ref,
    steps_ref, changes_ref, gram_ref, gradient_ref, rows_ref, padded_ref,
):
    lons, rows, lats = gradient_ref.shape
    weights = cycle_weights()
    mirror = 3 * lax.rem(cut_number(), 2)
    for k, ref in enumerate((far_halo_ref, far_ref, near_ref, near_halo_ref)):
        padded_ref[k ^ mirror] = ref[...]
    sums = [jnp.zeros((8, LANES), jnp.float32) for _ in range(2 * PAIRS)]
    for r in range(rows // 8):
        for b in range(lats // LANES):
            at = (slice(8 * r, 8 * r + 8), slice(LANES * b, LANES * (b + 1)))
            padded = [padded_ref[(k, a, *at)] for k in range(4) for a in range(RIM)]
            for a in range(lons):
                value = weights[RIM] * padded[a + RIM]
                for k in range(RIM):
                    value = value + weights[k] * (padded[a + k] + padded[a + 2 * RIM - k])
                gradient_ref[(a, *at)] = value
                for pair in range(PAIRS):
                    sums[pair] = sums[pair] + steps_ref[(pair, a, *at)] * value
                    sums[PAIRS + pair] = sums[PAIRS + pair] + changes_ref[(pair, a, *at)] * value
    row = gram_ref[...] + placed([(STEPS_GRADIENT + k, value) for k, value in enumerate(sums)])
    row = jnp.sum(row, axis=0, keepdims=True)
    rows_ref[...] = jnp.broadcast_to(row[None], rows_ref.shape)


def direction_kernel(
    rows_ref, gradient_ref, steps_ref, changes_ref, gradient_out, direction_out, direction_ref, semaphores
):
    written = pltpu.make_async_copy(gradient_ref, gradient_out, semaphores.at[0])
    written.start()
    row = jnp.broadcast_to(jnp.sum(rows_ref[...], axis=0), (8, LANES))
    lanes = lane_numbers()
    pairs = lax.broadcasted_iota(jnp.int32, (8, LANES), 0)

    def column(lane_of):
        picked = jnp.where(lanes == lane_of, row, 0.0)
        return jnp.broadcast_to(jnp.sum(picked, axis=1, keepdims=True), (8, LANES))

    def element(vector, i):
        return jnp.broadcast_to(vector[i : i + 1], (8, LANES))

    def square_lanes(j):
        low, high = jnp.minimum(pairs, j), jnp.maximum(pairs, j)
        return SQUARES + low * PAIRS - ((low * (low - 1)) >> 1) + high - low

    by_change = [column(pairs * PAIRS + i) for i in range(PAIRS)]
    by_step = [column(pairs + PAIRS * i) for i in range(PAIRS)]
    squares = [column(square_lanes(i)) for i in range(PAIRS)]
    curvs = column(pairs * (PAIRS + 1))
    steps_part = column(pairs + STEPS_GRADIENT)
    changes_part = column(pairs + CHANGES_GRADIENT)
    inverse = 1.0 / curvs
    scaling = element(curvs, PAIRS - 1) / element(squares[PAIRS - 1], PAIRS - 1)
    alphas = [None] * PAIRS
    for i in reversed(range(PAIRS)):
        alphas[i] = element(inverse * steps_part, i)
        steps_part = steps_part - alphas[i] * by_change[i]
        changes_part = changes_part - alphas[i] * squares[i]
    changes_part = scaling * changes_part
    weights = [None] * PAIRS
    for i in range(PAIRS):
        weights[i] = alphas[i] - element(inverse * changes_part, i)
        changes_part = changes_part + weights[i] * by_step[i]
    change_weights = [scaling * alpha for alpha in alphas]
    copies = []
    lons, pieces = gradient_ref.shape[0], 4
    for piece in range(pieces):
        at = slice(piece * lons // pieces, (piece + 1) * lons // pieces)
        for a, r, b in tiles(gradient_ref.shape):
            if at.start <= a < at.stop:
                value = -(scaling * gradient_ref[a, r, b])
                for i in range(PAIRS):
                    value = value + change_weights[i] * changes_ref[i, a, r, b]
                    value = value - weights[i] * steps_ref[i, a, r, b]
                direction_ref[a, r, b] = value
        if copies:
            copies[-1].start()
        copies.append(
            pltpu.make_async_copy(
                direction_ref.at[at], direction_out.at[at], semaphores.at[1 + piece]
            )
        )
    copies[-1].start()
    for copy in copies:
        copy.wait()
    written.wait()


def in_hbm(x):
    return pltpu.with_memory_space_constraint(x, pltpu.HBM)


def swapped(x, axis):
    return lax.ppermute(x, axis, [(0, 1), (1, 0)])


def cut_number():
    number = 0
    for axis in CUTS:
        number = number * lax.axis_size(axis) + lax.axis_index(axis)
    return number


def shards(kernels, steps, curvature):
    _, lons, rad_len, lats = kernels.shape
    rows = rad_len // 4
    block = ((lons, rows, lats), jnp.float32)
    size = lons * rows * lats
    half = ((RIM, rows, lats), jnp.float32)
    cuts, events = lax.axis_size(CUTS), lax.axis_size(EVENT)
    table = ((2 * rad_len, 2 * rad_len), jnp.bfloat16)
    flops = 4 * rad_len * kernels.size
    far_keep, far_pass, far_send_keep, far_send_pass, near_field, weights = call(
        far_radial_kernel,
        [half] * 4 + [((RIM, rad_len, lats), jnp.float32), table],
        flops,
        8 * kernels.size,
        in_specs=[pl.BlockSpec(memory_space=pltpu.HBM)],
        scratch_shapes=[
            pltpu.VMEM((RIM, rad_len, lats), jnp.float32),
            pltpu.SemaphoreType.DMA((2,)),
        ],
    )(in_hbm(kernels))
    far_core_pass = swapped(far_send_pass, "event_1")
    square = ((lats, lats), jnp.bfloat16)
    near_keep, near_pass, rest, high, low = call(
        near_radial_kernel,
        [half, half, ((3, RIM, rows, lats), jnp.float32), square, square],
        flops,
        4 * kernels.size,
    )(near_field, weights, far_send_keep)
    far_chip = swapped(far_pass + far_core_pass, "event_0")
    rest = swapped(rest, "event_1")
    near_chip = swapped(near_pass + rest[0], "event_0")
    row = ((8, LANES), jnp.float32)
    changes, first_row = call(
        first_gram_kernel,
        [(steps.shape, jnp.float32), row],
        2 * 40 * size,
        12 * steps.size,
        in_specs=[pl.BlockSpec(memory_space=pltpu.VMEM), pl.BlockSpec(memory_space=pltpu.HBM)],
        scratch_shapes=[pltpu.VMEM(curvature.shape, jnp.float32), pltpu.SemaphoreType.DMA((lons,))],
    )(steps, in_hbm(curvature))
    (gram,) = call(second_gram_kernel, [row], 2 * 68 * size, 8 * steps.size)(
        steps, changes, first_row
    )

    def plane_of(slot, *parts):
        kernel = functools.partial(latitude_kernel, slot)
        return call(kernel, [half], 4 * lats * size, 8 * size)(*parts, high, low)[0]

    far_plane = plane_of(2, far_keep, rest, far_chip)
    pairs = []
    for c in range(cuts):
        other, flip = (((c - 1) ^ 1) + 1) % cuts if c else cuts - 1, 2 if c == 0 else 0
        pairs += [(c * events + e, other * events + (e ^ flip)) for e in range(events)]
    far_halo = lax.ppermute(far_plane, CUTS_EVENT, pairs)
    far_plane = lax.ppermute(
        far_plane,
        CUTS_EVENT,
        [(e, e ^ 2) for e in range(events)] + [(d, d) for d in range(events, cuts * events)],
    )
    near_plane = plane_of(1, near_keep, rest, near_chip)
    near_halo = lax.ppermute(near_plane, CUTS, [(c, c ^ 1) for c in range(cuts)])
    gradient, outgoing = call(
        product_kernel,
        [block, ((cuts * events, 1, LANES), jnp.float32)],
        2 * 30 * size,
        4 * 20 * size,
        scratch_shapes=[pltpu.VMEM((4, RIM, rows, lats), jnp.float32)],
    )(far_halo, far_plane, near_plane, near_halo, steps, changes, gram)
    arrived = lax.all_to_all(outgoing, CUTS_EVENT, 0, 0, tiled=True)
    return call(
        direction_kernel,
        [block] * 2,
        2 * 17 * size,
        4 * 18 * size,
        out_specs=[pl.BlockSpec(memory_space=pltpu.HBM)] * 2,
        scratch_shapes=[pltpu.VMEM((lons, rows, lats), jnp.float32), pltpu.SemaphoreType.DMA((5,))],
    )(arrived, gradient, steps, changes)


def solution(mesh):
    torus = Mesh(
        mesh.devices.reshape(2, 4, 4, 2, 2), ("cuts_0", "cuts_1", "cuts_2", "event_0", "event_1")
    )
    in_specs = (P(EVENT, CUTS, None, None), P(None, CUTS, EVENT, None), P(None, CUTS, EVENT, None))
    out_specs = (P(CUTS, EVENT, None), P(CUTS, EVENT, None))
    return jax.shard_map(
        shards, mesh=torus, in_specs=in_specs, out_specs=out_specs, check_vma=False
    )
```

```python
import functools
import math

import jax
import jax.numpy as jnp
from jax import lax
from jax.experimental import pallas as pl
from jax.experimental.pallas import tpu as pltpu
from jax.sharding import Mesh
from jax.sharding import PartitionSpec as P

PAIRS = 8
RIM = 4
CUTS = ("cuts_0", "cuts_1", "cuts_2")
EVENT = ("event_0", "event_1")
CUTS_EVENT = ("cuts_0", "cuts_1", "cuts_2", "event_0", "event_1")
LANES = 128
SQUARES, STEPS_GRADIENT, CHANGES_GRADIENT = 64, 100, 108


def cycle_weights():
    unscaled = [math.exp(-((column - RIM) ** 2) / 4.5) for column in range(2 * RIM + 1)]
    whole = sum(unscaled)
    return [weight / whole for weight in unscaled]


def split(x):
    high = x.astype(jnp.bfloat16)
    low = (x - high.astype(jnp.float32)).astype(jnp.bfloat16)
    return high, low


def dot(a, b):
    return jnp.dot(a, b, preferred_element_type=jnp.float32)


def call(kernel, outs, flops, moved, limit=16, **options):
    return pl.pallas_call(
        kernel,
        out_shape=[jax.ShapeDtypeStruct(*out) for out in outs],
        compiler_params=pltpu.CompilerParams(vmem_limit_bytes=limit << 20),
        cost_estimate=pl.CostEstimate(flops=flops, bytes_accessed=moved, transcendentals=0),
        **options,
    )


def gauss_rows(length, sigma, rows, axis):
    offset = (rows - lax.broadcasted_iota(jnp.int32, rows.shape, axis)).astype(jnp.float32)
    matrix = jnp.exp(-offset * offset / (2.0 * sigma * sigma))
    return matrix / jnp.sum(matrix, axis=axis, keepdims=True)


def gauss_rows(length, sigma, rows, axis):
    offset = (rows - lax.broadcasted_iota(jnp.int32, rows.shape, axis)).astype(jnp.float32)
    matrix = jnp.exp(-offset * offset / (2.0 * sigma * sigma))
    return matrix / jnp.sum(matrix, axis=axis, keepdims=True)


def radial_products(field_ref, weights, keep_ref, pass_ref, send_keep_ref, send_pass_ref):
    for a in range(field_ref.shape[0]):
        both = dot(weights, jnp.concatenate(split(field_ref[a]), axis=0))
        length = both.shape[0] // 2
        rows = length // 4
        out = both[:length] + both[length:]
        for k, ref in enumerate((keep_ref, pass_ref, send_keep_ref, send_pass_ref)):
            ref[a] = out[k * rows : (k + 1) * rows]


def far_radial_kernel(
    kernels_ref, keep_ref, pass_ref, send_keep_ref, send_pass_ref, near_ref, weights_ref, far_ref, semaphores
):
    length = kernels_ref.shape[2]
    odd = lax.rem(cut_number(), 2)
    copies = []
    for piece, ref in enumerate((far_ref, near_ref)):
        source = kernels_ref.at[0, pl.ds(RIM * (odd ^ piece), RIM)]
        copies.append(pltpu.make_async_copy(source, ref, semaphores.at[piece]))
        copies[piece].start()
    part = 2 * lax.axis_index("event_0") + lax.axis_index("event_1")
    rows = length // 4
    local = lax.broadcasted_iota(jnp.int32, (rows, length), 0)

    def weights_of(first):
        order = [first, first ^ 2, first ^ 1, first ^ 3]
        matrix = jnp.concatenate(
            [gauss_rows(length, 3.0, local + rows * block, 1) for block in order], axis=0
        )
        return jnp.concatenate([jnp.concatenate([m, m], axis=1) for m in split(matrix)], axis=0)

    weights = weights_of(jnp.where(cut_number() == 0, part ^ 2, part))
    weights_ref[...] = weights_of(part)
    copies[0].wait()
    radial_products(far_ref, weights, keep_ref, pass_ref, send_keep_ref, send_pass_ref)
    copies[1].wait()


def near_radial_kernel(
    near_ref, weights_ref, far_send_keep_ref, keep_ref, pass_ref, rest_ref, high_ref, low_ref
):
    rest_ref[2] = far_send_keep_ref[...]
    parts = (keep_ref, pass_ref, rest_ref.at[1], rest_ref.at[0])
    radial_products(near_ref, weights_ref[...], *parts)
    lats = high_ref.shape[0]
    column = lax.broadcasted_iota(jnp.int32, (lats, lats), 1)
    high_ref[...], low_ref[...] = split(gauss_rows(lats, 4.0, column, 0))


def smoothed(field, high, low):
    count = field.shape[0]
    both = jnp.concatenate(split(field), axis=0)
    out = dot(both, high) + dot(both, low)
    return out[:count] + out[count:]


def latitude_kernel(slot, keep_ref, rest_ref, chip_ref, high_ref, low_ref, plane_ref):
    lons, rows, lats = plane_ref.shape
    summed = (keep_ref[...] + rest_ref[slot] + chip_ref[...]).reshape(lons * rows, lats)
    plane_ref[...] = smoothed(summed, high_ref[...], low_ref[...]).reshape(lons, rows, lats)


def lane_numbers():
    return lax.broadcasted_iota(jnp.int32, (8, LANES), 1)


def tiles(shape):
    return [
        (a, slice(8 * r, 8 * r + 8), slice(LANES * b, LANES * (b + 1)))
        for r in range(shape[1] // 8)
        for b in range(shape[2] // LANES)
        for a in range(shape[0])
    ]


def placed(sums):
    lanes = lane_numbers()
    row = jnp.zeros((8, LANES), jnp.float32)
    for lane, value in sums:
        row = row + jnp.where(lanes == lane, jnp.sum(value, axis=1, keepdims=True), 0.0)
    return row


def spots(shape):
    return [
        (slice(8 * r, 8 * r + 8), slice(LANES * b, LANES * (b + 1)))
        for r in range(shape[0] // 8)
        for b in range(shape[1] // LANES)
    ]


def summed_over(lons, step, size):
    return lax.fori_loop(0, lons, step, [jnp.zeros((8, LANES), jnp.float32)] * size)


def first_gram_kernel(
    steps_hbm, curvature_hbm, steps_ref, changes_ref, row_ref, curvature_ref, semaphores
):
    lons, *plane = steps_ref.shape[1:]

    def fetches(a):
        pairs = ((steps_hbm, steps_ref), (curvature_hbm, curvature_ref))
        return [
            pltpu.make_async_copy(source.at[:, a], target.at[:, a], semaphores.at[k, a])
            for k, (source, target) in enumerate(pairs)
        ]

    for a in range(lons):
        for fetch in fetches(a):
            fetch.start()
    half = PAIRS // 2

    def step(a, sums):
        for fetch in fetches(a):
            fetch.wait()
        for at in spots(plane):
            steps = [steps_ref[(i, a, *at)] for i in range(half)]
            changes = [None] * PAIRS
            for i in range(PAIRS):
                value = steps[i] if i < half else steps_ref[(i, a, *at)]
                changes[i] = curvature_ref[(i, a, *at)] * value
                changes_ref[(i, a, *at)] = changes[i]
            sums = [sums[k] + steps[k // PAIRS] * changes[k % PAIRS] for k in range(half * PAIRS)]
        return sums

    row_ref[...] = placed(enumerate(summed_over(lons, step, half * PAIRS)))


def second_gram_kernel(steps_ref, changes_ref, first_ref, row_ref):
    lons, *plane = steps_ref.shape[1:]
    half = PAIRS // 2
    upper = [(i, j) for i in range(PAIRS) for j in range(i, PAIRS)]

    def mixed(a, sums):
        for at in spots(plane):
            steps = [steps_ref[(i, a, *at)] for i in range(half, PAIRS)]
            changes = [changes_ref[(i, a, *at)] for i in range(PAIRS)]
            sums = [sums[k] + steps[k // PAIRS] * changes[k % PAIRS] for k in range(half * PAIRS)]
        return sums

    def squares(a, sums):
        for at in spots(plane):
            changes = [changes_ref[(i, a, *at)] for i in range(PAIRS)]
            sums = [value + changes[i] * changes[j] for value, (i, j) in zip(sums, upper)]
        return sums

    row = first_ref[...] + placed(enumerate(summed_over(lons, mixed, half * PAIRS), half * PAIRS))
    row_ref[...] = row + placed(enumerate(summed_over(lons, squares, len(upper)), SQUARES))


def product_kernel(
    far_halo_ref, far_ref, near_ref, near_halo_ref,
    steps_ref, changes_ref, gram_ref, gradient_ref, rows_ref, padded_ref,
):
    lons, rows, lats = gradient_ref.shape
    weights = cycle_weights()
    mirror = 3 * lax.rem(cut_number(), 2)
    for k, ref in enumerate((far_halo_ref, far_ref, near_ref, near_halo_ref)):
        padded_ref[k ^ mirror] = ref[...]
    sums = [jnp.zeros((8, LANES), jnp.float32) for _ in range(2 * PAIRS)]
    for r in range(rows // 8):
        for b in range(lats // LANES):
            at = (slice(8 * r, 8 * r + 8), slice(LANES * b, LANES * (b + 1)))
            padded = [padded_ref[(k, a, *at)] for k in range(4) for a in range(RIM)]
            for a in range(lons):
                value = weights[RIM] * padded[a + RIM]
                for k in range(RIM):
                    value = value + weights[k] * (padded[a + k] + padded[a + 2 * RIM - k])
                gradient_ref[(a, *at)] = value
                for pair in range(PAIRS):
                    sums[pair] = sums[pair] + steps_ref[(pair, a, *at)] * value
                    sums[PAIRS + pair] = sums[PAIRS + pair] + changes_ref[(pair, a, *at)] * value
    row = gram_ref[...] + placed([(STEPS_GRADIENT + k, value) for k, value in enumerate(sums)])
    row = jnp.sum(row, axis=0, keepdims=True)
    rows_ref[...] = jnp.broadcast_to(row[None], rows_ref.shape)


def direction_kernel(
    rows_ref, gradient_ref, steps_ref, changes_ref, gradient_out, direction_out, direction_ref, semaphores
):
    written = pltpu.make_async_copy(gradient_ref, gradient_out, semaphores.at[0])
    written.start()
    row = jnp.broadcast_to(jnp.sum(rows_ref[...], axis=0), (8, LANES))
    lanes = lane_numbers()
    pairs = lax.broadcasted_iota(jnp.int32, (8, LANES), 0)

    def column(lane_of):
        picked = jnp.where(lanes == lane_of, row, 0.0)
        return jnp.broadcast_to(jnp.sum(picked, axis=1, keepdims=True), (8, LANES))

    def element(vector, i):
        return jnp.broadcast_to(vector[i : i + 1], (8, LANES))

    def square_lanes(j):
        low, high = jnp.minimum(pairs, j), jnp.maximum(pairs, j)
        return SQUARES + low * PAIRS - ((low * (low - 1)) >> 1) + high - low

    by_change = [column(pairs * PAIRS + i) for i in range(PAIRS)]
    by_step = [column(pairs + PAIRS * i) for i in range(PAIRS)]
    squares = [column(square_lanes(i)) for i in range(PAIRS)]
    curvs = column(pairs * (PAIRS + 1))
    steps_part = column(pairs + STEPS_GRADIENT)
    changes_part = column(pairs + CHANGES_GRADIENT)
    inverse = 1.0 / curvs
    scaling = element(curvs, PAIRS - 1) / element(squares[PAIRS - 1], PAIRS - 1)
    alphas = [None] * PAIRS
    for i in reversed(range(PAIRS)):
        alphas[i] = element(inverse * steps_part, i)
        steps_part = steps_part - alphas[i] * by_change[i]
        changes_part = changes_part - alphas[i] * squares[i]
    changes_part = scaling * changes_part
    weights = [None] * PAIRS
    for i in range(PAIRS):
        weights[i] = alphas[i] - element(inverse * changes_part, i)
        changes_part = changes_part + weights[i] * by_step[i]
    change_weights = [scaling * alpha for alpha in alphas]
    copies = []
    lons, pieces = gradient_ref.shape[0], 4
    for piece in range(pieces):
        at = slice(piece * lons // pieces, (piece + 1) * lons // pieces)
        for a, r, b in tiles(gradient_ref.shape):
            if at.start <= a < at.stop:
                value = -(scaling * gradient_ref[a, r, b])
                for i in range(PAIRS):
                    value = value + change_weights[i] * changes_ref[i, a, r, b]
                    value = value - weights[i] * steps_ref[i, a, r, b]
                direction_ref[a, r, b] = value
        if copies:
            copies[-1].start()
        copies.append(
            pltpu.make_async_copy(
                direction_ref.at[at], direction_out.at[at], semaphores.at[1 + piece]
            )
        )
    copies[-1].start()
    for copy in copies:
        copy.wait()
    written.wait()


def in_hbm(x):
    return pltpu.with_memory_space_constraint(x, pltpu.HBM)


def swapped(x, axis):
    return lax.ppermute(x, axis, [(0, 1), (1, 0)])


def cut_number():
    number = 0
    for axis in CUTS:
        number = number * lax.axis_size(axis) + lax.axis_index(axis)
    return number


def shards(kernels, steps, curvature):
    _, lons, rad_len, lats = kernels.shape
    rows = rad_len // 4
    block = ((lons, rows, lats), jnp.float32)
    size = lons * rows * lats
    half = ((RIM, rows, lats), jnp.float32)
    cuts, events = lax.axis_size(CUTS), lax.axis_size(EVENT)
    table = ((2 * rad_len, 2 * rad_len), jnp.bfloat16)
    flops = 4 * rad_len * kernels.size
    far_keep, far_pass, far_send_keep, far_send_pass, near_field, weights = call(
        far_radial_kernel,
        [half] * 4 + [((RIM, rad_len, lats), jnp.float32), table],
        flops,
        8 * kernels.size,
        in_specs=[pl.BlockSpec(memory_space=pltpu.HBM)],
        scratch_shapes=[
            pltpu.VMEM((RIM, rad_len, lats), jnp.float32),
            pltpu.SemaphoreType.DMA((2,)),
        ],
    )(in_hbm(kernels))
    far_core_pass = swapped(far_send_pass, "event_1")
    square = ((lats, lats), jnp.bfloat16)
    near_keep, near_pass, rest, high, low = call(
        near_radial_kernel,
        [half, half, ((3, RIM, rows, lats), jnp.float32), square, square],
        flops,
        4 * kernels.size,
    )(near_field, weights, far_send_keep)
    far_chip = swapped(far_pass + far_core_pass, "event_0")
    rest = swapped(rest, "event_1")
    near_chip = swapped(near_pass + rest[0], "event_0")
    row = ((8, LANES), jnp.float32)
    held_steps, changes, first_row = call(
        first_gram_kernel,
        [(steps.shape, jnp.float32)] * 2 + [row],
        2 * 40 * size,
        16 * steps.size,
        in_specs=[pl.BlockSpec(memory_space=pltpu.HBM)] * 2,
        scratch_shapes=[
            pltpu.VMEM(curvature.shape, jnp.float32),
            pltpu.SemaphoreType.DMA((2, lons)),
        ],
    )(in_hbm(steps), in_hbm(curvature))
    (gram,) = call(second_gram_kernel, [row], 2 * 68 * size, 8 * steps.size)(
        held_steps, changes, first_row
    )

    def plane_of(slot, *parts):
        kernel = functools.partial(latitude_kernel, slot)
        return call(kernel, [half], 4 * lats * size, 8 * size)(*parts, high, low)[0]

    far_plane = plane_of(2, far_keep, rest, far_chip)
    pairs = []
    for c in range(cuts):
        other, flip = (((c - 1) ^ 1) + 1) % cuts if c else cuts - 1, 2 if c == 0 else 0
        pairs += [(c * events + e, other * events + (e ^ flip)) for e in range(events)]
    far_halo = lax.ppermute(far_plane, CUTS_EVENT, pairs)
    far_plane = lax.ppermute(
        far_plane,
        CUTS_EVENT,
        [(e, e ^ 2) for e in range(events)] + [(d, d) for d in range(events, cuts * events)],
    )
    near_plane = plane_of(1, near_keep, rest, near_chip)
    near_halo = lax.ppermute(near_plane, CUTS, [(c, c ^ 1) for c in range(cuts)])
    gradient, outgoing = call(
        product_kernel,
        [block, ((cuts * events, 1, LANES), jnp.float32)],
        2 * 30 * size,
        4 * 20 * size,
        scratch_shapes=[pltpu.VMEM((4, RIM, rows, lats), jnp.float32)],
    )(far_halo, far_plane, near_plane, near_halo, held_steps, changes, gram)
    arrived = lax.all_to_all(outgoing, CUTS_EVENT, 0, 0, tiled=True)
    return call(
        direction_kernel,
        [block] * 2,
        2 * 17 * size,
        4 * 18 * size,
        out_specs=[pl.BlockSpec(memory_space=pltpu.HBM)] * 2,
        scratch_shapes=[pltpu.VMEM((lons, rows, lats), jnp.float32), pltpu.SemaphoreType.DMA((5,))],
    )(arrived, gradient, held_steps, changes)


def solution(mesh):
    torus = Mesh(
        mesh.devices.reshape(2, 4, 4, 2, 2), ("cuts_0", "cuts_1", "cuts_2", "event_0", "event_1")
    )
    in_specs = (P(EVENT, CUTS, None, None), P(None, CUTS, EVENT, None), P(None, CUTS, EVENT, None))
    out_specs = (P(CUTS, EVENT, None), P(CUTS, EVENT, None))
    return jax.shard_map(
        shards, mesh=torus, in_specs=in_specs, out_specs=out_specs, check_vma=False
    )
```

```python
import functools
import math

import jax
import jax.numpy as jnp
from jax import lax
from jax.experimental import pallas as pl
from jax.experimental.pallas import tpu as pltpu
from jax.sharding import Mesh
from jax.sharding import PartitionSpec as P

PAIRS = 8
RIM = 4
CUTS = ("cuts_0", "cuts_1", "cuts_2")
EVENT = ("event_0", "event_1")
CUTS_EVENT = ("cuts_0", "cuts_1", "cuts_2", "event_0", "event_1")
LANES = 128
SQUARES, STEPS_GRADIENT, CHANGES_GRADIENT = 64, 100, 108


def cycle_weights():
    unscaled = [math.exp(-((column - RIM) ** 2) / 4.5) for column in range(2 * RIM + 1)]
    whole = sum(unscaled)
    return [weight / whole for weight in unscaled]


def split(x):
    high = x.astype(jnp.bfloat16)
    low = (x - high.astype(jnp.float32)).astype(jnp.bfloat16)
    return high, low


def dot(a, b):
    return jnp.dot(a, b, preferred_element_type=jnp.float32)


def call(kernel, outs, flops, moved, limit=16, **options):
    return pl.pallas_call(
        kernel,
        out_shape=[jax.ShapeDtypeStruct(*out) for out in outs],
        compiler_params=pltpu.CompilerParams(vmem_limit_bytes=limit << 20),
        cost_estimate=pl.CostEstimate(flops=flops, bytes_accessed=moved, transcendentals=0),
        **options,
    )


def gauss_rows(length, sigma, rows, axis):
    offset = (rows - lax.broadcasted_iota(jnp.int32, rows.shape, axis)).astype(jnp.float32)
    matrix = jnp.exp(-offset * offset / (2.0 * sigma * sigma))
    return matrix / jnp.sum(matrix, axis=axis, keepdims=True)


def gauss_rows(length, sigma, rows, axis):
    offset = (rows - lax.broadcasted_iota(jnp.int32, rows.shape, axis)).astype(jnp.float32)
    matrix = jnp.exp(-offset * offset / (2.0 * sigma * sigma))
    return matrix / jnp.sum(matrix, axis=axis, keepdims=True)


def radial_products(field_ref, weights, keep_ref, pass_ref, send_keep_ref, send_pass_ref):
    for a in range(field_ref.shape[0]):
        both = dot(weights, jnp.concatenate(split(field_ref[a]), axis=0))
        length = both.shape[0] // 2
        rows = length // 4
        out = both[:length] + both[length:]
        for k, ref in enumerate((keep_ref, pass_ref, send_keep_ref, send_pass_ref)):
            ref[a] = out[k * rows : (k + 1) * rows]


def far_radial_kernel(
    kernels_ref, keep_ref, pass_ref, send_keep_ref, send_pass_ref, near_ref, weights_ref, far_ref, semaphores
):
    length = kernels_ref.shape[2]
    odd = lax.rem(cut_number(), 2)
    copies = []
    for piece, ref in enumerate((far_ref, near_ref)):
        source = kernels_ref.at[0, pl.ds(RIM * (odd ^ piece), RIM)]
        copies.append(pltpu.make_async_copy(source, ref, semaphores.at[piece]))
        copies[piece].start()
    part = 2 * lax.axis_index("event_0") + lax.axis_index("event_1")
    rows = length // 4
    local = lax.broadcasted_iota(jnp.int32, (rows, length), 0)

    def weights_of(first):
        order = [first, first ^ 2, first ^ 1, first ^ 3]
        matrix = jnp.concatenate(
            [gauss_rows(length, 3.0, local + rows * block, 1) for block in order], axis=0
        )
        return jnp.concatenate([jnp.concatenate([m, m], axis=1) for m in split(matrix)], axis=0)

    cut = cut_number()
    at_wrap = jnp.logical_or(cut == 0, cut == lax.axis_size(CUTS) - 1)
    weights = weights_of(jnp.where(at_wrap, part ^ 2, part))
    weights_ref[...] = weights_of(part)
    copies[0].wait()
    radial_products(far_ref, weights, keep_ref, pass_ref, send_keep_ref, send_pass_ref)
    copies[1].wait()


def near_radial_kernel(
    near_ref, weights_ref, far_send_keep_ref, keep_ref, pass_ref, rest_ref, high_ref, low_ref
):
    rest_ref[2] = far_send_keep_ref[...]
    parts = (keep_ref, pass_ref, rest_ref.at[1], rest_ref.at[0])
    radial_products(near_ref, weights_ref[...], *parts)
    lats = high_ref.shape[0]
    column = lax.broadcasted_iota(jnp.int32, (lats, lats), 1)
    high_ref[...], low_ref[...] = split(gauss_rows(lats, 4.0, column, 0))


def smoothed(field, high, low):
    count = field.shape[0]
    both = jnp.concatenate(split(field), axis=0)
    out = dot(both, high) + dot(both, low)
    return out[:count] + out[count:]


def latitude_kernel(slot, keep_ref, rest_ref, chip_ref, high_ref, low_ref, plane_ref):
    lons, rows, lats = plane_ref.shape
    summed = (keep_ref[...] + rest_ref[slot] + chip_ref[...]).reshape(lons * rows, lats)
    plane_ref[...] = smoothed(summed, high_ref[...], low_ref[...]).reshape(lons, rows, lats)


def lane_numbers():
    return lax.broadcasted_iota(jnp.int32, (8, LANES), 1)


def tiles(shape):
    return [
        (a, slice(8 * r, 8 * r + 8), slice(LANES * b, LANES * (b + 1)))
        for r in range(shape[1] // 8)
        for b in range(shape[2] // LANES)
        for a in range(shape[0])
    ]


def placed(sums):
    lanes = lane_numbers()
    row = jnp.zeros((8, LANES), jnp.float32)
    for lane, value in sums:
        row = row + jnp.where(lanes == lane, jnp.sum(value, axis=1, keepdims=True), 0.0)
    return row


def spots(shape):
    return [
        (slice(8 * r, 8 * r + 8), slice(LANES * b, LANES * (b + 1)))
        for r in range(shape[0] // 8)
        for b in range(shape[1] // LANES)
    ]


def summed_over(lons, step, size):
    return lax.fori_loop(0, lons, step, [jnp.zeros((8, LANES), jnp.float32)] * size)


def fetch_kernel(curvature_hbm, curvature_ref, semaphore):
    copy = pltpu.make_async_copy(curvature_hbm, curvature_ref, semaphore)
    copy.start()
    copy.wait()


def gram_kernel(steps_ref, curvature_ref, changes_ref, row_ref):
    lons, *plane = steps_ref.shape[1:]
    half = PAIRS // 2
    upper = [(i, j) for i in range(PAIRS) for j in range(i, PAIRS)]

    def first(a, sums):
        for at in spots(plane):
            steps = [steps_ref[(i, a, *at)] for i in range(half)]
            changes = [None] * PAIRS
            for i in range(PAIRS):
                value = steps[i] if i < half else steps_ref[(i, a, *at)]
                changes[i] = curvature_ref[(i, a, *at)] * value
                changes_ref[(i, a, *at)] = changes[i]
            sums = [sums[k] + steps[k // PAIRS] * changes[k % PAIRS] for k in range(half * PAIRS)]
        return sums

    def second(a, sums):
        for at in spots(plane):
            steps = [steps_ref[(i, a, *at)] for i in range(half, PAIRS)]
            changes = [changes_ref[(i, a, *at)] for i in range(PAIRS)]
            sums = [sums[k] + steps[k // PAIRS] * changes[k % PAIRS] for k in range(half * PAIRS)]
        return sums

    def squares(a, sums):
        for at in spots(plane):
            changes = [changes_ref[(i, a, *at)] for i in range(PAIRS)]
            sums = [value + changes[i] * changes[j] for value, (i, j) in zip(sums, upper)]
        return sums

    row = placed(enumerate(summed_over(lons, first, half * PAIRS)))
    row = row + placed(enumerate(summed_over(lons, second, half * PAIRS), half * PAIRS))
    row_ref[...] = row + placed(enumerate(summed_over(lons, squares, len(upper)), SQUARES))


def near_base():
    return RIM * (1 - lax.rem(cut_number(), 2))


def side_products(base, halo_ref, side_ref, inner_ref, steps_ref, changes_ref, gradient_ref, padded_ref):
    lons, rows, lats = gradient_ref.shape
    weights = cycle_weights()
    outer = 2 * base // RIM
    padded_ref[outer] = halo_ref[...]
    padded_ref[1] = side_ref[...]
    padded_ref[2 - outer] = inner_ref[...]
    sums = [jnp.zeros((8, LANES), jnp.float32) for _ in range(2 * PAIRS)]
    for at in spots((rows, lats)):
        padded = [padded_ref[(k, a, *at)] for k in range(3) for a in range(RIM)]
        for a in range(lons):
            value = weights[RIM] * padded[a + RIM]
            for k in range(RIM):
                value = value + weights[k] * (padded[a + k] + padded[a + 2 * RIM - k])
            gradient_ref[(a, *at)] = value
            for pair in range(PAIRS):
                sums[pair] = sums[pair] + steps_ref[(pair, base + a, *at)] * value
                sums[PAIRS + pair] = sums[PAIRS + pair] + changes_ref[(pair, base + a, *at)] * value
    return placed(enumerate(sums, STEPS_GRADIENT))


def near_product_kernel(
    halo_ref, near_ref, far_ref, steps_ref, changes_ref, gram_ref, gradient_ref, row_ref, padded_ref
):
    operands = (halo_ref, near_ref, far_ref, steps_ref, changes_ref, gradient_ref, padded_ref)
    row_ref[...] = gram_ref[...] + side_products(near_base(), *operands)


def far_product_kernel(
    halo_ref, far_ref, near_ref, steps_ref, changes_ref, near_row_ref, gradient_ref, rows_ref, padded_ref
):
    operands = (halo_ref, far_ref, near_ref, steps_ref, changes_ref, gradient_ref, padded_ref)
    row = near_row_ref[...] + side_products(RIM - near_base(), *operands)
    row = jnp.sum(row, axis=0, keepdims=True)
    rows_ref[...] = jnp.broadcast_to(row[None], rows_ref.shape)


def direction_kernel(
    rows_ref, far_ref, near_ref, steps_ref, changes_ref,
    gradient_out, direction_out, direction_ref, semaphores,
):
    sides = ((RIM - near_base(), far_ref), (near_base(), near_ref))
    written = [
        pltpu.make_async_copy(ref, gradient_out.at[pl.ds(base, RIM)], semaphores.at[k])
        for k, (base, ref) in enumerate(sides)
    ]
    for copy in written:
        copy.start()
    row = jnp.broadcast_to(jnp.sum(rows_ref[...], axis=0), (8, LANES))
    lanes = lane_numbers()
    pairs = lax.broadcasted_iota(jnp.int32, (8, LANES), 0)

    def column(lane_of):
        picked = jnp.where(lanes == lane_of, row, 0.0)
        return jnp.broadcast_to(jnp.sum(picked, axis=1, keepdims=True), (8, LANES))

    def element(vector, i):
        return jnp.broadcast_to(vector[i : i + 1], (8, LANES))

    def square_lanes(j):
        low, high = jnp.minimum(pairs, j), jnp.maximum(pairs, j)
        return SQUARES + low * PAIRS - ((low * (low - 1)) >> 1) + high - low

    by_change = [column(pairs * PAIRS + i) for i in range(PAIRS)]
    by_step = [column(pairs + PAIRS * i) for i in range(PAIRS)]
    squares = [column(square_lanes(i)) for i in range(PAIRS)]
    curvs = column(pairs * (PAIRS + 1))
    steps_part = column(pairs + STEPS_GRADIENT)
    changes_part = column(pairs + CHANGES_GRADIENT)
    inverse = 1.0 / curvs
    scaling = element(curvs, PAIRS - 1) / element(squares[PAIRS - 1], PAIRS - 1)
    alphas = [None] * PAIRS
    for i in reversed(range(PAIRS)):
        alphas[i] = element(inverse * steps_part, i)
        steps_part = steps_part - alphas[i] * by_change[i]
        changes_part = changes_part - alphas[i] * squares[i]
    changes_part = scaling * changes_part
    weights = [None] * PAIRS
    for i in range(PAIRS):
        weights[i] = alphas[i] - element(inverse * changes_part, i)
        changes_part = changes_part + weights[i] * by_step[i]
    change_weights = [scaling * alpha for alpha in alphas]
    copies = []
    half = RIM // 2
    for piece in range(4):
        base, gradient_ref = sides[piece // 2]
        first = piece % 2 * half
        for a, r, b in tiles((half, *far_ref.shape[1:])):
            lon = base + first + a
            value = -(scaling * gradient_ref[first + a, r, b])
            for i in range(PAIRS):
                value = value + change_weights[i] * changes_ref[i, lon, r, b]
                value = value - weights[i] * steps_ref[i, lon, r, b]
            direction_ref[half * piece + a, r, b] = value
        if copies:
            copies[-1].start()
        copies.append(
            pltpu.make_async_copy(
                direction_ref.at[pl.ds(half * piece, half)],
                direction_out.at[pl.ds(base + first, half)],
                semaphores.at[2 + piece],
            )
        )
    copies[-1].start()
    for copy in copies + written:
        copy.wait()


def in_hbm(x):
    return pltpu.with_memory_space_constraint(x, pltpu.HBM)


def swapped(x, axis):
    return lax.ppermute(x, axis, [(0, 1), (1, 0)])


def cut_number():
    number = 0
    for axis in CUTS:
        number = number * lax.axis_size(axis) + lax.axis_index(axis)
    return number


def shards(kernels, steps, curvature):
    _, lons, rad_len, lats = kernels.shape
    rows = rad_len // 4
    block = ((lons, rows, lats), jnp.float32)
    size = lons * rows * lats
    half = ((RIM, rows, lats), jnp.float32)
    cuts, events = lax.axis_size(CUTS), lax.axis_size(EVENT)
    table = ((2 * rad_len, 2 * rad_len), jnp.bfloat16)
    flops = 4 * rad_len * kernels.size
    far_keep, far_pass, far_send_keep, far_send_pass, near_field, weights = call(
        far_radial_kernel,
        [half] * 4 + [((RIM, rad_len, lats), jnp.float32), table],
        flops,
        8 * kernels.size,
        in_specs=[pl.BlockSpec(memory_space=pltpu.HBM)],
        scratch_shapes=[
            pltpu.VMEM((RIM, rad_len, lats), jnp.float32),
            pltpu.SemaphoreType.DMA((2,)),
        ],
    )(in_hbm(kernels))
    far_core_pass = swapped(far_send_pass, "event_1")
    square = ((lats, lats), jnp.bfloat16)
    near_keep, near_pass, rest, high, low = call(
        near_radial_kernel,
        [half, half, ((3, RIM, rows, lats), jnp.float32), square, square],
        flops,
        4 * kernels.size,
    )(near_field, weights, far_send_keep)
    far_chip = swapped(far_pass + far_core_pass, "event_0")
    rest = swapped(rest, "event_1")
    near_chip = swapped(near_pass + rest[0], "event_0")
    row = ((8, LANES), jnp.float32)
    (held_curvature,) = call(
        fetch_kernel,
        [(curvature.shape, jnp.float32)],
        0,
        8 * curvature.size,
        in_specs=[pl.BlockSpec(memory_space=pltpu.HBM)],
        scratch_shapes=[pltpu.SemaphoreType.DMA],
    )(in_hbm(curvature))
    changes, gram = call(
        gram_kernel,
        [(steps.shape, jnp.float32), row],
        2 * 108 * size,
        12 * steps.size,
    )(steps, held_curvature)

    def plane_of(slot, *parts):
        kernel = functools.partial(latitude_kernel, slot)
        return call(kernel, [half], 4 * lats * size, 8 * size)(*parts, high, low)[0]

    far_plane = plane_of(2, far_keep, rest, far_chip)
    pairs, returns = [], []
    for c in range(cuts):
        other, flip = (((c - 1) ^ 1) + 1) % cuts, 0
        if c in (0, cuts - 1):
            other, flip = cuts - 1 - c, 2
        for e in range(events):
            pairs.append((c * events + e, other * events + (e ^ flip)))
            returns.append((c * events + e, c * events + (e ^ flip)))
    far_halo = lax.ppermute(far_plane, CUTS_EVENT, pairs)
    far_plane = lax.ppermute(far_plane, CUTS_EVENT, returns)
    near_plane = plane_of(1, near_keep, rest, near_chip)
    near_halo = lax.ppermute(near_plane, CUTS, [(c, c ^ 1) for c in range(cuts)])
    padded = [pltpu.VMEM((3, RIM, rows, lats), jnp.float32)]
    near_gradient, near_row = call(
        near_product_kernel, [half, row], 2 * 20 * size, 4 * 10 * size, scratch_shapes=padded
    )(near_halo, near_plane, far_plane, steps, changes, gram)
    far_gradient, outgoing = call(
        far_product_kernel,
        [half, ((cuts * events, 1, LANES), jnp.float32)],
        2 * 20 * size,
        4 * 10 * size,
        scratch_shapes=padded,
    )(far_halo, far_plane, near_plane, steps, changes, near_row)
    arrived = lax.all_to_all(outgoing, CUTS_EVENT, 0, 0, tiled=True)
    return call(
        direction_kernel,
        [block] * 2,
        2 * 17 * size,
        4 * 18 * size,
        out_specs=[pl.BlockSpec(memory_space=pltpu.HBM)] * 2,
        scratch_shapes=[pltpu.VMEM((lons, rows, lats), jnp.float32), pltpu.SemaphoreType.DMA((6,))],
    )(arrived, far_gradient, near_gradient, steps, changes)


def solution(mesh):
    torus = Mesh(
        mesh.devices.reshape(2, 4, 4, 2, 2), ("cuts_0", "cuts_1", "cuts_2", "event_0", "event_1")
    )
    in_specs = (P(EVENT, CUTS, None, None), P(None, CUTS, EVENT, None), P(None, CUTS, EVENT, None))
    out_specs = (P(CUTS, EVENT, None), P(CUTS, EVENT, None))
    return jax.shard_map(
        shards, mesh=torus, in_specs=in_specs, out_specs=out_specs, check_vma=False
    )
```

```python
import functools
import math

import jax
import jax.numpy as jnp
from jax import lax
from jax.experimental import pallas as pl
from jax.experimental.pallas import tpu as pltpu
from jax.sharding import Mesh
from jax.sharding import PartitionSpec as P

PAIRS = 8
RIM = 4
CUTS = ("cuts_0", "cuts_1", "cuts_2")
EVENT = ("event_0", "event_1")
CUTS_EVENT = ("cuts_0", "cuts_1", "cuts_2", "event_0", "event_1")
LANES = 128
SQUARES, STEPS_GRADIENT, CHANGES_GRADIENT = 64, 100, 108


def cycle_weights():
    unscaled = [math.exp(-((column - RIM) ** 2) / 4.5) for column in range(2 * RIM + 1)]
    whole = sum(unscaled)
    return [weight / whole for weight in unscaled]


def split(x):
    high = x.astype(jnp.bfloat16)
    low = (x - high.astype(jnp.float32)).astype(jnp.bfloat16)
    return high, low


def dot(a, b):
    return jnp.dot(a, b, preferred_element_type=jnp.float32)


def call(kernel, outs, flops, moved, limit=16, **options):
    return pl.pallas_call(
        kernel,
        out_shape=[jax.ShapeDtypeStruct(*out) for out in outs],
        compiler_params=pltpu.CompilerParams(vmem_limit_bytes=limit << 20),
        cost_estimate=pl.CostEstimate(flops=flops, bytes_accessed=moved, transcendentals=0),
        **options,
    )


def gauss_rows(length, sigma, rows, axis):
    offset = (rows - lax.broadcasted_iota(jnp.int32, rows.shape, axis)).astype(jnp.float32)
    matrix = jnp.exp(-offset * offset / (2.0 * sigma * sigma))
    return matrix / jnp.sum(matrix, axis=axis, keepdims=True)


def gauss_rows(length, sigma, rows, axis):
    offset = (rows - lax.broadcasted_iota(jnp.int32, rows.shape, axis)).astype(jnp.float32)
    matrix = jnp.exp(-offset * offset / (2.0 * sigma * sigma))
    return matrix / jnp.sum(matrix, axis=axis, keepdims=True)


def radial_products(field_ref, weights, keep_ref, pass_ref, send_keep_ref, send_pass_ref):
    for a in range(field_ref.shape[0]):
        both = dot(weights, jnp.concatenate(split(field_ref[a]), axis=0))
        length = both.shape[0] // 2
        rows = length // 4
        out = both[:length] + both[length:]
        for k, ref in enumerate((keep_ref, pass_ref, send_keep_ref, send_pass_ref)):
            ref[a] = out[k * rows : (k + 1) * rows]


def far_radial_kernel(
    kernels_ref, keep_ref, pass_ref, send_keep_ref, send_pass_ref, near_ref, weights_ref, far_ref, semaphores
):
    length = kernels_ref.shape[2]
    odd = lax.rem(cut_number(), 2)
    copies = []
    for piece, ref in enumerate((far_ref, near_ref)):
        source = kernels_ref.at[0, pl.ds(RIM * (odd ^ piece), RIM)]
        copies.append(pltpu.make_async_copy(source, ref, semaphores.at[piece]))
        copies[piece].start()
    part = 2 * lax.axis_index("event_0") + lax.axis_index("event_1")
    rows = length // 4
    local = lax.broadcasted_iota(jnp.int32, (rows, length), 0)

    def weights_of(first):
        order = [first, first ^ 2, first ^ 1, first ^ 3]
        matrix = jnp.concatenate(
            [gauss_rows(length, 3.0, local + rows * block, 1) for block in order], axis=0
        )
        return jnp.concatenate([jnp.concatenate([m, m], axis=1) for m in split(matrix)], axis=0)

    weights = weights_of(jnp.where(cut_number() == 0, part ^ 2, part))
    weights_ref[...] = weights_of(part)
    copies[0].wait()
    radial_products(far_ref, weights, keep_ref, pass_ref, send_keep_ref, send_pass_ref)
    copies[1].wait()


def near_radial_kernel(
    near_ref, weights_ref, far_send_keep_ref, keep_ref, pass_ref, rest_ref, high_ref, low_ref
):
    rest_ref[2] = far_send_keep_ref[...]
    parts = (keep_ref, pass_ref, rest_ref.at[1], rest_ref.at[0])
    radial_products(near_ref, weights_ref[...], *parts)
    lats = high_ref.shape[0]
    column = lax.broadcasted_iota(jnp.int32, (lats, lats), 1)
    high_ref[...], low_ref[...] = split(gauss_rows(lats, 4.0, column, 0))


def smoothed(field, high, low):
    count = field.shape[0]
    both = jnp.concatenate(split(field), axis=0)
    out = dot(both, high) + dot(both, low)
    return out[:count] + out[count:]


def latitude_kernel(slot, keep_ref, rest_ref, chip_ref, high_ref, low_ref, plane_ref):
    lons, rows, lats = plane_ref.shape
    summed = (keep_ref[...] + rest_ref[slot] + chip_ref[...]).reshape(lons * rows, lats)
    plane_ref[...] = smoothed(summed, high_ref[...], low_ref[...]).reshape(lons, rows, lats)


def lane_numbers():
    return lax.broadcasted_iota(jnp.int32, (8, LANES), 1)


def tiles(shape):
    return [
        (a, slice(8 * r, 8 * r + 8), slice(LANES * b, LANES * (b + 1)))
        for r in range(shape[1] // 8)
        for b in range(shape[2] // LANES)
        for a in range(shape[0])
    ]


def placed(sums):
    lanes = lane_numbers()
    row = jnp.zeros((8, LANES), jnp.float32)
    for lane, value in sums:
        row = row + jnp.where(lanes == lane, jnp.sum(value, axis=1, keepdims=True), 0.0)
    return row


def spots(shape):
    return [
        (slice(8 * r, 8 * r + 8), slice(LANES * b, LANES * (b + 1)))
        for r in range(shape[0] // 8)
        for b in range(shape[1] // LANES)
    ]


def summed_over(lons, step, size):
    return lax.fori_loop(0, lons, step, [jnp.zeros((8, LANES), jnp.float32)] * size)


def fetch_kernel(curvature_hbm, curvature_ref, semaphore):
    copy = pltpu.make_async_copy(curvature_hbm, curvature_ref, semaphore)
    copy.start()
    copy.wait()


def gram_kernel(steps_ref, curvature_ref, changes_ref, row_ref):
    lons, *plane = steps_ref.shape[1:]
    half = PAIRS // 2
    upper = [(i, j) for i in range(PAIRS) for j in range(i, PAIRS)]

    def first(a, sums):
        for at in spots(plane):
            steps = [steps_ref[(i, a, *at)] for i in range(half)]
            changes = [None] * PAIRS
            for i in range(PAIRS):
                value = steps[i] if i < half else steps_ref[(i, a, *at)]
                changes[i] = curvature_ref[(i, a, *at)] * value
                changes_ref[(i, a, *at)] = changes[i]
            sums = [sums[k] + steps[k // PAIRS] * changes[k % PAIRS] for k in range(half * PAIRS)]
        return sums

    def second(a, sums):
        for at in spots(plane):
            steps = [steps_ref[(i, a, *at)] for i in range(half, PAIRS)]
            changes = [changes_ref[(i, a, *at)] for i in range(PAIRS)]
            sums = [sums[k] + steps[k // PAIRS] * changes[k % PAIRS] for k in range(half * PAIRS)]
        return sums

    def squares(a, sums):
        for at in spots(plane):
            changes = [changes_ref[(i, a, *at)] for i in range(PAIRS)]
            sums = [value + changes[i] * changes[j] for value, (i, j) in zip(sums, upper)]
        return sums

    row = placed(enumerate(summed_over(lons, first, half * PAIRS)))
    row = row + placed(enumerate(summed_over(lons, second, half * PAIRS), half * PAIRS))
    row_ref[...] = row + placed(enumerate(summed_over(lons, squares, len(upper)), SQUARES))


def near_base():
    return RIM * (1 - lax.rem(cut_number(), 2))


def side_products(base, halo_ref, side_ref, inner_ref, steps_ref, changes_ref, gradient_ref, padded_ref):
    lons, rows, lats = gradient_ref.shape
    weights = cycle_weights()
    outer = 2 * base // RIM
    padded_ref[outer] = halo_ref[...]
    padded_ref[1] = side_ref[...]
    padded_ref[2 - outer] = inner_ref[...]
    sums = [jnp.zeros((8, LANES), jnp.float32) for _ in range(2 * PAIRS)]
    for at in spots((rows, lats)):
        padded = [padded_ref[(k, a, *at)] for k in range(3) for a in range(RIM)]
        for a in range(lons):
            value = weights[RIM] * padded[a + RIM]
            for k in range(RIM):
                value = value + weights[k] * (padded[a + k] + padded[a + 2 * RIM - k])
            gradient_ref[(a, *at)] = value
            for pair in range(PAIRS):
                sums[pair] = sums[pair] + steps_ref[(pair, base + a, *at)] * value
                sums[PAIRS + pair] = sums[PAIRS + pair] + changes_ref[(pair, base + a, *at)] * value
    return placed(enumerate(sums, STEPS_GRADIENT))


def near_product_kernel(
    halo_ref, near_ref, far_ref, steps_ref, changes_ref, gram_ref, gradient_ref, row_ref, padded_ref
):
    operands = (halo_ref, near_ref, far_ref, steps_ref, changes_ref, gradient_ref, padded_ref)
    row_ref[...] = gram_ref[...] + side_products(near_base(), *operands)


def far_product_kernel(
    halo_ref, far_ref, near_ref, steps_ref, changes_ref, near_row_ref, gradient_ref, rows_ref, padded_ref
):
    operands = (halo_ref, far_ref, near_ref, steps_ref, changes_ref, gradient_ref, padded_ref)
    row = near_row_ref[...] + side_products(RIM - near_base(), *operands)
    row = jnp.sum(row, axis=0, keepdims=True)
    rows_ref[...] = jnp.broadcast_to(row[None], rows_ref.shape)


def direction_kernel(
    rows_ref, far_ref, near_ref, steps_ref, changes_ref,
    gradient_out, direction_out, direction_ref, semaphores,
):
    sides = ((RIM - near_base(), far_ref), (near_base(), near_ref))
    written = [
        pltpu.make_async_copy(ref, gradient_out.at[pl.ds(base, RIM)], semaphores.at[k])
        for k, (base, ref) in enumerate(sides)
    ]
    for copy in written:
        copy.start()
    row = jnp.broadcast_to(jnp.sum(rows_ref[...], axis=0), (8, LANES))
    lanes = lane_numbers()
    pairs = lax.broadcasted_iota(jnp.int32, (8, LANES), 0)

    def column(lane_of):
        picked = jnp.where(lanes == lane_of, row, 0.0)
        return jnp.broadcast_to(jnp.sum(picked, axis=1, keepdims=True), (8, LANES))

    def element(vector, i):
        return jnp.broadcast_to(vector[i : i + 1], (8, LANES))

    def square_lanes(j):
        low, high = jnp.minimum(pairs, j), jnp.maximum(pairs, j)
        return SQUARES + low * PAIRS - ((low * (low - 1)) >> 1) + high - low

    by_change = [column(pairs * PAIRS + i) for i in range(PAIRS)]
    by_step = [column(pairs + PAIRS * i) for i in range(PAIRS)]
    squares = [column(square_lanes(i)) for i in range(PAIRS)]
    curvs = column(pairs * (PAIRS + 1))
    steps_part = column(pairs + STEPS_GRADIENT)
    changes_part = column(pairs + CHANGES_GRADIENT)
    inverse = 1.0 / curvs
    scaling = element(curvs, PAIRS - 1) / element(squares[PAIRS - 1], PAIRS - 1)
    alphas = [None] * PAIRS
    for i in reversed(range(PAIRS)):
        alphas[i] = element(inverse * steps_part, i)
        steps_part = steps_part - alphas[i] * by_change[i]
        changes_part = changes_part - alphas[i] * squares[i]
    changes_part = scaling * changes_part
    weights = [None] * PAIRS
    for i in range(PAIRS):
        weights[i] = alphas[i] - element(inverse * changes_part, i)
        changes_part = changes_part + weights[i] * by_step[i]
    change_weights = [scaling * alpha for alpha in alphas]
    copies = []
    half = RIM // 2
    for piece in range(4):
        base, gradient_ref = sides[piece // 2]
        first = piece % 2 * half
        for a, r, b in tiles((half, *far_ref.shape[1:])):
            lon = base + first + a
            value = -(scaling * gradient_ref[first + a, r, b])
            for i in range(PAIRS):
                value = value + change_weights[i] * changes_ref[i, lon, r, b]
                value = value - weights[i] * steps_ref[i, lon, r, b]
            direction_ref[half * piece + a, r, b] = value
        if copies:
            copies[-1].start()
        copies.append(
            pltpu.make_async_copy(
                direction_ref.at[pl.ds(half * piece, half)],
                direction_out.at[pl.ds(base + first, half)],
                semaphores.at[2 + piece],
            )
        )
    copies[-1].start()
    for copy in copies + written:
        copy.wait()


def in_hbm(x):
    return pltpu.with_memory_space_constraint(x, pltpu.HBM)


def swapped(x, axis):
    return lax.ppermute(x, axis, [(0, 1), (1, 0)])


def cut_number():
    number = 0
    for axis in CUTS:
        number = number * lax.axis_size(axis) + lax.axis_index(axis)
    return number


def shards(kernels, steps, curvature):
    _, lons, rad_len, lats = kernels.shape
    rows = rad_len // 4
    block = ((lons, rows, lats), jnp.float32)
    size = lons * rows * lats
    half = ((RIM, rows, lats), jnp.float32)
    cuts, events = lax.axis_size(CUTS), lax.axis_size(EVENT)
    table = ((2 * rad_len, 2 * rad_len), jnp.bfloat16)
    flops = 4 * rad_len * kernels.size
    far_keep, far_pass, far_send_keep, far_send_pass, near_field, weights = call(
        far_radial_kernel,
        [half] * 4 + [((RIM, rad_len, lats), jnp.float32), table],
        flops,
        8 * kernels.size,
        in_specs=[pl.BlockSpec(memory_space=pltpu.HBM)],
        scratch_shapes=[
            pltpu.VMEM((RIM, rad_len, lats), jnp.float32),
            pltpu.SemaphoreType.DMA((2,)),
        ],
    )(in_hbm(kernels))
    far_core_pass = swapped(far_send_pass, "event_1")
    square = ((lats, lats), jnp.bfloat16)
    near_keep, near_pass, rest, high, low = call(
        near_radial_kernel,
        [half, half, ((3, RIM, rows, lats), jnp.float32), square, square],
        flops,
        4 * kernels.size,
    )(near_field, weights, far_send_keep)
    far_chip = swapped(far_pass + far_core_pass, "event_0")
    rest = swapped(rest, "event_1")
    near_chip = swapped(near_pass + rest[0], "event_0")
    row = ((8, LANES), jnp.float32)
    (held_curvature,) = call(
        fetch_kernel,
        [(curvature.shape, jnp.float32)],
        0,
        8 * curvature.size,
        in_specs=[pl.BlockSpec(memory_space=pltpu.HBM)],
        scratch_shapes=[pltpu.SemaphoreType.DMA],
    )(in_hbm(curvature))
    changes, gram = call(
        gram_kernel,
        [(steps.shape, jnp.float32), row],
        2 * 108 * size,
        12 * steps.size,
    )(steps, held_curvature)

    def plane_of(slot, *parts):
        kernel = functools.partial(latitude_kernel, slot)
        return call(kernel, [half], 4 * lats * size, 8 * size)(*parts, high, low)[0]

    far_plane = plane_of(2, far_keep, rest, far_chip)
    pairs = []
    for c in range(cuts):
        other, flip = (((c - 1) ^ 1) + 1) % cuts if c else cuts - 1, 2 if c == 0 else 0
        pairs += [(c * events + e, other * events + (e ^ flip)) for e in range(events)]
    far_halo = lax.ppermute(far_plane, CUTS_EVENT, pairs)
    far_plane = lax.ppermute(
        far_plane,
        CUTS_EVENT,
        [(e, e ^ 2) for e in range(events)] + [(d, d) for d in range(events, cuts * events)],
    )
    near_plane = plane_of(1, near_keep, rest, near_chip)
    near_halo = lax.ppermute(near_plane, CUTS, [(c, c ^ 1) for c in range(cuts)])
    padded = [pltpu.VMEM((3, RIM, rows, lats), jnp.float32)]
    near_gradient, near_row = call(
        near_product_kernel, [half, row], 2 * 20 * size, 4 * 10 * size, scratch_shapes=padded
    )(near_halo, near_plane, far_plane, steps, changes, gram)
    far_gradient, outgoing = call(
        far_product_kernel,
        [half, ((cuts * events, 1, LANES), jnp.float32)],
        2 * 20 * size,
        4 * 10 * size,
        scratch_shapes=padded,
    )(far_halo, far_plane, near_plane, steps, changes, near_row)
    arrived = lax.all_to_all(outgoing, CUTS_EVENT, 0, 0, tiled=True)
    return call(
        direction_kernel,
        [block] * 2,
        2 * 17 * size,
        4 * 18 * size,
        out_specs=[pl.BlockSpec(memory_space=pltpu.HBM)] * 2,
        scratch_shapes=[pltpu.VMEM((lons, rows, lats), jnp.float32), pltpu.SemaphoreType.DMA((6,))],
    )(arrived, far_gradient, near_gradient, steps, changes)


def solution(mesh):
    torus = Mesh(
        mesh.devices.reshape(2, 4, 4, 2, 2), ("cuts_0", "cuts_1", "cuts_2", "event_0", "event_1")
    )
    in_specs = (P(EVENT, CUTS, None, None), P(None, CUTS, EVENT, None), P(None, CUTS, EVENT, None))
    out_specs = (P(CUTS, EVENT, None), P(CUTS, EVENT, None))
    return jax.shard_map(
        shards, mesh=torus, in_specs=in_specs, out_specs=out_specs, check_vma=False
    )
```

```python
import functools
import math

import jax
import jax.numpy as jnp
from jax import lax
from jax.experimental import pallas as pl
from jax.experimental.pallas import tpu as pltpu
from jax.sharding import Mesh
from jax.sharding import PartitionSpec as P

PAIRS = 8
RIM = 4
CUTS = ("cuts_0", "cuts_1", "cuts_2")
EVENT = ("event_0", "event_1")
CUTS_EVENT = ("cuts_0", "cuts_1", "cuts_2", "event_0", "event_1")
LANES = 128
SQUARES, STEPS_GRADIENT, CHANGES_GRADIENT = 64, 100, 108


def cycle_weights():
    unscaled = [math.exp(-((column - RIM) ** 2) / 4.5) for column in range(2 * RIM + 1)]
    whole = sum(unscaled)
    return [weight / whole for weight in unscaled]


def split(x):
    high = x.astype(jnp.bfloat16)
    low = (x - high.astype(jnp.float32)).astype(jnp.bfloat16)
    return high, low


def dot(a, b):
    return jnp.dot(a, b, preferred_element_type=jnp.float32)


def call(kernel, outs, flops, moved, limit=16, **options):
    return pl.pallas_call(
        kernel,
        out_shape=[jax.ShapeDtypeStruct(*out) for out in outs],
        compiler_params=pltpu.CompilerParams(vmem_limit_bytes=limit << 20),
        cost_estimate=pl.CostEstimate(flops=flops, bytes_accessed=moved, transcendentals=0),
        **options,
    )


def gauss_rows(length, sigma, rows, axis):
    offset = (rows - lax.broadcasted_iota(jnp.int32, rows.shape, axis)).astype(jnp.float32)
    matrix = jnp.exp(-offset * offset / (2.0 * sigma * sigma))
    return matrix / jnp.sum(matrix, axis=axis, keepdims=True)


def gauss_rows(length, sigma, rows, axis):
    offset = (rows - lax.broadcasted_iota(jnp.int32, rows.shape, axis)).astype(jnp.float32)
    matrix = jnp.exp(-offset * offset / (2.0 * sigma * sigma))
    return matrix / jnp.sum(matrix, axis=axis, keepdims=True)


def radial_products(field_ref, weights, keep_ref, pass_ref, send_keep_ref, send_pass_ref):
    for a in range(field_ref.shape[0]):
        both = dot(weights, jnp.concatenate(split(field_ref[a]), axis=0))
        length = both.shape[0] // 2
        rows = length // 4
        out = both[:length] + both[length:]
        for k, ref in enumerate((keep_ref, pass_ref, send_keep_ref, send_pass_ref)):
            ref[a] = out[k * rows : (k + 1) * rows]


def far_radial_kernel(
    kernels_ref, keep_ref, pass_ref, send_keep_ref, send_pass_ref, near_ref, weights_ref, far_ref, semaphores
):
    length = kernels_ref.shape[2]
    odd = lax.rem(cut_number(), 2)
    copies = []
    for piece, ref in enumerate((far_ref, near_ref)):
        source = kernels_ref.at[0, pl.ds(RIM * (odd ^ piece), RIM)]
        copies.append(pltpu.make_async_copy(source, ref, semaphores.at[piece]))
        copies[piece].start()
    part = 2 * lax.axis_index("event_0") + lax.axis_index("event_1")
    rows = length // 4
    local = lax.broadcasted_iota(jnp.int32, (rows, length), 0)

    def weights_of(first):
        order = [first, first ^ 2, first ^ 1, first ^ 3]
        matrix = jnp.concatenate(
            [gauss_rows(length, 3.0, local + rows * block, 1) for block in order], axis=0
        )
        return jnp.concatenate([jnp.concatenate([m, m], axis=1) for m in split(matrix)], axis=0)

    weights = weights_of(jnp.where(cut_number() == 0, part ^ 2, part))
    weights_ref[...] = weights_of(part)
    copies[0].wait()
    radial_products(far_ref, weights, keep_ref, pass_ref, send_keep_ref, send_pass_ref)
    copies[1].wait()


def near_radial_kernel(
    near_ref, weights_ref, far_send_keep_ref, keep_ref, pass_ref, rest_ref, high_ref, low_ref
):
    rest_ref[2] = far_send_keep_ref[...]
    parts = (keep_ref, pass_ref, rest_ref.at[1], rest_ref.at[0])
    radial_products(near_ref, weights_ref[...], *parts)
    lats = high_ref.shape[0]
    column = lax.broadcasted_iota(jnp.int32, (lats, lats), 1)
    high_ref[...], low_ref[...] = split(gauss_rows(lats, 4.0, column, 0))


def smoothed(field, high, low):
    count = field.shape[0]
    both = jnp.concatenate(split(field), axis=0)
    out = dot(both, high) + dot(both, low)
    return out[:count] + out[count:]


def latitude_kernel(slot, keep_ref, rest_ref, chip_ref, high_ref, low_ref, plane_ref):
    lons, rows, lats = plane_ref.shape
    summed = (keep_ref[...] + rest_ref[slot] + chip_ref[...]).reshape(lons * rows, lats)
    plane_ref[...] = smoothed(summed, high_ref[...], low_ref[...]).reshape(lons, rows, lats)


def lane_numbers():
    return lax.broadcasted_iota(jnp.int32, (8, LANES), 1)


def tiles(shape):
    return [
        (a, slice(8 * r, 8 * r + 8), slice(LANES * b, LANES * (b + 1)))
        for r in range(shape[1] // 8)
        for b in range(shape[2] // LANES)
        for a in range(shape[0])
    ]


def placed(sums):
    lanes = lane_numbers()
    row = jnp.zeros((8, LANES), jnp.float32)
    for lane, value in sums:
        row = row + jnp.where(lanes == lane, jnp.sum(value, axis=1, keepdims=True), 0.0)
    return row


def spots(shape):
    return [
        (slice(8 * r, 8 * r + 8), slice(LANES * b, LANES * (b + 1)))
        for r in range(shape[0] // 8)
        for b in range(shape[1] // LANES)
    ]


def summed_over(lons, step, size):
    return lax.fori_loop(0, lons, step, [jnp.zeros((8, LANES), jnp.float32)] * size)


def first_gram_kernel(
    steps_hbm, curvature_hbm, steps_ref, changes_ref, row_ref, curvature_ref, semaphores
):
    lons, *plane = steps_ref.shape[1:]

    def fetches(a):
        pairs = ((steps_hbm, steps_ref), (curvature_hbm, curvature_ref))
        return [
            pltpu.make_async_copy(source.at[:, a], target.at[:, a], semaphores.at[k, a])
            for k, (source, target) in enumerate(pairs)
        ]

    for a in range(lons):
        for fetch in fetches(a):
            fetch.start()
    half = PAIRS // 2

    def step(a, sums):
        for fetch in fetches(a):
            fetch.wait()
        for at in spots(plane):
            steps = [steps_ref[(i, a, *at)] for i in range(half)]
            changes = [None] * PAIRS
            for i in range(PAIRS):
                value = steps[i] if i < half else steps_ref[(i, a, *at)]
                changes[i] = curvature_ref[(i, a, *at)] * value
                changes_ref[(i, a, *at)] = changes[i]
            sums = [sums[k] + steps[k // PAIRS] * changes[k % PAIRS] for k in range(half * PAIRS)]
        return sums

    row_ref[...] = placed(enumerate(summed_over(lons, step, half * PAIRS)))


def second_gram_kernel(steps_ref, changes_ref, first_ref, row_ref):
    lons, *plane = steps_ref.shape[1:]
    half = PAIRS // 2
    upper = [(i, j) for i in range(PAIRS) for j in range(i, PAIRS)]

    def mixed(a, sums):
        for at in spots(plane):
            steps = [steps_ref[(i, a, *at)] for i in range(half, PAIRS)]
            changes = [changes_ref[(i, a, *at)] for i in range(PAIRS)]
            sums = [sums[k] + steps[k // PAIRS] * changes[k % PAIRS] for k in range(half * PAIRS)]
        return sums

    def squares(a, sums):
        for at in spots(plane):
            changes = [changes_ref[(i, a, *at)] for i in range(PAIRS)]
            sums = [value + changes[i] * changes[j] for value, (i, j) in zip(sums, upper)]
        return sums

    row = first_ref[...] + placed(enumerate(summed_over(lons, mixed, half * PAIRS), half * PAIRS))
    row_ref[...] = row + placed(enumerate(summed_over(lons, squares, len(upper)), SQUARES))


def near_base():
    return RIM * (1 - lax.rem(cut_number(), 2))


def side_products(base, halo_ref, side_ref, inner_ref, steps_ref, changes_ref, gradient_ref, padded_ref):
    lons, rows, lats = gradient_ref.shape
    weights = cycle_weights()
    outer = 2 * base // RIM
    padded_ref[outer] = halo_ref[...]
    padded_ref[1] = side_ref[...]
    padded_ref[2 - outer] = inner_ref[...]
    sums = [jnp.zeros((8, LANES), jnp.float32) for _ in range(2 * PAIRS)]
    for at in spots((rows, lats)):
        padded = [padded_ref[(k, a, *at)] for k in range(3) for a in range(RIM)]
        for a in range(lons):
            value = weights[RIM] * padded[a + RIM]
            for k in range(RIM):
                value = value + weights[k] * (padded[a + k] + padded[a + 2 * RIM - k])
            gradient_ref[(a, *at)] = value
            for pair in range(PAIRS):
                sums[pair] = sums[pair] + steps_ref[(pair, base + a, *at)] * value
                sums[PAIRS + pair] = sums[PAIRS + pair] + changes_ref[(pair, base + a, *at)] * value
    return placed(enumerate(sums, STEPS_GRADIENT))


def near_product_kernel(
    halo_ref, near_ref, far_ref, steps_ref, changes_ref, gram_ref, gradient_ref, row_ref, padded_ref
):
    operands = (halo_ref, near_ref, far_ref, steps_ref, changes_ref, gradient_ref, padded_ref)
    row_ref[...] = gram_ref[...] + side_products(near_base(), *operands)


def far_product_kernel(
    halo_ref, far_ref, near_ref, steps_ref, changes_ref, near_row_ref, gradient_ref, rows_ref, padded_ref
):
    operands = (halo_ref, far_ref, near_ref, steps_ref, changes_ref, gradient_ref, padded_ref)
    row = near_row_ref[...] + side_products(RIM - near_base(), *operands)
    row = jnp.sum(row, axis=0, keepdims=True)
    rows_ref[...] = jnp.broadcast_to(row[None], rows_ref.shape)


def direction_kernel(
    rows_ref, far_ref, near_ref, steps_ref, changes_ref,
    gradient_out, direction_out, direction_ref, semaphores,
):
    sides = ((RIM - near_base(), far_ref), (near_base(), near_ref))
    written = [
        pltpu.make_async_copy(ref, gradient_out.at[pl.ds(base, RIM)], semaphores.at[k])
        for k, (base, ref) in enumerate(sides)
    ]
    for copy in written:
        copy.start()
    row = jnp.broadcast_to(jnp.sum(rows_ref[...], axis=0), (8, LANES))
    lanes = lane_numbers()
    pairs = lax.broadcasted_iota(jnp.int32, (8, LANES), 0)

    def column(lane_of):
        picked = jnp.where(lanes == lane_of, row, 0.0)
        return jnp.broadcast_to(jnp.sum(picked, axis=1, keepdims=True), (8, LANES))

    def element(vector, i):
        return jnp.broadcast_to(vector[i : i + 1], (8, LANES))

    def square_lanes(j):
        low, high = jnp.minimum(pairs, j), jnp.maximum(pairs, j)
        return SQUARES + low * PAIRS - ((low * (low - 1)) >> 1) + high - low

    by_change = [column(pairs * PAIRS + i) for i in range(PAIRS)]
    by_step = [column(pairs + PAIRS * i) for i in range(PAIRS)]
    squares = [column(square_lanes(i)) for i in range(PAIRS)]
    curvs = column(pairs * (PAIRS + 1))
    steps_part = column(pairs + STEPS_GRADIENT)
    changes_part = column(pairs + CHANGES_GRADIENT)
    inverse = 1.0 / curvs
    scaling = element(curvs, PAIRS - 1) / element(squares[PAIRS - 1], PAIRS - 1)
    alphas = [None] * PAIRS
    for i in reversed(range(PAIRS)):
        alphas[i] = element(inverse * steps_part, i)
        steps_part = steps_part - alphas[i] * by_change[i]
        changes_part = changes_part - alphas[i] * squares[i]
    changes_part = scaling * changes_part
    weights = [None] * PAIRS
    for i in range(PAIRS):
        weights[i] = alphas[i] - element(inverse * changes_part, i)
        changes_part = changes_part + weights[i] * by_step[i]
    change_weights = [scaling * alpha for alpha in alphas]
    copies = []
    half = RIM // 2
    for piece in range(4):
        base, gradient_ref = sides[piece // 2]
        first = piece % 2 * half
        for a, r, b in tiles((half, *far_ref.shape[1:])):
            lon = base + first + a
            value = -(scaling * gradient_ref[first + a, r, b])
            for i in range(PAIRS):
                value = value + change_weights[i] * changes_ref[i, lon, r, b]
                value = value - weights[i] * steps_ref[i, lon, r, b]
            direction_ref[half * piece + a, r, b] = value
        if copies:
            copies[-1].start()
        copies.append(
            pltpu.make_async_copy(
                direction_ref.at[pl.ds(half * piece, half)],
                direction_out.at[pl.ds(base + first, half)],
                semaphores.at[2 + piece],
            )
        )
    copies[-1].start()
    for copy in copies + written:
        copy.wait()


def in_hbm(x):
    return pltpu.with_memory_space_constraint(x, pltpu.HBM)


def swapped(x, axis):
    return lax.ppermute(x, axis, [(0, 1), (1, 0)])


def cut_number():
    number = 0
    for axis in CUTS:
        number = number * lax.axis_size(axis) + lax.axis_index(axis)
    return number


def shards(kernels, steps, curvature):
    _, lons, rad_len, lats = kernels.shape
    rows = rad_len // 4
    block = ((lons, rows, lats), jnp.float32)
    size = lons * rows * lats
    half = ((RIM, rows, lats), jnp.float32)
    cuts, events = lax.axis_size(CUTS), lax.axis_size(EVENT)
    table = ((2 * rad_len, 2 * rad_len), jnp.bfloat16)
    flops = 4 * rad_len * kernels.size
    far_keep, far_pass, far_send_keep, far_send_pass, near_field, weights = call(
        far_radial_kernel,
        [half] * 4 + [((RIM, rad_len, lats), jnp.float32), table],
        flops,
        8 * kernels.size,
        in_specs=[pl.BlockSpec(memory_space=pltpu.HBM)],
        scratch_shapes=[
            pltpu.VMEM((RIM, rad_len, lats), jnp.float32),
            pltpu.SemaphoreType.DMA((2,)),
        ],
    )(in_hbm(kernels))
    far_core_pass = swapped(far_send_pass, "event_1")
    square = ((lats, lats), jnp.bfloat16)
    near_keep, near_pass, rest, high, low = call(
        near_radial_kernel,
        [half, half, ((3, RIM, rows, lats), jnp.float32), square, square],
        flops,
        4 * kernels.size,
    )(near_field, weights, far_send_keep)
    far_chip = swapped(far_pass + far_core_pass, "event_0")
    rest = swapped(rest, "event_1")
    near_chip = swapped(near_pass + rest[0], "event_0")
    row = ((8, LANES), jnp.float32)
    held_steps, changes, first_row = call(
        first_gram_kernel,
        [(steps.shape, jnp.float32)] * 2 + [row],
        2 * 40 * size,
        16 * steps.size,
        in_specs=[pl.BlockSpec(memory_space=pltpu.HBM)] * 2,
        scratch_shapes=[
            pltpu.VMEM(curvature.shape, jnp.float32),
            pltpu.SemaphoreType.DMA((2, lons)),
        ],
    )(in_hbm(steps), in_hbm(curvature))
    (gram,) = call(second_gram_kernel, [row], 2 * 68 * size, 8 * steps.size)(
        held_steps, changes, first_row
    )

    def plane_of(slot, *parts):
        kernel = functools.partial(latitude_kernel, slot)
        return call(kernel, [half], 4 * lats * size, 8 * size)(*parts, high, low)[0]

    far_plane = plane_of(2, far_keep, rest, far_chip)
    pairs = []
    for c in range(cuts):
        other, flip = (((c - 1) ^ 1) + 1) % cuts if c else cuts - 1, 2 if c == 0 else 0
        pairs += [(c * events + e, other * events + (e ^ flip)) for e in range(events)]
    far_halo = lax.ppermute(far_plane, CUTS_EVENT, pairs)
    far_plane = lax.ppermute(
        far_plane,
        CUTS_EVENT,
        [(e, e ^ 2) for e in range(events)] + [(d, d) for d in range(events, cuts * events)],
    )
    near_plane = plane_of(1, near_keep, rest, near_chip)
    near_halo = lax.ppermute(near_plane, CUTS, [(c, c ^ 1) for c in range(cuts)])
    padded = [pltpu.VMEM((3, RIM, rows, lats), jnp.float32)]
    near_gradient, near_row = call(
        near_product_kernel, [half, row], 2 * 20 * size, 4 * 10 * size, scratch_shapes=padded
    )(near_halo, near_plane, far_plane, held_steps, changes, gram)
    far_gradient, outgoing = call(
        far_product_kernel,
        [half, ((cuts * events, 1, LANES), jnp.float32)],
        2 * 20 * size,
        4 * 10 * size,
        scratch_shapes=padded,
    )(far_halo, far_plane, near_plane, held_steps, changes, near_row)
    arrived = lax.all_to_all(outgoing, CUTS_EVENT, 0, 0, tiled=True)
    return call(
        direction_kernel,
        [block] * 2,
        2 * 17 * size,
        4 * 18 * size,
        out_specs=[pl.BlockSpec(memory_space=pltpu.HBM)] * 2,
        scratch_shapes=[pltpu.VMEM((lons, rows, lats), jnp.float32), pltpu.SemaphoreType.DMA((6,))],
    )(arrived, far_gradient, near_gradient, held_steps, changes)


def solution(mesh):
    torus = Mesh(
        mesh.devices.reshape(2, 4, 4, 2, 2), ("cuts_0", "cuts_1", "cuts_2", "event_0", "event_1")
    )
    in_specs = (P(EVENT, CUTS, None, None), P(None, CUTS, EVENT, None), P(None, CUTS, EVENT, None))
    out_specs = (P(CUTS, EVENT, None), P(CUTS, EVENT, None))
    return jax.shard_map(
        shards, mesh=torus, in_specs=in_specs, out_specs=out_specs, check_vma=False
    )
```

```python
import functools
import math

import jax
import jax.numpy as jnp
from jax import lax
from jax.experimental import pallas as pl
from jax.experimental.pallas import tpu as pltpu
from jax.sharding import Mesh
from jax.sharding import PartitionSpec as P

PAIRS = 8
RIM = 4
CUTS = ("cuts_0", "cuts_1", "cuts_2")
EVENT = ("event_0", "event_1")
CUTS_EVENT = ("cuts_0", "cuts_1", "cuts_2", "event_0", "event_1")
LANES = 128
SQUARES, STEPS_GRADIENT, CHANGES_GRADIENT = 64, 100, 108


def cycle_weights():
    unscaled = [math.exp(-((column - RIM) ** 2) / 4.5) for column in range(2 * RIM + 1)]
    whole = sum(unscaled)
    return [weight / whole for weight in unscaled]


def split(x):
    high = x.astype(jnp.bfloat16)
    low = (x - high.astype(jnp.float32)).astype(jnp.bfloat16)
    return high, low


def dot(a, b):
    return jnp.dot(a, b, preferred_element_type=jnp.float32)


def call(kernel, outs, flops, moved, limit=16, **options):
    return pl.pallas_call(
        kernel,
        out_shape=[jax.ShapeDtypeStruct(*out) for out in outs],
        compiler_params=pltpu.CompilerParams(vmem_limit_bytes=limit << 20),
        cost_estimate=pl.CostEstimate(flops=flops, bytes_accessed=moved, transcendentals=0),
        **options,
    )


def gauss_rows(length, sigma, rows, axis):
    offset = (rows - lax.broadcasted_iota(jnp.int32, rows.shape, axis)).astype(jnp.float32)
    matrix = jnp.exp(-offset * offset / (2.0 * sigma * sigma))
    return matrix / jnp.sum(matrix, axis=axis, keepdims=True)


def gauss_rows(length, sigma, rows, axis):
    offset = (rows - lax.broadcasted_iota(jnp.int32, rows.shape, axis)).astype(jnp.float32)
    matrix = jnp.exp(-offset * offset / (2.0 * sigma * sigma))
    return matrix / jnp.sum(matrix, axis=axis, keepdims=True)


def radial_products(field_ref, weights, keep_ref, pass_ref, send_keep_ref, send_pass_ref):
    for a in range(field_ref.shape[0]):
        both = dot(weights, jnp.concatenate(split(field_ref[a]), axis=0))
        length = both.shape[0] // 2
        rows = length // 4
        out = both[:length] + both[length:]
        for k, ref in enumerate((keep_ref, pass_ref, send_keep_ref, send_pass_ref)):
            ref[a] = out[k * rows : (k + 1) * rows]


def far_radial_kernel(
    kernels_ref, keep_ref, pass_ref, send_keep_ref, send_pass_ref, near_ref, weights_ref, far_ref, semaphores
):
    length = kernels_ref.shape[2]
    odd = lax.rem(cut_number(), 2)
    copies = []
    for piece, ref in enumerate((far_ref, near_ref)):
        source = kernels_ref.at[0, pl.ds(RIM * (odd ^ piece), RIM)]
        copies.append(pltpu.make_async_copy(source, ref, semaphores.at[piece]))
        copies[piece].start()
    part = 2 * lax.axis_index("event_0") + lax.axis_index("event_1")
    rows = length // 4
    local = lax.broadcasted_iota(jnp.int32, (rows, length), 0)

    def weights_of(first):
        order = [first, first ^ 2, first ^ 1, first ^ 3]
        matrix = jnp.concatenate(
            [gauss_rows(length, 3.0, local + rows * block, 1) for block in order], axis=0
        )
        return jnp.concatenate([jnp.concatenate([m, m], axis=1) for m in split(matrix)], axis=0)

    weights = weights_of(jnp.where(cut_number() == 0, part ^ 2, part))
    weights_ref[...] = weights_of(part)
    copies[0].wait()
    radial_products(far_ref, weights, keep_ref, pass_ref, send_keep_ref, send_pass_ref)
    copies[1].wait()


def near_radial_kernel(
    near_ref, weights_ref, far_send_keep_ref, keep_ref, pass_ref, rest_ref, high_ref, low_ref
):
    rest_ref[2] = far_send_keep_ref[...]
    parts = (keep_ref, pass_ref, rest_ref.at[1], rest_ref.at[0])
    radial_products(near_ref, weights_ref[...], *parts)
    lats = high_ref.shape[0]
    column = lax.broadcasted_iota(jnp.int32, (lats, lats), 1)
    high_ref[...], low_ref[...] = split(gauss_rows(lats, 4.0, column, 0))


def smoothed(field, high, low):
    count = field.shape[0]
    both = jnp.concatenate(split(field), axis=0)
    out = dot(both, high) + dot(both, low)
    return out[:count] + out[count:]


def latitude_kernel(slot, keep_ref, rest_ref, chip_ref, high_ref, low_ref, plane_ref):
    lons, rows, lats = plane_ref.shape
    summed = (keep_ref[...] + rest_ref[slot] + chip_ref[...]).reshape(lons * rows, lats)
    plane_ref[...] = smoothed(summed, high_ref[...], low_ref[...]).reshape(lons, rows, lats)


def lane_numbers():
    return lax.broadcasted_iota(jnp.int32, (8, LANES), 1)


def tiles(shape):
    return [
        (a, slice(8 * r, 8 * r + 8), slice(LANES * b, LANES * (b + 1)))
        for r in range(shape[1] // 8)
        for b in range(shape[2] // LANES)
        for a in range(shape[0])
    ]


def placed(sums):
    lanes = lane_numbers()
    row = jnp.zeros((8, LANES), jnp.float32)
    for lane, value in sums:
        row = row + jnp.where(lanes == lane, jnp.sum(value, axis=1, keepdims=True), 0.0)
    return row


def spots(shape):
    return [
        (slice(8 * r, 8 * r + 8), slice(LANES * b, LANES * (b + 1)))
        for r in range(shape[0] // 8)
        for b in range(shape[1] // LANES)
    ]


def summed_over(lons, step, size):
    return lax.fori_loop(0, lons, step, [jnp.zeros((8, LANES), jnp.float32)] * size)


def fetch_kernel(curvature_hbm, curvature_ref, semaphore):
    copy = pltpu.make_async_copy(curvature_hbm, curvature_ref, semaphore)
    copy.start()
    copy.wait()


def gram_kernel(steps_ref, curvature_ref, changes_ref, row_ref):
    lons, *plane = steps_ref.shape[1:]
    half = PAIRS // 2
    upper = [(i, j) for i in range(PAIRS) for j in range(i, PAIRS)]

    def first(a, sums):
        for at in spots(plane):
            steps = [steps_ref[(i, a, *at)] for i in range(half)]
            changes = [None] * PAIRS
            for i in range(PAIRS):
                value = steps[i] if i < half else steps_ref[(i, a, *at)]
                changes[i] = curvature_ref[(i, a, *at)] * value
                changes_ref[(i, a, *at)] = changes[i]
            sums = [sums[k] + steps[k // PAIRS] * changes[k % PAIRS] for k in range(half * PAIRS)]
        return sums

    def second(a, sums):
        for at in spots(plane):
            steps = [steps_ref[(i, a, *at)] for i in range(half, PAIRS)]
            changes = [changes_ref[(i, a, *at)] for i in range(PAIRS)]
            sums = [sums[k] + steps[k // PAIRS] * changes[k % PAIRS] for k in range(half * PAIRS)]
        return sums

    def squares(a, sums):
        for at in spots(plane):
            changes = [changes_ref[(i, a, *at)] for i in range(PAIRS)]
            sums = [value + changes[i] * changes[j] for value, (i, j) in zip(sums, upper)]
        return sums

    row = placed(enumerate(summed_over(lons, first, half * PAIRS)))
    row = row + placed(enumerate(summed_over(lons, second, half * PAIRS), half * PAIRS))
    row_ref[...] = row + placed(enumerate(summed_over(lons, squares, len(upper)), SQUARES))


def near_base():
    return RIM * (1 - lax.rem(cut_number(), 2))


def side_products(base, halo_ref, side_ref, inner_ref, steps_ref, changes_ref, gradient_ref, padded_ref):
    lons, rows, lats = gradient_ref.shape
    weights = cycle_weights()
    outer = 2 * base // RIM
    padded_ref[outer] = halo_ref[...]
    padded_ref[1] = side_ref[...]
    padded_ref[2 - outer] = inner_ref[...]
    sums = [jnp.zeros((8, LANES), jnp.float32) for _ in range(2 * PAIRS)]
    for at in spots((rows, lats)):
        padded = [padded_ref[(k, a, *at)] for k in range(3) for a in range(RIM)]
        for a in range(lons):
            value = weights[RIM] * padded[a + RIM]
            for k in range(RIM):
                value = value + weights[k] * (padded[a + k] + padded[a + 2 * RIM - k])
            gradient_ref[(a, *at)] = value
            for pair in range(PAIRS):
                sums[pair] = sums[pair] + steps_ref[(pair, base + a, *at)] * value
                sums[PAIRS + pair] = sums[PAIRS + pair] + changes_ref[(pair, base + a, *at)] * value
    return placed(enumerate(sums, STEPS_GRADIENT))


def near_product_kernel(
    halo_ref, near_ref, far_ref, steps_ref, changes_ref, gram_ref, gradient_ref, row_ref, padded_ref
):
    operands = (halo_ref, near_ref, far_ref, steps_ref, changes_ref, gradient_ref, padded_ref)
    row_ref[...] = gram_ref[...] + side_products(near_base(), *operands)


def far_product_kernel(
    halo_ref, far_ref, near_ref, steps_ref, changes_ref, near_row_ref, gradient_ref, rows_ref, padded_ref
):
    operands = (halo_ref, far_ref, near_ref, steps_ref, changes_ref, gradient_ref, padded_ref)
    row = near_row_ref[...] + side_products(RIM - near_base(), *operands)
    row = jnp.sum(row, axis=0, keepdims=True)
    rows_ref[...] = jnp.broadcast_to(row[None], rows_ref.shape)


def direction_kernel(
    rows_ref, far_ref, near_ref, steps_ref, changes_ref,
    gradient_out, direction_out, direction_ref, semaphores,
):
    sides = ((RIM - near_base(), far_ref), (near_base(), near_ref))
    written = [
        pltpu.make_async_copy(ref, gradient_out.at[pl.ds(base, RIM)], semaphores.at[k])
        for k, (base, ref) in enumerate(sides)
    ]
    for copy in written:
        copy.start()
    row = jnp.sum(jnp.sum(rows_ref[...], axis=0), axis=0, keepdims=True)
    row = jnp.broadcast_to(row, (8, LANES))
    lanes = lane_numbers()
    pairs = lax.broadcasted_iota(jnp.int32, (8, LANES), 0)

    def column(lane_of):
        picked = jnp.where(lanes == lane_of, row, 0.0)
        return jnp.broadcast_to(jnp.sum(picked, axis=1, keepdims=True), (8, LANES))

    def element(vector, i):
        return jnp.broadcast_to(vector[i : i + 1], (8, LANES))

    def square_lanes(j):
        low, high = jnp.minimum(pairs, j), jnp.maximum(pairs, j)
        return SQUARES + low * PAIRS - ((low * (low - 1)) >> 1) + high - low

    by_change = [column(pairs * PAIRS + i) for i in range(PAIRS)]
    by_step = [column(pairs + PAIRS * i) for i in range(PAIRS)]
    squares = [column(square_lanes(i)) for i in range(PAIRS)]
    curvs = column(pairs * (PAIRS + 1))
    steps_part = column(pairs + STEPS_GRADIENT)
    changes_part = column(pairs + CHANGES_GRADIENT)
    inverse = 1.0 / curvs
    scaling = element(curvs, PAIRS - 1) / element(squares[PAIRS - 1], PAIRS - 1)
    alphas = [None] * PAIRS
    for i in reversed(range(PAIRS)):
        alphas[i] = element(inverse * steps_part, i)
        steps_part = steps_part - alphas[i] * by_change[i]
        changes_part = changes_part - alphas[i] * squares[i]
    changes_part = scaling * changes_part
    weights = [None] * PAIRS
    for i in range(PAIRS):
        weights[i] = alphas[i] - element(inverse * changes_part, i)
        changes_part = changes_part + weights[i] * by_step[i]
    change_weights = [scaling * alpha for alpha in alphas]
    copies = []
    half = RIM // 2
    for piece in range(4):
        base, gradient_ref = sides[piece // 2]
        first = piece % 2 * half
        for a, r, b in tiles((half, *far_ref.shape[1:])):
            lon = base + first + a
            value = -(scaling * gradient_ref[first + a, r, b])
            for i in range(PAIRS):
                value = value + change_weights[i] * changes_ref[i, lon, r, b]
                value = value - weights[i] * steps_ref[i, lon, r, b]
            direction_ref[half * piece + a, r, b] = value
        if copies:
            copies[-1].start()
        copies.append(
            pltpu.make_async_copy(
                direction_ref.at[pl.ds(half * piece, half)],
                direction_out.at[pl.ds(base + first, half)],
                semaphores.at[2 + piece],
            )
        )
    copies[-1].start()
    for copy in copies + written:
        copy.wait()


def in_hbm(x):
    return pltpu.with_memory_space_constraint(x, pltpu.HBM)


def swapped(x, axis):
    return lax.ppermute(x, axis, [(0, 1), (1, 0)])


def cut_number():
    number = 0
    for axis in CUTS:
        number = number * lax.axis_size(axis) + lax.axis_index(axis)
    return number


def shards(kernels, steps, curvature):
    _, lons, rad_len, lats = kernels.shape
    rows = rad_len // 4
    block = ((lons, rows, lats), jnp.float32)
    size = lons * rows * lats
    half = ((RIM, rows, lats), jnp.float32)
    cuts, events = lax.axis_size(CUTS), lax.axis_size(EVENT)
    table = ((2 * rad_len, 2 * rad_len), jnp.bfloat16)
    flops = 4 * rad_len * kernels.size
    far_keep, far_pass, far_send_keep, far_send_pass, near_field, weights = call(
        far_radial_kernel,
        [half] * 4 + [((RIM, rad_len, lats), jnp.float32), table],
        flops,
        8 * kernels.size,
        in_specs=[pl.BlockSpec(memory_space=pltpu.HBM)],
        scratch_shapes=[
            pltpu.VMEM((RIM, rad_len, lats), jnp.float32),
            pltpu.SemaphoreType.DMA((2,)),
        ],
    )(in_hbm(kernels))
    far_core_pass = swapped(far_send_pass, "event_1")
    square = ((lats, lats), jnp.bfloat16)
    near_keep, near_pass, rest, high, low = call(
        near_radial_kernel,
        [half, half, ((3, RIM, rows, lats), jnp.float32), square, square],
        flops,
        4 * kernels.size,
    )(near_field, weights, far_send_keep)
    far_chip = swapped(far_pass + far_core_pass, "event_0")
    rest = swapped(rest, "event_1")
    near_chip = swapped(near_pass + rest[0], "event_0")
    row = ((8, LANES), jnp.float32)
    (held_curvature,) = call(
        fetch_kernel,
        [(curvature.shape, jnp.float32)],
        0,
        8 * curvature.size,
        in_specs=[pl.BlockSpec(memory_space=pltpu.HBM)],
        scratch_shapes=[pltpu.SemaphoreType.DMA],
    )(in_hbm(curvature))
    changes, gram = call(
        gram_kernel,
        [(steps.shape, jnp.float32), row],
        2 * 108 * size,
        12 * steps.size,
    )(steps, held_curvature)

    def plane_of(slot, *parts):
        kernel = functools.partial(latitude_kernel, slot)
        return call(kernel, [half], 4 * lats * size, 8 * size)(*parts, high, low)[0]

    far_plane = plane_of(2, far_keep, rest, far_chip)
    pairs = []
    for c in range(cuts):
        other, flip = (((c - 1) ^ 1) + 1) % cuts if c else cuts - 1, 2 if c == 0 else 0
        pairs += [(c * events + e, other * events + (e ^ flip)) for e in range(events)]
    far_halo = lax.ppermute(far_plane, CUTS_EVENT, pairs)
    far_plane = lax.ppermute(
        far_plane,
        CUTS_EVENT,
        [(e, e ^ 2) for e in range(events)] + [(d, d) for d in range(events, cuts * events)],
    )
    near_plane = plane_of(1, near_keep, rest, near_chip)
    near_halo = lax.ppermute(near_plane, CUTS, [(c, c ^ 1) for c in range(cuts)])
    padded = [pltpu.VMEM((3, RIM, rows, lats), jnp.float32)]
    near_gradient, near_row = call(
        near_product_kernel, [half, row], 2 * 20 * size, 4 * 10 * size, scratch_shapes=padded
    )(near_halo, near_plane, far_plane, steps, changes, gram)
    far_gradient, outgoing = call(
        far_product_kernel,
        [half, ((cuts * events // 8, 8, LANES), jnp.float32)],
        2 * 20 * size,
        4 * 10 * size,
        scratch_shapes=padded,
    )(far_halo, far_plane, near_plane, steps, changes, near_row)
    outgoing = outgoing.reshape(cuts * events, 1, LANES)
    arrived = lax.all_to_all(outgoing, CUTS_EVENT, 0, 0, tiled=True).reshape(-1, 8, LANES)
    return call(
        direction_kernel,
        [block] * 2,
        2 * 17 * size,
        4 * 18 * size,
        out_specs=[pl.BlockSpec(memory_space=pltpu.HBM)] * 2,
        scratch_shapes=[pltpu.VMEM((lons, rows, lats), jnp.float32), pltpu.SemaphoreType.DMA((6,))],
    )(arrived, far_gradient, near_gradient, steps, changes)


def solution(mesh):
    torus = Mesh(
        mesh.devices.reshape(2, 4, 4, 2, 2), ("cuts_0", "cuts_1", "cuts_2", "event_0", "event_1")
    )
    in_specs = (P(EVENT, CUTS, None, None), P(None, CUTS, EVENT, None), P(None, CUTS, EVENT, None))
    out_specs = (P(CUTS, EVENT, None), P(CUTS, EVENT, None))
    return jax.shard_map(
        shards, mesh=torus, in_specs=in_specs, out_specs=out_specs, check_vma=False
    )
```

```python
import functools
import math

import jax
import jax.numpy as jnp
from jax import lax
from jax.experimental import pallas as pl
from jax.experimental.pallas import tpu as pltpu
from jax.sharding import Mesh
from jax.sharding import PartitionSpec as P

PAIRS = 8
RIM = 4
CUTS = ("cuts_0", "cuts_1", "cuts_2")
EVENT = ("event_0", "event_1")
CUTS_EVENT = ("cuts_0", "cuts_1", "cuts_2", "event_0", "event_1")
LANES = 128
SQUARES, STEPS_GRADIENT, CHANGES_GRADIENT = 64, 100, 108


def cycle_weights():
    unscaled = [math.exp(-((column - RIM) ** 2) / 4.5) for column in range(2 * RIM + 1)]
    whole = sum(unscaled)
    return [weight / whole for weight in unscaled]


def split(x):
    high = x.astype(jnp.bfloat16)
    low = (x - high.astype(jnp.float32)).astype(jnp.bfloat16)
    return high, low


def dot(a, b):
    return jnp.dot(a, b, preferred_element_type=jnp.float32)


def call(kernel, outs, flops, moved, limit=16, **options):
    return pl.pallas_call(
        kernel,
        out_shape=[jax.ShapeDtypeStruct(*out) for out in outs],
        compiler_params=pltpu.CompilerParams(vmem_limit_bytes=limit << 20),
        cost_estimate=pl.CostEstimate(flops=flops, bytes_accessed=moved, transcendentals=0),
        **options,
    )


def gauss_rows(length, sigma, rows, axis):
    offset = (rows - lax.broadcasted_iota(jnp.int32, rows.shape, axis)).astype(jnp.float32)
    matrix = jnp.exp(-offset * offset / (2.0 * sigma * sigma))
    return matrix / jnp.sum(matrix, axis=axis, keepdims=True)


def gauss_rows(length, sigma, rows, axis):
    offset = (rows - lax.broadcasted_iota(jnp.int32, rows.shape, axis)).astype(jnp.float32)
    matrix = jnp.exp(-offset * offset / (2.0 * sigma * sigma))
    return matrix / jnp.sum(matrix, axis=axis, keepdims=True)


def radial_products(field_ref, weights, keep_ref, pass_ref, send_keep_ref, send_pass_ref):
    for a in range(field_ref.shape[0]):
        both = dot(weights, jnp.concatenate(split(field_ref[a]), axis=0))
        length = both.shape[0] // 2
        rows = length // 4
        out = both[:length] + both[length:]
        for k, ref in enumerate((keep_ref, pass_ref, send_keep_ref, send_pass_ref)):
            ref[a] = out[k * rows : (k + 1) * rows]


def far_radial_kernel(
    kernels_ref, keep_ref, pass_ref, send_keep_ref, send_pass_ref, near_ref, weights_ref, far_ref, semaphores
):
    length = kernels_ref.shape[2]
    odd = lax.rem(cut_number(), 2)
    copies = []
    for piece, ref in enumerate((far_ref, near_ref)):
        source = kernels_ref.at[0, pl.ds(RIM * (odd ^ piece), RIM)]
        copies.append(pltpu.make_async_copy(source, ref, semaphores.at[piece]))
        copies[piece].start()
    part = 2 * lax.axis_index("event_0") + lax.axis_index("event_1")
    rows = length // 4
    local = lax.broadcasted_iota(jnp.int32, (rows, length), 0)

    def weights_of(first):
        order = [first, first ^ 2, first ^ 1, first ^ 3]
        matrix = jnp.concatenate(
            [gauss_rows(length, 3.0, local + rows * block, 1) for block in order], axis=0
        )
        return jnp.concatenate([jnp.concatenate([m, m], axis=1) for m in split(matrix)], axis=0)

    weights = weights_of(jnp.where(cut_number() == 0, part ^ 2, part))
    weights_ref[...] = weights_of(part)
    copies[0].wait()
    radial_products(far_ref, weights, keep_ref, pass_ref, send_keep_ref, send_pass_ref)
    copies[1].wait()


def near_radial_kernel(
    near_ref, weights_ref, far_send_keep_ref, keep_ref, pass_ref, rest_ref, high_ref, low_ref
):
    rest_ref[2] = far_send_keep_ref[...]
    parts = (keep_ref, pass_ref, rest_ref.at[1], rest_ref.at[0])
    radial_products(near_ref, weights_ref[...], *parts)
    lats = high_ref.shape[0]
    column = lax.broadcasted_iota(jnp.int32, (lats, lats), 1)
    high_ref[...], low_ref[...] = split(gauss_rows(lats, 4.0, column, 0))


def smoothed(field, high, low):
    count = field.shape[0]
    both = jnp.concatenate(split(field), axis=0)
    out = dot(both, high) + dot(both, low)
    return out[:count] + out[count:]


def latitude_kernel(slot, keep_ref, rest_ref, chip_ref, high_ref, low_ref, plane_ref):
    lons, rows, lats = plane_ref.shape
    summed = (keep_ref[...] + rest_ref[slot] + chip_ref[...]).reshape(lons * rows, lats)
    plane_ref[...] = smoothed(summed, high_ref[...], low_ref[...]).reshape(lons, rows, lats)


def lane_numbers():
    return lax.broadcasted_iota(jnp.int32, (8, LANES), 1)


def tiles(shape):
    return [
        (a, slice(8 * r, 8 * r + 8), slice(LANES * b, LANES * (b + 1)))
        for r in range(shape[1] // 8)
        for b in range(shape[2] // LANES)
        for a in range(shape[0])
    ]


def placed(sums):
    lanes = lane_numbers()
    row = jnp.zeros((8, LANES), jnp.float32)
    for lane, value in sums:
        row = row + jnp.where(lanes == lane, jnp.sum(value, axis=1, keepdims=True), 0.0)
    return row


def spots(shape):
    return [
        (slice(8 * r, 8 * r + 8), slice(LANES * b, LANES * (b + 1)))
        for r in range(shape[0] // 8)
        for b in range(shape[1] // LANES)
    ]


def summed_over(lons, step, size):
    return lax.fori_loop(0, lons, step, [jnp.zeros((8, LANES), jnp.float32)] * size)


def first_gram_kernel(
    steps_hbm, curvature_hbm, steps_ref, changes_ref, row_ref, curvature_ref, semaphores
):
    lons, *plane = steps_ref.shape[1:]

    def fetches(a):
        pairs = ((steps_hbm, steps_ref), (curvature_hbm, curvature_ref))
        return [
            pltpu.make_async_copy(source.at[:, a], target.at[:, a], semaphores.at[k, a])
            for k, (source, target) in enumerate(pairs)
        ]

    for a in range(lons):
        for fetch in fetches(a):
            fetch.start()
    half = PAIRS // 2

    def step(a, sums):
        for fetch in fetches(a):
            fetch.wait()
        for at in spots(plane):
            steps = [steps_ref[(i, a, *at)] for i in range(half)]
            changes = [None] * PAIRS
            for i in range(PAIRS):
                value = steps[i] if i < half else steps_ref[(i, a, *at)]
                changes[i] = curvature_ref[(i, a, *at)] * value
                changes_ref[(i, a, *at)] = changes[i]
            sums = [sums[k] + steps[k // PAIRS] * changes[k % PAIRS] for k in range(half * PAIRS)]
        return sums

    row_ref[...] = placed(enumerate(summed_over(lons, step, half * PAIRS)))


def second_gram_kernel(steps_ref, changes_ref, first_ref, row_ref):
    lons, *plane = steps_ref.shape[1:]
    half = PAIRS // 2
    upper = [(i, j) for i in range(PAIRS) for j in range(i, PAIRS)]

    def mixed(a, sums):
        for at in spots(plane):
            steps = [steps_ref[(i, a, *at)] for i in range(half, PAIRS)]
            changes = [changes_ref[(i, a, *at)] for i in range(PAIRS)]
            sums = [sums[k] + steps[k // PAIRS] * changes[k % PAIRS] for k in range(half * PAIRS)]
        return sums

    def squares(a, sums):
        for at in spots(plane):
            changes = [changes_ref[(i, a, *at)] for i in range(PAIRS)]
            sums = [value + changes[i] * changes[j] for value, (i, j) in zip(sums, upper)]
        return sums

    row = first_ref[...] + placed(enumerate(summed_over(lons, mixed, half * PAIRS), half * PAIRS))
    row_ref[...] = row + placed(enumerate(summed_over(lons, squares, len(upper)), SQUARES))


def near_base():
    return RIM * (1 - lax.rem(cut_number(), 2))


def side_products(base, halo_ref, side_ref, inner_ref, steps_ref, changes_ref, gradient_ref, padded_ref):
    lons, rows, lats = gradient_ref.shape
    weights = cycle_weights()
    outer = 2 * base // RIM
    padded_ref[outer] = halo_ref[...]
    padded_ref[1] = side_ref[...]
    padded_ref[2 - outer] = inner_ref[...]
    sums = [jnp.zeros((8, LANES), jnp.float32) for _ in range(2 * PAIRS)]
    for at in spots((rows, lats)):
        padded = [padded_ref[(k, a, *at)] for k in range(3) for a in range(RIM)]
        for a in range(lons):
            value = weights[RIM] * padded[a + RIM]
            for k in range(RIM):
                value = value + weights[k] * (padded[a + k] + padded[a + 2 * RIM - k])
            gradient_ref[(a, *at)] = value
            for pair in range(PAIRS):
                sums[pair] = sums[pair] + steps_ref[(pair, base + a, *at)] * value
                sums[PAIRS + pair] = sums[PAIRS + pair] + changes_ref[(pair, base + a, *at)] * value
    return placed(enumerate(sums, STEPS_GRADIENT))


def near_product_kernel(
    halo_ref, near_ref, far_ref, steps_ref, changes_ref, gram_ref, gradient_ref, row_ref, padded_ref
):
    operands = (halo_ref, near_ref, far_ref, steps_ref, changes_ref, gradient_ref, padded_ref)
    row_ref[...] = gram_ref[...] + side_products(near_base(), *operands)


def far_product_kernel(
    halo_ref, far_ref, near_ref, steps_ref, changes_ref, near_row_ref, gradient_ref, rows_ref, padded_ref
):
    operands = (halo_ref, far_ref, near_ref, steps_ref, changes_ref, gradient_ref, padded_ref)
    row = near_row_ref[...] + side_products(RIM - near_base(), *operands)
    row = jnp.sum(row, axis=0, keepdims=True)
    rows_ref[...] = jnp.broadcast_to(row[None], rows_ref.shape)


def direction_kernel(
    rows_ref, far_ref, near_ref, steps_ref, changes_ref,
    gradient_out, direction_out, direction_ref, semaphores,
):
    sides = ((RIM - near_base(), far_ref), (near_base(), near_ref))
    written = [
        pltpu.make_async_copy(ref, gradient_out.at[pl.ds(base, RIM)], semaphores.at[k])
        for k, (base, ref) in enumerate(sides)
    ]
    for copy in written:
        copy.start()
    row = jnp.sum(jnp.sum(rows_ref[...], axis=0), axis=0, keepdims=True)
    row = jnp.broadcast_to(row, (8, LANES))
    lanes = lane_numbers()
    pairs = lax.broadcasted_iota(jnp.int32, (8, LANES), 0)

    def column(lane_of):
        picked = jnp.where(lanes == lane_of, row, 0.0)
        return jnp.broadcast_to(jnp.sum(picked, axis=1, keepdims=True), (8, LANES))

    def element(vector, i):
        return jnp.broadcast_to(vector[i : i + 1], (8, LANES))

    def square_lanes(j):
        low, high = jnp.minimum(pairs, j), jnp.maximum(pairs, j)
        return SQUARES + low * PAIRS - ((low * (low - 1)) >> 1) + high - low

    by_change = [column(pairs * PAIRS + i) for i in range(PAIRS)]
    by_step = [column(pairs + PAIRS * i) for i in range(PAIRS)]
    squares = [column(square_lanes(i)) for i in range(PAIRS)]
    curvs = column(pairs * (PAIRS + 1))
    steps_part = column(pairs + STEPS_GRADIENT)
    changes_part = column(pairs + CHANGES_GRADIENT)
    inverse = 1.0 / curvs
    scaling = element(curvs, PAIRS - 1) / element(squares[PAIRS - 1], PAIRS - 1)
    alphas = [None] * PAIRS
    for i in reversed(range(PAIRS)):
        alphas[i] = element(inverse * steps_part, i)
        steps_part = steps_part - alphas[i] * by_change[i]
        changes_part = changes_part - alphas[i] * squares[i]
    changes_part = scaling * changes_part
    weights = [None] * PAIRS
    for i in range(PAIRS):
        weights[i] = alphas[i] - element(inverse * changes_part, i)
        changes_part = changes_part + weights[i] * by_step[i]
    change_weights = [scaling * alpha for alpha in alphas]
    copies = []
    half = RIM // 2
    for piece in range(4):
        base, gradient_ref = sides[piece // 2]
        first = piece % 2 * half
        for a, r, b in tiles((half, *far_ref.shape[1:])):
            lon = base + first + a
            value = -(scaling * gradient_ref[first + a, r, b])
            for i in range(PAIRS):
                value = value + change_weights[i] * changes_ref[i, lon, r, b]
                value = value - weights[i] * steps_ref[i, lon, r, b]
            direction_ref[half * piece + a, r, b] = value
        if copies:
            copies[-1].start()
        copies.append(
            pltpu.make_async_copy(
                direction_ref.at[pl.ds(half * piece, half)],
                direction_out.at[pl.ds(base + first, half)],
                semaphores.at[2 + piece],
            )
        )
    copies[-1].start()
    for copy in copies + written:
        copy.wait()


def in_hbm(x):
    return pltpu.with_memory_space_constraint(x, pltpu.HBM)


def swapped(x, axis):
    return lax.ppermute(x, axis, [(0, 1), (1, 0)])


def cut_number():
    number = 0
    for axis in CUTS:
        number = number * lax.axis_size(axis) + lax.axis_index(axis)
    return number


def shards(kernels, steps, curvature):
    _, lons, rad_len, lats = kernels.shape
    rows = rad_len // 4
    block = ((lons, rows, lats), jnp.float32)
    size = lons * rows * lats
    half = ((RIM, rows, lats), jnp.float32)
    cuts, events = lax.axis_size(CUTS), lax.axis_size(EVENT)
    table = ((2 * rad_len, 2 * rad_len), jnp.bfloat16)
    flops = 4 * rad_len * kernels.size
    far_keep, far_pass, far_send_keep, far_send_pass, near_field, weights = call(
        far_radial_kernel,
        [half] * 4 + [((RIM, rad_len, lats), jnp.float32), table],
        flops,
        8 * kernels.size,
        in_specs=[pl.BlockSpec(memory_space=pltpu.HBM)],
        scratch_shapes=[
            pltpu.VMEM((RIM, rad_len, lats), jnp.float32),
            pltpu.SemaphoreType.DMA((2,)),
        ],
    )(in_hbm(kernels))
    far_core_pass = swapped(far_send_pass, "event_1")
    square = ((lats, lats), jnp.bfloat16)
    near_keep, near_pass, rest, high, low = call(
        near_radial_kernel,
        [half, half, ((3, RIM, rows, lats), jnp.float32), square, square],
        flops,
        4 * kernels.size,
    )(near_field, weights, far_send_keep)
    far_chip = swapped(far_pass + far_core_pass, "event_0")
    rest = swapped(rest, "event_1")
    near_chip = swapped(near_pass + rest[0], "event_0")
    row = ((8, LANES), jnp.float32)
    held_steps, changes, first_row = call(
        first_gram_kernel,
        [(steps.shape, jnp.float32)] * 2 + [row],
        2 * 40 * size,
        16 * steps.size,
        in_specs=[pl.BlockSpec(memory_space=pltpu.HBM)] * 2,
        scratch_shapes=[
            pltpu.VMEM(curvature.shape, jnp.float32),
            pltpu.SemaphoreType.DMA((2, lons)),
        ],
    )(in_hbm(steps), in_hbm(curvature))
    (gram,) = call(second_gram_kernel, [row], 2 * 68 * size, 8 * steps.size)(
        held_steps, changes, first_row
    )

    def plane_of(slot, *parts):
        kernel = functools.partial(latitude_kernel, slot)
        return call(kernel, [half], 4 * lats * size, 8 * size)(*parts, high, low)[0]

    far_plane = plane_of(2, far_keep, rest, far_chip)
    pairs = []
    for c in range(cuts):
        other, flip = (((c - 1) ^ 1) + 1) % cuts if c else cuts - 1, 2 if c == 0 else 0
        pairs += [(c * events + e, other * events + (e ^ flip)) for e in range(events)]
    far_halo = lax.ppermute(far_plane, CUTS_EVENT, pairs)
    far_plane = lax.ppermute(
        far_plane,
        CUTS_EVENT,
        [(e, e ^ 2) for e in range(events)] + [(d, d) for d in range(events, cuts * events)],
    )
    near_plane = plane_of(1, near_keep, rest, near_chip)
    near_halo = lax.ppermute(near_plane, CUTS, [(c, c ^ 1) for c in range(cuts)])
    padded = [pltpu.VMEM((3, RIM, rows, lats), jnp.float32)]
    near_gradient, near_row = call(
        near_product_kernel, [half, row], 2 * 20 * size, 4 * 10 * size, scratch_shapes=padded
    )(near_halo, near_plane, far_plane, held_steps, changes, gram)
    far_gradient, outgoing = call(
        far_product_kernel,
        [half, ((cuts * events // 8, 8, LANES), jnp.float32)],
        2 * 20 * size,
        4 * 10 * size,
        scratch_shapes=padded,
    )(far_halo, far_plane, near_plane, held_steps, changes, near_row)
    outgoing = outgoing.reshape(cuts * events, 1, LANES)
    arrived = lax.all_to_all(outgoing, CUTS_EVENT, 0, 0, tiled=True).reshape(-1, 8, LANES)
    return call(
        direction_kernel,
        [block] * 2,
        2 * 17 * size,
        4 * 18 * size,
        out_specs=[pl.BlockSpec(memory_space=pltpu.HBM)] * 2,
        scratch_shapes=[pltpu.VMEM((lons, rows, lats), jnp.float32), pltpu.SemaphoreType.DMA((6,))],
    )(arrived, far_gradient, near_gradient, held_steps, changes)


def solution(mesh):
    torus = Mesh(
        mesh.devices.reshape(2, 4, 4, 2, 2), ("cuts_0", "cuts_1", "cuts_2", "event_0", "event_1")
    )
    in_specs = (P(EVENT, CUTS, None, None), P(None, CUTS, EVENT, None), P(None, CUTS, EVENT, None))
    out_specs = (P(CUTS, EVENT, None), P(CUTS, EVENT, None))
    return jax.shard_map(
        shards, mesh=torus, in_specs=in_specs, out_specs=out_specs, check_vma=False
    )
```

```python
import functools
import math

import jax
import jax.numpy as jnp
from jax import lax
from jax.experimental import pallas as pl
from jax.experimental.pallas import tpu as pltpu
from jax.sharding import Mesh
from jax.sharding import PartitionSpec as P

PAIRS = 8
RIM = 4
CUTS = ("cuts_0", "cuts_1", "cuts_2")
EVENT = ("event_0", "event_1")
CUTS_EVENT = ("cuts_0", "cuts_1", "cuts_2", "event_0", "event_1")
LANES = 128
SQUARES, STEPS_GRADIENT, CHANGES_GRADIENT = 64, 100, 108


def cycle_weights():
    unscaled = [math.exp(-((column - RIM) ** 2) / 4.5) for column in range(2 * RIM + 1)]
    whole = sum(unscaled)
    return [weight / whole for weight in unscaled]


def split(x):
    high = x.astype(jnp.bfloat16)
    low = (x - high.astype(jnp.float32)).astype(jnp.bfloat16)
    return high, low


def dot(a, b):
    return jnp.dot(a, b, preferred_element_type=jnp.float32)


def call(kernel, outs, flops, moved, limit=16, **options):
    return pl.pallas_call(
        kernel,
        out_shape=[jax.ShapeDtypeStruct(*out) for out in outs],
        compiler_params=pltpu.CompilerParams(vmem_limit_bytes=limit << 20),
        cost_estimate=pl.CostEstimate(flops=flops, bytes_accessed=moved, transcendentals=0),
        **options,
    )


def gauss_rows(length, sigma, rows, axis):
    offset = (rows - lax.broadcasted_iota(jnp.int32, rows.shape, axis)).astype(jnp.float32)
    matrix = jnp.exp(-offset * offset / (2.0 * sigma * sigma))
    return matrix / jnp.sum(matrix, axis=axis, keepdims=True)


def gauss_rows(length, sigma, rows, axis):
    offset = (rows - lax.broadcasted_iota(jnp.int32, rows.shape, axis)).astype(jnp.float32)
    matrix = jnp.exp(-offset * offset / (2.0 * sigma * sigma))
    return matrix / jnp.sum(matrix, axis=axis, keepdims=True)


def radial_products(field_ref, weights, keep_ref, pass_ref, send_keep_ref, send_pass_ref):
    for a in range(field_ref.shape[0]):
        both = dot(weights, jnp.concatenate(split(field_ref[a]), axis=0))
        length = both.shape[0] // 2
        rows = length // 4
        out = both[:length] + both[length:]
        for k, ref in enumerate((keep_ref, pass_ref, send_keep_ref, send_pass_ref)):
            ref[a] = out[k * rows : (k + 1) * rows]


def far_radial_kernel(
    kernels_ref, keep_ref, pass_ref, send_keep_ref, send_pass_ref, near_ref, weights_ref, far_ref, semaphores
):
    length = kernels_ref.shape[2]
    odd = lax.rem(cut_number(), 2)
    copies = []
    for piece, ref in enumerate((far_ref, near_ref)):
        source = kernels_ref.at[0, pl.ds(RIM * (odd ^ piece), RIM)]
        copies.append(pltpu.make_async_copy(source, ref, semaphores.at[piece]))
        copies[piece].start()
    part = 2 * lax.axis_index("event_0") + lax.axis_index("event_1")
    rows = length // 4
    local = lax.broadcasted_iota(jnp.int32, (rows, length), 0)

    def weights_of(first):
        order = [first, first ^ 2, first ^ 1, first ^ 3]
        matrix = jnp.concatenate(
            [gauss_rows(length, 3.0, local + rows * block, 1) for block in order], axis=0
        )
        return jnp.concatenate([jnp.concatenate([m, m], axis=1) for m in split(matrix)], axis=0)

    weights = weights_of(jnp.where(cut_number() == 0, part ^ 2, part))
    weights_ref[...] = weights_of(part)
    copies[0].wait()
    radial_products(far_ref, weights, keep_ref, pass_ref, send_keep_ref, send_pass_ref)
    copies[1].wait()


def near_radial_kernel(
    near_ref, weights_ref, far_send_keep_ref, keep_ref, pass_ref, rest_ref, high_ref, low_ref
):
    rest_ref[2] = far_send_keep_ref[...]
    parts = (keep_ref, pass_ref, rest_ref.at[1], rest_ref.at[0])
    radial_products(near_ref, weights_ref[...], *parts)
    lats = high_ref.shape[0]
    column = lax.broadcasted_iota(jnp.int32, (lats, lats), 1)
    high_ref[...], low_ref[...] = split(gauss_rows(lats, 4.0, column, 0))


def smoothed(field, high, low):
    count = field.shape[0]
    both = jnp.concatenate(split(field), axis=0)
    out = dot(both, high) + dot(both, low)
    return out[:count] + out[count:]


def latitude_kernel(slot, keep_ref, rest_ref, chip_ref, high_ref, low_ref, plane_ref):
    lons, rows, lats = plane_ref.shape
    summed = (keep_ref[...] + rest_ref[slot] + chip_ref[...]).reshape(lons * rows, lats)
    plane_ref[...] = smoothed(summed, high_ref[...], low_ref[...]).reshape(lons, rows, lats)


def lane_numbers():
    return lax.broadcasted_iota(jnp.int32, (8, LANES), 1)


def tiles(shape):
    return [
        (a, slice(8 * r, 8 * r + 8), slice(LANES * b, LANES * (b + 1)))
        for r in range(shape[1] // 8)
        for b in range(shape[2] // LANES)
        for a in range(shape[0])
    ]


def placed(sums):
    lanes = lane_numbers()
    row = jnp.zeros((8, LANES), jnp.float32)
    for lane, value in sums:
        row = row + jnp.where(lanes == lane, jnp.sum(value, axis=1, keepdims=True), 0.0)
    return row


def spots(shape):
    return [
        (slice(8 * r, 8 * r + 8), slice(LANES * b, LANES * (b + 1)))
        for r in range(shape[0] // 8)
        for b in range(shape[1] // LANES)
    ]


def summed_over(lons, step, size):
    return lax.fori_loop(0, lons, step, [jnp.zeros((8, LANES), jnp.float32)] * size)


def first_gram_kernel(
    steps_hbm, curvature_hbm, steps_ref, changes_ref, row_ref, curvature_ref, semaphores
):
    lons, *plane = steps_ref.shape[1:]

    def fetches(a):
        pairs = ((steps_hbm, steps_ref), (curvature_hbm, curvature_ref))
        return [
            pltpu.make_async_copy(source.at[:, a], target.at[:, a], semaphores.at[k, a])
            for k, (source, target) in enumerate(pairs)
        ]

    for a in range(lons):
        for fetch in fetches(a):
            fetch.start()
    half = PAIRS // 2

    def step(a, sums):
        for fetch in fetches(a):
            fetch.wait()
        for at in spots(plane):
            steps = [steps_ref[(i, a, *at)] for i in range(half)]
            changes = [None] * PAIRS
            for i in range(PAIRS):
                value = steps[i] if i < half else steps_ref[(i, a, *at)]
                changes[i] = curvature_ref[(i, a, *at)] * value
                changes_ref[(i, a, *at)] = changes[i]
            sums = [sums[k] + steps[k // PAIRS] * changes[k % PAIRS] for k in range(half * PAIRS)]
        return sums

    row_ref[...] = placed(enumerate(summed_over(lons, step, half * PAIRS)))


def second_gram_kernel(steps_ref, changes_ref, first_ref, row_ref):
    lons, *plane = steps_ref.shape[1:]
    half = PAIRS // 2
    upper = [(i, j) for i in range(PAIRS) for j in range(i, PAIRS)]

    def mixed(a, sums):
        for at in spots(plane):
            steps = [steps_ref[(i, a, *at)] for i in range(half, PAIRS)]
            changes = [changes_ref[(i, a, *at)] for i in range(PAIRS)]
            sums = [sums[k] + steps[k // PAIRS] * changes[k % PAIRS] for k in range(half * PAIRS)]
        return sums

    def squares(a, sums):
        for at in spots(plane):
            changes = [changes_ref[(i, a, *at)] for i in range(PAIRS)]
            sums = [value + changes[i] * changes[j] for value, (i, j) in zip(sums, upper)]
        return sums

    row = first_ref[...] + placed(enumerate(summed_over(lons, mixed, half * PAIRS), half * PAIRS))
    row_ref[...] = row + placed(enumerate(summed_over(lons, squares, len(upper)), SQUARES))


def near_base():
    return RIM * (1 - lax.rem(cut_number(), 2))


def side_products(base, halo_ref, side_ref, inner_ref, steps_ref, changes_ref, gradient_ref, padded_ref):
    lons, rows, lats = gradient_ref.shape
    weights = cycle_weights()
    outer = 2 * base // RIM
    padded_ref[outer] = halo_ref[...]
    padded_ref[1] = side_ref[...]
    padded_ref[2 - outer] = inner_ref[...]
    sums = [jnp.zeros((8, LANES), jnp.float32) for _ in range(2 * PAIRS)]
    for at in spots((rows, lats)):
        padded = [padded_ref[(k, a, *at)] for k in range(3) for a in range(RIM)]
        for a in range(lons):
            value = weights[RIM] * padded[a + RIM]
            for k in range(RIM):
                value = value + weights[k] * (padded[a + k] + padded[a + 2 * RIM - k])
            gradient_ref[(a, *at)] = value
            for pair in range(PAIRS):
                sums[pair] = sums[pair] + steps_ref[(pair, base + a, *at)] * value
                sums[PAIRS + pair] = sums[PAIRS + pair] + changes_ref[(pair, base + a, *at)] * value
    return placed(enumerate(sums, STEPS_GRADIENT))


def near_product_kernel(
    halo_ref, near_ref, far_ref, steps_ref, changes_ref, gram_ref, gradient_ref, row_ref, padded_ref
):
    operands = (halo_ref, near_ref, far_ref, steps_ref, changes_ref, gradient_ref, padded_ref)
    row_ref[...] = gram_ref[...] + side_products(near_base(), *operands)


def far_product_kernel(
    halo_ref, far_ref, near_ref, steps_ref, changes_ref, near_row_ref, gradient_ref, rows_ref, padded_ref
):
    operands = (halo_ref, far_ref, near_ref, steps_ref, changes_ref, gradient_ref, padded_ref)
    row = near_row_ref[...] + side_products(RIM - near_base(), *operands)
    row = jnp.sum(row, axis=0, keepdims=True)
    rows_ref[...] = jnp.broadcast_to(row[None], rows_ref.shape)


def direction_kernel(
    rows_ref, far_ref, near_ref, steps_ref, changes_ref,
    gradient_out, direction_out, direction_ref, semaphores,
):
    sides = ((RIM - near_base(), far_ref), (near_base(), near_ref))
    written = [
        pltpu.make_async_copy(ref, gradient_out.at[pl.ds(base, RIM)], semaphores.at[k])
        for k, (base, ref) in enumerate(sides)
    ]
    for copy in written:
        copy.start()
    row = jnp.sum(jnp.sum(rows_ref[...], axis=0), axis=0, keepdims=True)
    row = jnp.broadcast_to(row, (8, LANES))
    lanes = lane_numbers()
    pairs = lax.broadcasted_iota(jnp.int32, (8, LANES), 0)

    def column(lane_of):
        picked = jnp.where(lanes == lane_of, row, 0.0)
        return jnp.broadcast_to(jnp.sum(picked, axis=1, keepdims=True), (8, LANES))

    def element(vector, i):
        return jnp.broadcast_to(vector[i : i + 1], (8, LANES))

    def square_lanes(j):
        low, high = jnp.minimum(pairs, j), jnp.maximum(pairs, j)
        return SQUARES + low * PAIRS - ((low * (low - 1)) >> 1) + high - low

    by_change = [column(pairs * PAIRS + i) for i in range(PAIRS)]
    by_step = [column(pairs + PAIRS * i) for i in range(PAIRS)]
    squares = [column(square_lanes(i)) for i in range(PAIRS)]
    curvs = column(pairs * (PAIRS + 1))
    steps_part = column(pairs + STEPS_GRADIENT)
    changes_part = column(pairs + CHANGES_GRADIENT)
    inverse = 1.0 / curvs
    scaling = element(curvs, PAIRS - 1) / element(squares[PAIRS - 1], PAIRS - 1)
    alphas = [None] * PAIRS
    for i in reversed(range(PAIRS)):
        alphas[i] = element(inverse * steps_part, i)
        steps_part = steps_part - alphas[i] * by_change[i]
        changes_part = changes_part - alphas[i] * squares[i]
    changes_part = scaling * changes_part
    weights = [None] * PAIRS
    for i in range(PAIRS):
        weights[i] = alphas[i] - element(inverse * changes_part, i)
        changes_part = changes_part + weights[i] * by_step[i]
    change_weights = [scaling * alpha for alpha in alphas]
    copies = []
    half = RIM // 4
    for piece in range(8):
        base, gradient_ref = sides[piece // 4]
        first = piece % 4 * half
        for a, r, b in tiles((half, *far_ref.shape[1:])):
            lon = base + first + a
            value = -(scaling * gradient_ref[first + a, r, b])
            for i in range(PAIRS):
                value = value + change_weights[i] * changes_ref[i, lon, r, b]
                value = value - weights[i] * steps_ref[i, lon, r, b]
            direction_ref[half * piece + a, r, b] = value
        if copies:
            copies[-1].start()
        copies.append(
            pltpu.make_async_copy(
                direction_ref.at[pl.ds(half * piece, half)],
                direction_out.at[pl.ds(base + first, half)],
                semaphores.at[2 + piece],
            )
        )
    copies[-1].start()
    for copy in copies + written:
        copy.wait()


def in_hbm(x):
    return pltpu.with_memory_space_constraint(x, pltpu.HBM)


def swapped(x, axis):
    return lax.ppermute(x, axis, [(0, 1), (1, 0)])


def cut_number():
    number = 0
    for axis in CUTS:
        number = number * lax.axis_size(axis) + lax.axis_index(axis)
    return number


def shards(kernels, steps, curvature):
    _, lons, rad_len, lats = kernels.shape
    rows = rad_len // 4
    block = ((lons, rows, lats), jnp.float32)
    size = lons * rows * lats
    half = ((RIM, rows, lats), jnp.float32)
    cuts, events = lax.axis_size(CUTS), lax.axis_size(EVENT)
    table = ((2 * rad_len, 2 * rad_len), jnp.bfloat16)
    flops = 4 * rad_len * kernels.size
    far_keep, far_pass, far_send_keep, far_send_pass, near_field, weights = call(
        far_radial_kernel,
        [half] * 4 + [((RIM, rad_len, lats), jnp.float32), table],
        flops,
        8 * kernels.size,
        in_specs=[pl.BlockSpec(memory_space=pltpu.HBM)],
        scratch_shapes=[
            pltpu.VMEM((RIM, rad_len, lats), jnp.float32),
            pltpu.SemaphoreType.DMA((2,)),
        ],
    )(in_hbm(kernels))
    far_core_pass = swapped(far_send_pass, "event_1")
    square = ((lats, lats), jnp.bfloat16)
    near_keep, near_pass, rest, high, low = call(
        near_radial_kernel,
        [half, half, ((3, RIM, rows, lats), jnp.float32), square, square],
        flops,
        4 * kernels.size,
    )(near_field, weights, far_send_keep)
    far_chip = swapped(far_pass + far_core_pass, "event_0")
    rest = swapped(rest, "event_1")
    near_chip = swapped(near_pass + rest[0], "event_0")
    row = ((8, LANES), jnp.float32)
    held_steps, changes, first_row = call(
        first_gram_kernel,
        [(steps.shape, jnp.float32)] * 2 + [row],
        2 * 40 * size,
        16 * steps.size,
        in_specs=[pl.BlockSpec(memory_space=pltpu.HBM)] * 2,
        scratch_shapes=[
            pltpu.VMEM(curvature.shape, jnp.float32),
            pltpu.SemaphoreType.DMA((2, lons)),
        ],
    )(in_hbm(steps), in_hbm(curvature))
    (gram,) = call(second_gram_kernel, [row], 2 * 68 * size, 8 * steps.size)(
        held_steps, changes, first_row
    )

    def plane_of(slot, *parts):
        kernel = functools.partial(latitude_kernel, slot)
        return call(kernel, [half], 4 * lats * size, 8 * size)(*parts, high, low)[0]

    far_plane = plane_of(2, far_keep, rest, far_chip)
    pairs = []
    for c in range(cuts):
        other, flip = (((c - 1) ^ 1) + 1) % cuts if c else cuts - 1, 2 if c == 0 else 0
        pairs += [(c * events + e, other * events + (e ^ flip)) for e in range(events)]
    far_halo = lax.ppermute(far_plane, CUTS_EVENT, pairs)
    far_plane = lax.ppermute(
        far_plane,
        CUTS_EVENT,
        [(e, e ^ 2) for e in range(events)] + [(d, d) for d in range(events, cuts * events)],
    )
    near_plane = plane_of(1, near_keep, rest, near_chip)
    near_halo = lax.ppermute(near_plane, CUTS, [(c, c ^ 1) for c in range(cuts)])
    padded = [pltpu.VMEM((3, RIM, rows, lats), jnp.float32)]
    near_gradient, near_row = call(
        near_product_kernel, [half, row], 2 * 20 * size, 4 * 10 * size, scratch_shapes=padded
    )(near_halo, near_plane, far_plane, held_steps, changes, gram)
    far_gradient, outgoing = call(
        far_product_kernel,
        [half, ((cuts * events // 8, 8, LANES), jnp.float32)],
        2 * 20 * size,
        4 * 10 * size,
        scratch_shapes=padded,
    )(far_halo, far_plane, near_plane, held_steps, changes, near_row)
    outgoing = outgoing.reshape(cuts * events, 1, LANES)
    arrived = lax.all_to_all(outgoing, CUTS_EVENT, 0, 0, tiled=True).reshape(-1, 8, LANES)
    return call(
        direction_kernel,
        [block] * 2,
        2 * 17 * size,
        4 * 18 * size,
        out_specs=[pl.BlockSpec(memory_space=pltpu.HBM)] * 2,
        scratch_shapes=[
            pltpu.VMEM((lons, rows, lats), jnp.float32),
            pltpu.SemaphoreType.DMA((10,)),
        ],
    )(arrived, far_gradient, near_gradient, held_steps, changes)


def solution(mesh):
    torus = Mesh(
        mesh.devices.reshape(2, 4, 4, 2, 2), ("cuts_0", "cuts_1", "cuts_2", "event_0", "event_1")
    )
    in_specs = (P(EVENT, CUTS, None, None), P(None, CUTS, EVENT, None), P(None, CUTS, EVENT, None))
    out_specs = (P(CUTS, EVENT, None), P(CUTS, EVENT, None))
    return jax.shard_map(
        shards, mesh=torus, in_specs=in_specs, out_specs=out_specs, check_vma=False
    )
```
